32 devices in a mesh: gx: 4 (over z), gy: 2 (over x), gz: 4 (over y, core).
Axes of the slice: x: 2, y: 2, z: 4, core: 2. Of those that a mesh axis runs over, the one named last changes fastest.
Arguments:
- block_x: float32 [16, 24, 12, 512], P(None, 'gz', 'gy', 'gx')
- block_hx: float32 [16, 24, 12, 512], P(None, 'gz', 'gy', 'gx')
- block_p: float32 [16, 24, 12, 512], P(None, 'gz', 'gy', 'gx')
- block_hp: float32 [16, 24, 12, 512], P(None, 'gz', 'gy', 'gx')
- potential: float32 [24, 12, 512], P('gz', 'gy', 'gx'), may hold values from -2 to 2
- projectors: float32 [4, 2, 4, 8, 4, 256], P('gz', 'gy', 'gx'), may hold values from -0.75 to 0.75
- coupling: float32 [4, 2, 4, 8, 4, 4], P('gz', 'gy', 'gx'), may hold values from 0.25 to 1.25
- atom_count: int32 [4, 2, 4], P('gz', 'gy', 'gx'), may hold values from 0 to 8, as said below
- proj_count: int32 [4, 2, 4, 8], P('gz', 'gy', 'gx'), may hold values from 1 to 4
- offsets: int32 [3, 4, 2, 4, 8], P(None, 'gz', 'gy', 'gx'), may hold values from 0 to 127, as said below
- extents: int32 [3, 4, 2, 4, 8], P(None, 'gz', 'gy', 'gx'), may hold values from 2 to 16, as said below
Outputs:
- w_block: float32 [16, 24, 12, 512], P(None, 'gz', 'gy', 'gx')
- hw_block: float32 [16, 24, 12, 512], P(None, 'gz', 'gy', 'gx')
- gram: float32 [48, 48], replicated
- rayleigh: float32 [48, 48], replicated
The draws below stay inside these ranges and needn't reach their ends.
Inputs may be any that keep to these rules, and one draw needn't show every extreme that they name: `atom_count`: slots at and above a domain's count are empty; some domain is full in every draw. The first proj_count projectors of a slot are used. `offsets`: components z, y, x are below 6, 6, 128. `extents`: components z, y, x are at most 4, 4, 16; some slot has the full box in every draw.
All inputs are finite; a program needn't handle non-finite values.
Results may differ from the reference program's by a relative error of at most 0.0003.
Values sent between devices are 32-bit elements; how exact they have to be, the bound alone decides.
A program may use at most 64 MiB of HBM per device.

```python
import math
import jax
import jax.numpy as jnp
from jax import lax

NCOL = 16
NPROJ = 4
CZ = 6
CY = 6
CX = 128
SLOTS = 8
BZ = 4
BY = 4
BX = 16
BOXC = 256
DOMAINS_Z = 4
DOMAINS_Y = 2
DOMAINS_X = 4
NZ = 24
NY = 12
NX = 512


def paired_fields(key, salt):
    base_key = jax.random.fold_in(key, salt)
    keys = jax.random.split(base_key, 6)
    shape = (NCOL, NZ, NY, NX)
    rough = jax.random.normal(keys[1], shape, jnp.float32)
    domain_scale = jnp.exp(jax.random.uniform(keys[2], (NZ // CZ, NY // CY, 1), jnp.float32, -1.2, 1.2))
    scale_field = jnp.repeat(jnp.repeat(domain_scale, CZ, axis=0), CY, axis=1)
    first_field = rough * scale_field[None]
    mixing = jnp.diag(jax.random.uniform(keys[3], (NCOL,), jnp.float32, 1.0, 4.0)) + 0.3 * jax.random.normal(keys[4], (NCOL, NCOL), jnp.float32) / math.sqrt(NCOL)
    second_field = jnp.einsum('kzyx,kj->jzyx', first_field, mixing) + 0.5 * jax.random.normal(keys[5], shape, jnp.float32) * scale_field[None]
    return (first_field, second_field)


def draw_block_x(key, part):
    return paired_fields(key, 11)[0]


def draw_block_hx(key, part):
    return paired_fields(key, 11)[1]


def draw_block_p(key, part):
    return paired_fields(key, 23)[0]


def draw_block_hp(key, part):
    return paired_fields(key, 23)[1]


def corner_slot():
    shape = (DOMAINS_Z, DOMAINS_Y, DOMAINS_X, SLOTS)
    total_slots = DOMAINS_Z * DOMAINS_Y * DOMAINS_X * SLOTS
    flat_index = jnp.arange(total_slots, dtype=jnp.int32).reshape(shape)
    return flat_index == total_slots - SLOTS


def draw_atom_count(key, part):
    keys = jax.random.split(jax.random.fold_in(key, 5), 4)
    shape = (DOMAINS_Z, DOMAINS_Y, DOMAINS_X)
    heavy_domain = jax.random.randint(keys[0], shape, 0, 4) == 0
    large_count = jax.random.randint(keys[1], shape, SLOTS // 2, SLOTS + 1)
    small_count = jax.random.randint(keys[2], shape, 0, SLOTS // 4 + 1)
    counts = jnp.where(heavy_domain, large_count, small_count)
    domain_total = DOMAINS_Z * DOMAINS_Y * DOMAINS_X
    chosen = jax.random.randint(keys[3], (), 0, domain_total)
    flat_index = jnp.arange(domain_total, dtype=jnp.int32).reshape(shape)
    full_domain = (flat_index == chosen) | (flat_index == domain_total - 1)
    return jnp.where(full_domain, SLOTS, counts).astype(jnp.int32)


def draw_offsets(key, part):
    keys = jax.random.split(jax.random.fold_in(key, 31), 3)
    shape = (DOMAINS_Z, DOMAINS_Y, DOMAINS_X, SLOTS)
    edge_slot = corner_slot()
    along_z = jnp.where(edge_slot, CZ - 1, jax.random.randint(keys[0], shape, 0, CZ))
    along_y = jnp.where(edge_slot, CY - 1, jax.random.randint(keys[1], shape, 0, CY))
    along_x = jnp.where(edge_slot, CX - 1, jax.random.randint(keys[2], shape, 0, CX))
    return jnp.stack([along_z, along_y, along_x]).astype(jnp.int32)


def draw_extents(key, part):
    keys = jax.random.split(jax.random.fold_in(key, 47), 4)
    shape = (DOMAINS_Z, DOMAINS_Y, DOMAINS_X, SLOTS)
    total_slots = DOMAINS_Z * DOMAINS_Y * DOMAINS_X * SLOTS
    chosen = jax.random.randint(keys[3], (), 0, total_slots)
    flat_index = jnp.arange(total_slots, dtype=jnp.int32).reshape(shape)
    full_box = (flat_index == chosen) | corner_slot()
    along_z = jnp.where(full_box, BZ, jax.random.randint(keys[0], shape, 2, BZ + 1))
    along_y = jnp.where(full_box, BY, jax.random.randint(keys[1], shape, 2, BY + 1))
    along_x = jnp.where(full_box, BX, jax.random.randint(keys[2], shape, 2, BX + 1))
    return jnp.stack([along_z, along_y, along_x]).astype(jnp.int32)


def place_ends(array, rng, low, top_value):
    dims = array.shape
    index_at = [jax.random.randint(jax.random.fold_in(rng, axis), (), 0, dims[axis]) for axis in range(len(dims))]
    array = array.at[tuple(index_at)].set(low)
    longest = dims.index(max(dims))
    index_at[longest] = (index_at[longest] + 1) % dims[longest]
    return array.at[tuple(index_at)].set(top_value)


def block_levels(own_key, extent, cuts, low, largest):
    gain, own = 1.0, jax.random.fold_in(own_key, 6)
    for axis_at, blocks in cuts:
        heights = jnp.exp(jax.random.uniform(jax.random.fold_in(own, axis_at), (blocks,), jnp.float32, low / len(cuts), largest / len(cuts)))
        gain = gain * jnp.repeat(heights, extent[axis_at] // blocks).reshape([-1 if axis == axis_at else 1 for axis in range(len(extent))])
    return gain


def gaussian(stream_key, dims, scale, bound, pieces=(), kind=jnp.bfloat16):
    values = scale * jax.random.normal(stream_key, dims, jnp.float32)
    if pieces:
        values = values * block_levels(stream_key, dims, pieces, -0.22, 0.18)
    return jnp.clip(values, -bound, bound).astype(kind)


def setup_inputs(seed: int = 0) -> dict:
    splits = jax.random.split(jax.random.key(seed), 12)
    block_x = draw_block_x(jax.random.fold_in(splits[11], 71), 0)
    block_hx = draw_block_hx(jax.random.fold_in(splits[11], 71), 0)
    block_p = draw_block_p(jax.random.fold_in(splits[11], 71), 0)
    block_hp = draw_block_hp(jax.random.fold_in(splits[11], 71), 0)
    potential = jnp.clip(jax.random.uniform(splits[4], (NZ, NY, NX), jnp.float32, -2.0, 2.0) * block_levels(splits[4], (NZ, NY, NX), ((0, 4), (1, 2), (2, 4)), -0.4, 0.0), -2.0, 2.0)
    projectors = gaussian(splits[5], (DOMAINS_Z, DOMAINS_Y, DOMAINS_X, SLOTS, NPROJ, BOXC), 0.125, 0.75, ((0, 4), (1, 2), (2, 4)), jnp.float32)
    coupling = jnp.clip(0.25 + 1.0 * jax.random.uniform(splits[6], (DOMAINS_Z, DOMAINS_Y, DOMAINS_X, SLOTS, NPROJ, NPROJ), jnp.float32) ** block_levels(splits[6], (DOMAINS_Z, DOMAINS_Y, DOMAINS_X, SLOTS, NPROJ, NPROJ), ((0, 4), (1, 2), (2, 4)), -0.2, 0.2), 0.25, 1.25)
    atom_count = draw_atom_count(jax.random.fold_in(splits[11], 71), 0)
    proj_count = place_ends(jax.random.randint(splits[8], (DOMAINS_Z, DOMAINS_Y, DOMAINS_X, SLOTS), 1, NPROJ + 1), jax.random.fold_in(splits[8], 1), 1, NPROJ).astype(jnp.int32)
    offsets = draw_offsets(jax.random.fold_in(splits[11], 71), 0)
    extents = draw_extents(jax.random.fold_in(splits[11], 71), 0)
    return {"block_x": block_x, "block_hx": block_hx, "block_p": block_p, "block_hp": block_hp, "potential": potential, "projectors": projectors, "coupling": coupling, "atom_count": atom_count, "proj_count": proj_count, "offsets": offsets, "extents": extents}


LAP_CENTER = -5369.0 / 1800.0
LAP_COEFFS = (12.0 / 7.0, -15.0 / 56.0, 10.0 / 189.0, -1.0 / 112.0, 2.0 / 1925.0, -1.0 / 16632.0)
HIGHEST = lax.Precision.HIGHEST

def masked_projectors(projectors, atom_count, proj_count, extents):
    slot_index = jnp.arange(projectors.shape[-3], dtype=jnp.int32)
    live_slot = slot_index < atom_count[..., None]
    proj_index = jnp.arange(projectors.shape[-2], dtype=jnp.int32)
    live_proj = proj_index < proj_count[..., None]
    cell_index = jnp.arange(projectors.shape[-1], dtype=jnp.int32)
    along_z = cell_index // (BY * BX)
    along_y = cell_index // BX % BY
    along_x = cell_index % BX
    inside = (along_z < extents[0][..., None]) & (along_y < extents[1][..., None]) & (along_x < extents[2][..., None])
    keeper = live_slot[..., None, None] & live_proj[..., None] & inside[..., None, :]
    return jnp.where(keeper, projectors, jnp.zeros_like(projectors))

def kinetic_term(column_block):
    summed = 3.0 * LAP_CENTER * column_block
    for distance, weight in enumerate(LAP_COEFFS, start=1):
        for axis_number in (1, 2, 3):
            summed = summed + weight * (jnp.roll(column_block, distance, axis_number) + jnp.roll(column_block, -distance, axis_number))
    return -0.5 * summed

def nonlocal_term(column_block, beta_masked, sym_coupling, offsets):
    columns = column_block.shape[0]
    start_z = jnp.arange(DOMAINS_Z, dtype=jnp.int32)[:, None, None, None] * CZ + offsets[0]
    start_y = jnp.arange(DOMAINS_Y, dtype=jnp.int32)[None, :, None, None] * CY + offsets[1]
    start_x = jnp.arange(DOMAINS_X, dtype=jnp.int32)[None, None, :, None] * CX + offsets[2]
    cell_index = jnp.arange(BZ * BY * BX, dtype=jnp.int32)
    grid_z = (start_z[..., None] + cell_index // (BY * BX)) % NZ
    grid_y = (start_y[..., None] + cell_index // BX % BY) % NY
    grid_x = (start_x[..., None] + cell_index % BX) % NX
    flat_index = ((grid_z * NY + grid_y) * NX + grid_x).astype(jnp.int32)
    flat_block = column_block.reshape(columns, NZ * NY * NX)
    gathered = flat_block[:, flat_index]
    correlations = jnp.einsum('abcspk,nabcsk->abcspn', beta_masked, gathered, precision=HIGHEST)
    weights_out = jnp.einsum('abcspq,abcsqn->abcspn', sym_coupling, correlations, precision=HIGHEST)
    spread = jnp.einsum('abcspk,abcspn->nabcsk', beta_masked, weights_out, precision=HIGHEST)
    result = jnp.zeros_like(flat_block).at[:, flat_index.reshape(-1)].add(spread.reshape(columns, -1))
    return result.reshape(column_block.shape)

def inner_product(left_block, right_block, cell_weight):
    left_flat = left_block.reshape(left_block.shape[0], -1)
    right_flat = right_block.reshape(right_block.shape[0], -1)
    return jnp.einsum('ic,jc->ij', left_flat, right_flat, precision=HIGHEST) * cell_weight

def reference(block_x, block_hx, block_p, block_hp, potential, projectors, coupling, atom_count, proj_count, offsets, extents):
    cell_weight = 1.0 / (NZ * NY * NX)
    beta_masked = masked_projectors(projectors, atom_count, proj_count, extents)
    sym_coupling = 0.5 * (coupling + jnp.swapaxes(coupling, -1, -2))
    correlation = inner_product(block_x, block_x, cell_weight)
    projected = inner_product(block_x, block_hx, cell_weight)
    factor = jnp.linalg.cholesky(correlation)
    ritz_theta = jax.scipy.linalg.cho_solve((factor, True), projected)
    residual = block_hx - jnp.einsum('kzyx,kj->jzyx', block_x, ritz_theta, precision=HIGHEST)
    w_block = residual / (1.0 + potential * potential)
    hw_block = kinetic_term(w_block) + potential * w_block + nonlocal_term(w_block, beta_masked, sym_coupling, offsets)
    search_space = (block_x, w_block, block_p)
    images = (block_hx, hw_block, block_hp)
    gram = jnp.concatenate([jnp.concatenate([inner_product(left_block, right_block, cell_weight) for right_block in search_space], axis=1) for left_block in search_space], axis=0)
    rayleigh = jnp.concatenate([jnp.concatenate([inner_product(left_block, right_block, cell_weight) for right_block in images], axis=1) for left_block in search_space], axis=0)
    return (w_block, hw_block, gram, rayleigh)
```

```python
import functools

import jax
import jax.numpy as jnp
from jax import lax
from jax.experimental import pallas as pl
from jax.experimental.pallas import tpu as pltpu
from jax.sharding import PartitionSpec as P

BZ, BY, BX = 4, 4, 16
LAP_CENTER = -5369.0 / 1800.0
LAP_COEFFS = (12.0 / 7.0, -15.0 / 56.0, 10.0 / 189.0, -1.0 / 112.0, 2.0 / 1925.0, -1.0 / 16632.0)
MESH = pl.DeviceIdType.MESH
VMEM_LIMIT = (63 << 20) - (64 << 10)
AXES = ("gz", "gy", "gx")
F32 = jnp.float32
BF16 = jnp.bfloat16
HP, HX, XX, PP, WW, HW = range(6)


def tiles_of(count):
    return -(-count // 8)


def solved(packed, cols, acol):
    shape = (8, 128)

    def spread(lane_at):
        return jnp.broadcast_to(packed[:, lane_at : lane_at + 1], shape)

    for j in range(cols):
        if j < 8:
            acol[j, 0:8] = spread(2 * cols + j)
        acol[j, 8:16] = spread(3 * cols + j)
    a = {}
    for j in range(cols):
        for i in range(j, cols):
            a[i, j] = jnp.broadcast_to(acol[j, i : i + 1, :], shape)
    scale = [lax.rsqrt(a[i, i]) for i in range(cols)]
    for i, j in a:
        a[i, j] = a[i, j] * scale[i] * scale[j]
    right = [
        [spread(half * cols + k) * scale[k] for half in range(2)] for k in range(cols)
    ]
    low = {}
    inverse = []
    for k in range(0, cols, 2):
        p, q, r = a[k, k], a[k + 1, k], a[k + 1, k + 1]
        det = 1.0 / (p * r - q * q)
        p, q, r = r * det, -q * det, p * det
        inverse.append((p, q, r))
        for i in range(k + 2, cols):
            low[i, k] = a[i, k] * p + a[i, k + 1] * q
            low[i, k + 1] = a[i, k] * q + a[i, k + 1] * r
            for j in range(k + 2, i + 1):
                a[i, j] = a[i, j] - (low[i, k] * a[j, k] + low[i, k + 1] * a[j, k + 1])
            right[i] = [
                right[i][h] - (low[i, k] * right[k][h] + low[i, k + 1] * right[k + 1][h])
                for h in range(2)
            ]
    out = [None] * cols
    for k in range(cols - 2, -1, -2):
        p, q, r = inverse[k // 2]
        halves = []
        for h in range(2):
            first = right[k][h] * p + right[k + 1][h] * q
            second = right[k][h] * q + right[k + 1][h] * r
            for i in range(cols - 1, k + 1, -1):
                first = first - low[i, k] * out[i][h]
                second = second - low[i, k + 1] * out[i][h]
            halves.append((first, second))
        out[k] = [halves[0][0], halves[1][0]]
        out[k + 1] = [halves[0][1], halves[1][1]]
    return [
        jnp.concatenate([out[k][0] * scale[k], out[k][1] * scale[k]], 0) for k in range(cols)
    ]


def kernel(
    sizes, groups, dims,
    off_ref, ext_ref, count_ref, proj_ref, d_in, x_in, hx_in, p_in, hp_in, v_in, beta_in,
    w_out, hw_out, gram_out, ray_out, red1_ref, w_ref, hw_ref, gram_ref, ray_ref,
    acol, dtab, d_ref, v_ref, beta_ref,
    stack, zext, ybuf, zybuf, plow, phigh, xr, xl, frame, frame_x, halo_x,
    blo, bhi, pieces, nf, nh, spack, rz, ry, rzy, rx, wout,
    *rest,
):
    cz, cy, cx, slots, nproj, cols = dims
    nz, ny, nx = sizes
    n_red = len(groups)
    bufs = (rest[:n_red], rest[n_red : 2 * n_red], rest[2 * n_red : 3 * n_red])
    rest = rest[3 * n_red :]
    red_send, red_recv, halo_send, halo_recv, spill_send, spill_recv = rest[:6]
    load_sem, out_sem, x_ref, hx_ref, p_ref, hp_ref = rest[6:]
    loads = []
    for i, (source, target) in enumerate(
        (
            (x_in, x_ref), (hx_in, hx_ref), (v_in, v_ref), (beta_in, beta_ref),
            (p_in, p_ref), (hp_in, hp_ref), (d_in, d_ref),
        )
    ):
        loads.append(pltpu.make_async_copy(source, target, load_sem.at[i]))
        loads[-1].start()
    zi, yi, xi = (lax.axis_index(a) for a in AXES)
    size_of = dict(zip(AXES, sizes))
    here = dict(zip(AXES, (zi, yi, xi)))
    fz, fy = cz + BZ - 1, cy + BY - 1
    own = cz * cy
    lane = lax.broadcasted_iota(jnp.int32, (cols, 128), 1)

    def neighbour(dz, dy, dx):
        step = dict(zip(AXES, (dz, dy, dx)))
        return {a: lax.rem(here[a] + step[a] + size_of[a], size_of[a]) for a in AXES}

    def member(group, offset):
        total = 1
        index = 0
        for a in group:
            total *= size_of[a]
            index = index * size_of[a] + here[a]
        target = lax.rem(index + offset, total)
        device = {}
        for a in reversed(group):
            device[a] = lax.rem(target, size_of[a])
            target = target // size_of[a]
        return {a: device.get(a, here[a]) for a in AXES}, index, total

    octant = [(1, 0, 0), (0, 1, 0), (1, 1, 0), (0, 0, 1), (1, 0, 1), (0, 1, 1), (1, 1, 1)]
    barrier = pltpu.get_barrier_semaphore()
    greeted = 0
    for group in groups:
        total = member(group, 0)[2]
        for offset in range(1, total):
            pl.semaphore_signal(
                barrier, inc=1, device_id=member(group, offset)[0], device_id_type=MESH
            )
            greeted += 1
    for dz, dy, dx in octant:
        for sign in (1, -1):
            pl.semaphore_signal(
                barrier, inc=1, device_id=neighbour(sign * dz, sign * dy, sign * dx),
                device_id_type=MESH,
            )
            greeted += 1

    def split_store(kind, cell, value):
        high = value.astype(BF16)
        low = (value - high.astype(F32)).astype(BF16)
        start = cell * 128 if isinstance(cell, int) else pl.multiple_of(cell * 128, 128)
        stack[kind * 32 : kind * 32 + 32, pl.ds(start, 128)] = jnp.concatenate([high, low], 0)

    def split_all(*kinds):
        @pl.loop(0, cz)
        def _(z):
            for y in range(cy):
                cell = z * cy + y
                for kind, ref in kinds:
                    split_store(kind, cell, ref[cell])

    for load in loads[:2]:
        load.wait()
    split_all((HX, hx_ref), (XX, x_ref))

    def products(left, right_from, right_to, count=1):
        m = lax.dot_general(
            stack[left * 32 : (left + count) * 32, :],
            stack[right_from * 32 : right_to * 32, :],
            (((1,), (1,)), ((), ())),
            preferred_element_type=F32,
        )
        parts = [m[32 * i : 32 * i + cols] + m[32 * i + cols : 32 * i + 32] for i in range(count)]
        return parts if count > 1 else parts[0]

    def reduced(which, payload):
        base = which * sum(member(g, 0)[2] for g in groups)
        for phase, group in enumerate(groups):
            buf = bufs[which][phase]
            _, index, total = member(group, 0)
            buf[index] = payload
            if phase == 0 and which == 2:
                pl.semaphore_wait(barrier, greeted)
            copies = []
            for offset in range(1, total):
                copies.append(
                    pltpu.make_async_remote_copy(
                        src_ref=buf.at[index],
                        dst_ref=buf.at[index],
                        send_sem=red_send.at[base + offset],
                        recv_sem=red_recv.at[base + offset],
                        device_id=member(group, offset)[0],
                        device_id_type=MESH,
                    )
                )
                copies[-1].start()
            base += total
            yield None
            for copy in copies:
                copy.wait()
            payload = buf[0]
            for slot in range(1, total):
                payload = payload + buf[slot]
        yield payload

    def finish(steps):
        out = None
        for out in steps:
            pass
        return out

    both = lax.dot_general(
        stack[HX * 32 : XX * 32 + 32, :], stack[XX * 32 : XX * 32 + 32, :],
        (((1,), (1,)), ((), ())), preferred_element_type=F32,
    )
    both = jnp.concatenate([both, jnp.zeros((64, 96), F32)], 1)
    turn_hx = both[:cols] + both[cols:32]
    corr = both[32 : 32 + cols] + both[32 + cols :]
    narrow = lax.broadcasted_iota(jnp.int32, (8, 128), 1)

    def merged(tile):
        return tile + pltpu.roll(tile, 128 - cols, 1)

    payload0 = jnp.where(narrow < cols, merged(turn_hx[:8]), 0.0)
    for at, tile in ((1, turn_hx[8:]), (2, corr[:8]), (3, corr[8:])):
        moved = pltpu.roll(merged(tile), at * cols, 1)
        payload0 = jnp.where((narrow >= at * cols) & (narrow < at * cols + cols), moved, payload0)
    solving = reduced(2, payload0)
    next(solving)
    for load in loads[2:]:
        load.wait()
    split_all((HP, hp_ref), (PP, p_ref))
    hx_row, x_row, p_row = products(HX, HP, WW, 3)
    first = jnp.where((lane >= 32) & (lane < 64), pltpu.roll(hx_row, 96, 1), x_row)

    def paired(upper, lower):
        upper = upper + pltpu.roll(upper, 112, 1)
        lower = lower + pltpu.roll(lower, 112, 1)
        return jnp.where(lane % 32 < 16, upper, pltpu.roll(lower, 16, 1))

    reduction = reduced(0, paired(first, p_row))

    per_slot = BZ * BY * nproj
    lane_p = lax.broadcasted_iota(jnp.int32, (nproj, 128), 1)
    row_p = lax.broadcasted_iota(jnp.int32, (nproj, 128), 0)
    in_tile = 128 // BX
    for s in range(slots):
        ox = off_ref[2, 0, 0, 0, s]
        along = lax.rem(lane_p - ox + 128, 128)
        along = jnp.where(row_p < proj_ref[0, s], along, 128)
        low_side = lane_p >= ox
        live = s < count_ref[0, 0, 0]
        for a in range(BZ):
            for b in range(BY):
                used = live & (a < ext_ref[0, 0, 0, 0, s]) & (b < ext_ref[1, 0, 0, 0, s])
                limit = jnp.where(used, jnp.minimum(ext_ref[2, 0, 0, 0, s], BX), 0)
                box = a * BY + b
                part = beta_ref[s, :, (box // in_tile) * 128 : (box // in_tile) * 128 + 128]
                part = pltpu.roll(part, lax.rem(ox + 128 - BX * (box % in_tile), 128), 1)
                part = jnp.where(along < limit, part, 0.0)
                row = s * per_slot + box * nproj
                blo[row : row + nproj, :] = jnp.where(low_side, part, 0.0)
                bhi[row : row + nproj, :] = jnp.where(low_side, 0.0, part)
    for p in range(nproj):
        for s in range(slots):
            dtab[s, p * nproj : p * nproj + nproj, :] = jnp.broadcast_to(
                d_ref[p, :, s : s + 1], (nproj, 128)
            )
    rim_y = BY + 2
    rim = (BZ + 2) * rim_y

    @pl.loop(0, slots)
    def _(s):
        for i in range(rim):
            if i < rim_y or i >= rim - rim_y or i % rim_y in (0, rim_y - 1):
                pieces[s * rim + i] = jnp.zeros(pieces.shape[1:], F32)

    next(solving)
    next(reduction)
    sums0 = finish(solving)
    next(reduction)
    sums0 = solved(sums0, cols, acol)
    theta_cols = sums0

    @pl.loop(0, cz)
    def _(z):
        for y in range(cy):
            cell = z * cy + y
            xs = x_ref[cell]
            value = hx_ref[cell]
            for k in range(cols):
                value = value - theta_cols[k] * xs[k : k + 1, :]
            vv = v_ref[z, y : y + 1, :]
            value = value * (1.0 / (1.0 + vv * vv))
            zext[cz + z, y] = value
            w_ref[cell] = value
            split_store(WW, cell, value)

    for q in range(tiles_of(own)):
        low = jnp.zeros((cols, 128), F32)
        high = low
        for j in range(min(8, own - 8 * q)):
            tile = zext[cz + (8 * q + j) // cy, (8 * q + j) % cy]
            keep = (lane >= 16 * j) & (lane < 16 * j + 16)
            low = jnp.where(keep, pltpu.roll(tile, 16 * j, 1) if j else tile, low)
            high = jnp.where(keep, pltpu.roll(tile, (16 * j + 16) % 128, 1) if j < 7 else tile, high)
        plow[q] = low
        phigh[q] = high

    two_y = ny == 2
    more_z, more_y = fz - cz, fy - cy
    z_tiles = tiles_of(more_z * cy)
    corner_tiles = tiles_of((more_z - 1) * cy + more_y)

    def some(ref, z, dz, y, dy):
        return ref.at[pl.ds(z, dz), pl.ds(y, dy)]

    def layers(target, base, z, dz, y, dy, where):
        return some(zext, cz + z, dz, y, dy), some(target, base + z, dz, y, dy), where

    early = [
        (some(zext, cz, more_z, 0, more_y), zybuf, (-1, -1, 0)),
        (plow.at[pl.ds(0, corner_tiles)], xr.at[3, pl.ds(0, corner_tiles)], (-1, -1, -1)),
        (plow, xr.at[2], (0, -1, -1)),
        (plow.at[pl.ds(0, z_tiles)], xr.at[1, pl.ds(0, z_tiles)], (-1, 0, -1)),
        (plow, xr.at[0], (0, 0, -1)),
        layers(ybuf.at[1], 0, 0, cz, 0, more_y, (0, -1, 0)),
        layers(zext, 2 * cz, 0, more_z, 0, cy, (-1, 0, 0)),
    ]
    late = [
        (phigh, xl, (0, 0, 1)),
        layers(ybuf.at[1], 0, 0, cz, more_y, cy - more_y, (0, -1, 0)),
        layers(zext, 2 * cz, more_z, cz - more_z, 0, cy, (-1, 0, 0)),
        layers(zext, 0, 0, cz, 0, cy, (1, 0, 0)),
    ]
    if not two_y:
        late.append(layers(ybuf.at[0], 0, 0, cz, 0, cy, (0, 1, 0)))

    def launch(sends, send_sem, recv_sem, first=0):
        copies = []
        for i, (source, target, where) in enumerate(sends, start=first):
            copies.append(
                pltpu.make_async_remote_copy(
                    src_ref=source,
                    dst_ref=target,
                    send_sem=send_sem.at[i],
                    recv_sem=recv_sem.at[i],
                    device_id=neighbour(*where),
                    device_id_type=MESH,
                )
            )
            copies[-1].start()
        return copies

    copies = launch(early, halo_send, halo_recv)
    late_copies = launch(late, halo_send, halo_recv, len(early))
    outs = [
        pltpu.make_async_copy(source, target, out_sem.at[i])
        for i, (source, target) in enumerate(
            ((w_ref, w_out), (hw_ref, hw_out), (gram_ref, gram_out), (ray_ref, ray_out))
        )
    ]
    outs[0].start()
    w_row = products(WW, HP, WW)
    w_row2 = products(WW, XX, HW)
    red1_ref[...] = finish(reduction)
    for copy in copies:
        copy.wait()

    below_y = 1 if two_y else 0
    for z in range(fz):
        for y in range(fy):
            up_z, up_y = z >= cz, y >= cy
            local = (z - cz * up_z) * cy + (y - cy * up_y)
            if up_z and up_y:
                tile = zybuf[z - cz, y - cy]
            elif up_z:
                tile = zext[cz + z, y]
            elif up_y:
                tile = ybuf[1, z, y - cy]
            else:
                tile = zext[cz + z, y]
            frame[z * fy + y] = tile
            shift = (128 - 16 * (local % 8)) % 128
            tile = xr[up_z + 2 * up_y, local // 8]
            tile = pltpu.roll(tile, shift, 1) if shift else tile
            frame_x[z * fy + y] = tile

    @pl.loop(0, slots)
    def _(s):
        oz, oy = off_ref[0, 0, 0, 0, s], off_ref[1, 0, 0, 0, s]
        sums = [jnp.zeros((cols, 128), F32) for _ in range(nproj)]
        for a in range(BZ):
            for b in range(BY):
                at = (oz + a) * fy + oy + b
                tile, tile_x = frame[at], frame_x[at]
                base = s * per_slot + (a * BY + b) * nproj
                for q in range(nproj):
                    sums[q] = sums[q] + tile * blo[pl.ds(base + q, 1), :]
                    sums[q] = sums[q] + jnp.where(
                        lane < 16, tile_x * bhi[pl.ds(base + q, 1), :], 0.0
                    )
        overlaps = [jnp.broadcast_to(jnp.sum(v, axis=1, keepdims=True), (cols, 128)) for v in sums]
        outs = []
        dm = {}
        for p in range(nproj):
            for q in range(nproj):
                at = p * nproj + q
                dm[p, q] = dtab[s, at : at + 1, :]
        for p in range(nproj):
            value = overlaps[p] * dm[p, p]
            for q in range(nproj):
                if q != p:
                    value = value + overlaps[q] * (0.5 * (dm[p, q] + dm[q, p]))
            outs.append(value)
        for a in range(BZ):
            for b in range(BY):
                base = s * per_slot + (a * BY + b) * nproj
                low = outs[0] * blo[pl.ds(base, 1), :]
                high = outs[0] * bhi[pl.ds(base, 1), :]
                for p in range(1, nproj):
                    low = low + outs[p] * blo[pl.ds(base + p, 1), :]
                    high = high + outs[p] * bhi[pl.ds(base + p, 1), :]
                place = s * rim + (a + 1) * rim_y + b + 1
                pieces[place, 0] = low
                pieces[place, 1] = high

    @pl.loop(0, fz)
    def _(z):
        starts = []
        for s in range(slots):
            a = jnp.minimum(jnp.maximum(z - off_ref[0, 0, 0, 0, s], -1), BZ) + 1
            starts.append(s * rim + a * rim_y)
        for y in range(fy):
            low = jnp.zeros((cols, 128), F32)
            high = low
            for s in range(slots):
                b = jnp.minimum(jnp.maximum(y - off_ref[1, 0, 0, 0, s], -1), BY) + 1
                low = low + pieces[starts[s] + b, 0]
                high = high + pieces[starts[s] + b, 1]
            nf[z, y] = low
            nh[z, y] = high

    spans = []
    filled = 0
    for up_z in (0, 1):
        for up_y in (0, 1):
            cells = [
                (z, y)
                for z in (range(cz, fz) if up_z else range(cz))
                for y in (range(cy, fy) if up_y else range(cy))
            ]
            spans.append((filled, up_z, up_y, cells))
            for q in range(tiles_of(len(cells))):
                tile = jnp.zeros((cols, 128), F32)
                for j, (z, y) in enumerate(cells[8 * q : 8 * q + 8]):
                    keep = (lane >= 16 * j) & (lane < 16 * j + 16)
                    value = nh[z, y]
                    tile = jnp.where(keep, pltpu.roll(value, 16 * j, 1) if j else value, tile)
                spack[filled + q] = tile
            filled += tiles_of(len(cells))
    sends = [
        (nf.at[pl.ds(cz, more_z), pl.ds(0, cy)], rz, (1, 0, 0)),
        (nf.at[pl.ds(0, cz), pl.ds(cy, more_y)], ry, (0, 1, 0)),
        (nf.at[pl.ds(cz, more_z), pl.ds(cy, more_y)], rzy, (1, 1, 0)),
    ]
    for begin, up_z, up_y, cells in spans:
        part = pl.ds(begin, tiles_of(len(cells)))
        sends.append((spack.at[part], rx.at[part], (up_z, up_y, 1)))
    copies = launch(sends, spill_send, spill_recv)

    for copy in late_copies:
        copy.wait()
    for cell in range(own):
        turn = (112 - 16 * (cell % 8)) % 128
        left = xl[cell // 8]
        left = pltpu.roll(left, turn, 1) if turn else left
        halo_x[cell] = jnp.where(lane < 64, frame_x[cell // cy * fy + cell % cy], left)

    @pl.loop(0, cz)
    def _(z):
        for y in range(cy):
            cell = z * cy + y
            centre = zext[cz + z, y]
            edge = halo_x[cell]
            vv = v_ref[z, y : y + 1, :]
            total = centre * (vv - 1.5 * LAP_CENTER)
            for k, weight in enumerate(LAP_COEFFS, start=1):
                beside = zext[cz + z + k, y] + zext[cz + z - k, y]
                for target in (y + k, y - k):
                    if target >= cy:
                        beside = beside + ybuf[1, z, target - cy]
                    elif target < 0:
                        beside = beside + ybuf[below_y, z, target + cy]
                    else:
                        beside = beside + zext[cz + z, target]
                beside = beside + pltpu.roll(jnp.where(lane < k, edge, centre), 128 - k, 1)
                beside = beside + pltpu.roll(jnp.where(lane >= 128 - k, edge, centre), k, 1)
                total = total - 0.5 * weight * beside
            hw_ref[cell] = total + nf[z, y]

    for copy in copies:
        copy.wait()
    for z in range(cz):
        for y in range(cy):
            cell = z * cy + y
            value = hw_ref[cell]
            if z < more_z:
                value = value + rz[z, y]
            if y < more_y:
                value = value + ry[z, y]
            if z < more_z and y < more_y:
                value = value + rzy[z, y]
            extra = None
            for begin, up_z, up_y, cells in spans:
                where = (z + cz * up_z, y + cy * up_y)
                if where in cells:
                    index = cells.index(where)
                    tile = rx[begin + index // 8]
                    shift = (128 - 16 * (index % 8)) % 128
                    tile = pltpu.roll(tile, shift, 1) if shift else tile
                    extra = tile if extra is None else extra + tile
            value = value + jnp.where(lane < 16, extra, 0.0)
            hw_ref[cell] = value
            split_store(HW, cell, value)

    outs[1].start()
    hw_row = products(HW, XX, HW + 1)
    second = jnp.where(lane < 96, hw_row, pltpu.roll(w_row2_pad(w_row2), 32, 1))
    sums2 = finish(reduced(1, paired(w_row, second)))
    weight = 1.0 / (own * cx * nz * ny * nx)
    sums1 = red1_ref[...]
    rows = jnp.concatenate([sums1, pltpu.roll(sums1, 112, 1), sums2, pltpu.roll(sums2, 112, 1)], 0)
    rows = rows * weight
    turned = jnp.transpose(jnp.concatenate([rows, jnp.zeros_like(rows)], 0))

    def direct(row, group, target):
        return rows[16 * row : 16 * row + 16, :], 32 * group, target

    def flipped(row, group, target):
        return turned[32 * group : 32 * group + 16, :], 16 * row, target

    def laid(parts):
        total = None
        for tile, begin, target in parts:
            shift = (16 * target - begin) % 128
            tile = pltpu.roll(tile, shift, 1) if shift else tile
            tile = jnp.where((lane >= 16 * target) & (lane < 16 * target + 16), tile, 0.0)
            total = tile if total is None else total + tile
        return total

    gram = [
        [direct(0, 2, 0), flipped(2, 2, 1), direct(0, 3, 2)],
        [direct(2, 2, 0), direct(3, 3, 1), direct(2, 3, 2)],
        [direct(1, 2, 0), flipped(2, 3, 1), direct(1, 3, 2)],
    ]
    rayleigh = [
        [flipped(0, 1, 0), flipped(3, 0, 1), direct(0, 0, 2)],
        [direct(2, 1, 0), flipped(3, 2, 1), direct(2, 0, 2)],
        [direct(1, 1, 0), flipped(3, 1, 1), direct(1, 0, 2)],
    ]
    for i in range(3):
        gram_ref[16 * i : 16 * i + 16, :] = laid(gram[i])[:, :48]
        ray_ref[16 * i : 16 * i + 16, :] = laid(rayleigh[i])[:, :48]
    for out in outs[2:]:
        out.start()
    for out in outs:
        out.wait()


def put_out(*refs):
    sems = refs[-1]
    half = len(refs) // 2
    copies = [
        pltpu.make_async_copy(source, target, sems.at[i])
        for i, (source, target) in enumerate(zip(refs[:half], refs[half : 2 * half]))
    ]
    for copy in copies:
        copy.start()
    for copy in copies:
        copy.wait()


def w_row2_pad(row):
    return jnp.concatenate([row, jnp.zeros((row.shape[0], 128 - row.shape[1]), row.dtype)], 1)


def per_device(
    sizes,
    block_x, block_hx, block_p, block_hp, potential, projectors, coupling,
    atom_count, proj_count, offsets, extents,
):
    cols, cz, cy, cx = block_x.shape
    slots, nproj = projectors.shape[-3], projectors.shape[-2]
    nz, ny, nx = sizes
    own = cz * cy
    fz, fy = cz + BZ - 1, cy + BY - 1
    turned = [
        jnp.transpose(b, (1, 2, 0, 3)).reshape(own, cols, cx)
        for b in (block_x, block_hx, block_p, block_hp)
    ]
    groups = (("gz", "gy"), ("gx",)) if nz * ny <= 16 else (("gz",), ("gy",), ("gx",))
    size_of = dict(zip(AXES, sizes))
    totals = []
    for group in groups:
        total = 1
        for a in group:
            total *= size_of[a]
        totals.append(total)
    tile = (cols, 128)
    more_z, more_y = fz - cz, fy - cy
    packed = sum(
        tiles_of(zc * yc) for zc in (cz, more_z) for yc in (cy, more_y)
    )
    per_slot = BZ * BY * nproj
    scratch = [
        pltpu.VMEM((cols, 128), F32),
        pltpu.VMEM((own,) + tile, F32),
        pltpu.VMEM((own,) + tile, F32),
        pltpu.VMEM((3 * cols, 3 * cols), F32),
        pltpu.VMEM((3 * cols, 3 * cols), F32),
        pltpu.VMEM((cols, cols, 128), F32),
        pltpu.VMEM((slots, nproj * nproj, 128), F32),
        pltpu.VMEM((nproj, nproj, slots), F32),
        pltpu.VMEM(potential.shape, F32),
        pltpu.VMEM(projectors.shape[3:], F32),
        pltpu.VMEM((192, own * 128), BF16),
        pltpu.VMEM((3 * cz, cy) + tile, F32),
        pltpu.VMEM((2, cz, cy) + tile, F32),
        pltpu.VMEM((BZ - 1, BY - 1) + tile, F32),
        pltpu.VMEM((tiles_of(own),) + tile, F32),
        pltpu.VMEM((tiles_of(own),) + tile, F32),
        pltpu.VMEM((4, tiles_of(own)) + tile, F32),
        pltpu.VMEM((tiles_of(own),) + tile, F32),
        pltpu.VMEM((fz * fy,) + tile, F32),
        pltpu.VMEM((fz * fy,) + tile, F32),
        pltpu.VMEM((own,) + tile, F32),
        pltpu.VMEM((slots * per_slot, 128), F32),
        pltpu.VMEM((slots * per_slot, 128), F32),
        pltpu.VMEM((slots * (BZ + 2) * (BY + 2), 2) + tile, F32),
        pltpu.VMEM((fz, fy) + tile, F32),
        pltpu.VMEM((fz, fy) + tile, F32),
        pltpu.VMEM((packed,) + tile, F32),
        pltpu.VMEM((more_z, cy) + tile, F32),
        pltpu.VMEM((cz, more_y) + tile, F32),
        pltpu.VMEM((more_z, more_y) + tile, F32),
        pltpu.VMEM((packed,) + tile, F32),
        pltpu.VMEM((8, 128), F32),
    ]
    scratch += [pltpu.VMEM((t, cols, 128), F32) for t in totals] * 2
    scratch += [pltpu.VMEM((t, 8, 128), F32) for t in totals]
    scratch += [
        pltpu.SemaphoreType.DMA((3 * sum(totals),)),
        pltpu.SemaphoreType.DMA((3 * sum(totals),)),
        pltpu.SemaphoreType.DMA((12,)),
        pltpu.SemaphoreType.DMA((12,)),
        pltpu.SemaphoreType.DMA((7,)),
        pltpu.SemaphoreType.DMA((7,)),
        pltpu.SemaphoreType.DMA((7,)),
        pltpu.SemaphoreType.DMA((4,)),
    ]
    scratch += [pltpu.VMEM((own,) + tile, F32)] * 4
    vmem = pl.BlockSpec(memory_space=pltpu.VMEM)
    smem = pl.BlockSpec(memory_space=pltpu.SMEM)
    w, hw, gram, rayleigh = pl.pallas_call(
        functools.partial(kernel, sizes, groups, (cz, cy, cx, slots, nproj, cols)),
        out_shape=(
            pltpu.VMEM((own,) + tile, F32),
            pltpu.VMEM((own,) + tile, F32),
            pltpu.VMEM((3 * cols, 3 * cols), F32),
            pltpu.VMEM((3 * cols, 3 * cols), F32),
        ),
        in_specs=[smem] * 4 + [pl.BlockSpec(memory_space=pltpu.HBM)] * 7,
        out_specs=(pl.BlockSpec(memory_space=pl.ANY),) * 4,
        scratch_shapes=scratch,
        compiler_params=pltpu.CompilerParams(
            collective_id=0, has_side_effects=True, vmem_limit_bytes=VMEM_LIMIT
        ),
    )(
        offsets, extents, atom_count, proj_count[0, 0],
        jnp.transpose(coupling[0, 0, 0], (1, 2, 0)),
        *turned, potential, projectors[0, 0, 0],
    )
    w, hw, gram, rayleigh = pl.pallas_call(
        put_out,
        out_shape=tuple(jax.ShapeDtypeStruct(b.shape, F32) for b in (w, hw, gram, rayleigh)),
        in_specs=[vmem] * 4,
        out_specs=(pl.BlockSpec(memory_space=pl.ANY),) * 4,
        scratch_shapes=[pltpu.SemaphoreType.DMA((4,))],
        compiler_params=pltpu.CompilerParams(vmem_limit_bytes=4 << 20),
    )(w, hw, gram, rayleigh)
    w, hw = (jnp.transpose(b.reshape(cz, cy, cols, cx), (2, 0, 1, 3)) for b in (w, hw))
    return (w, hw, gram, rayleigh)


def solution(mesh):
    sizes = tuple(mesh.shape[a] for a in AXES)
    in_specs = (
        P(None, "gz", "gy", "gx"),
        P(None, "gz", "gy", "gx"),
        P(None, "gz", "gy", "gx"),
        P(None, "gz", "gy", "gx"),
        P("gz", "gy", "gx"),
        P("gz", "gy", "gx", None, None, None),
        P("gz", "gy", "gx", None, None, None),
        P("gz", "gy", "gx"),
        P("gz", "gy", "gx", None),
        P(None, "gz", "gy", "gx", None),
        P(None, "gz", "gy", "gx", None),
    )
    out_specs = (P(None, "gz", "gy", "gx"), P(None, "gz", "gy", "gx"), P(), P())
    return jax.shard_map(
        functools.partial(per_device, sizes),
        mesh=mesh, in_specs=in_specs, out_specs=out_specs, check_vma=False,
    )
```

```python
import functools

import jax
import jax.numpy as jnp
from jax import lax
from jax.experimental import pallas as pl
from jax.experimental.pallas import tpu as pltpu
from jax.sharding import PartitionSpec as P

BZ, BY, BX = 4, 4, 16
LAP_CENTER = -5369.0 / 1800.0
LAP_COEFFS = (12.0 / 7.0, -15.0 / 56.0, 10.0 / 189.0, -1.0 / 112.0, 2.0 / 1925.0, -1.0 / 16632.0)
MESH = pl.DeviceIdType.MESH
VMEM_LIMIT = (63 << 20) - (64 << 10)
AXES = ("gz", "gy", "gx")
F32 = jnp.float32
BF16 = jnp.bfloat16
HP, HX, XX, PP, WW, HW = range(6)


def tiles_of(count):
    return -(-count // 8)


def solved(packed, cols, acol):
    shape = (8, 128)

    def spread(lane_at):
        return jnp.broadcast_to(packed[:, lane_at : lane_at + 1], shape)

    for j in range(cols):
        if j < 8:
            acol[j, 0:8] = spread(2 * cols + j)
        acol[j, 8:16] = spread(3 * cols + j)
    a = {}
    for j in range(cols):
        for i in range(j, cols):
            a[i, j] = jnp.broadcast_to(acol[j, i : i + 1, :], shape)
    scale = [lax.rsqrt(a[i, i]) for i in range(cols)]
    for i, j in a:
        a[i, j] = a[i, j] * scale[i] * scale[j]
    right = [
        [spread(half * cols + k) * scale[k] for half in range(2)] for k in range(cols)
    ]
    low = {}
    inverse = []
    for k in range(0, cols, 2):
        p, q, r = a[k, k], a[k + 1, k], a[k + 1, k + 1]
        det = 1.0 / (p * r - q * q)
        p, q, r = r * det, -q * det, p * det
        inverse.append((p, q, r))
        for i in range(k + 2, cols):
            low[i, k] = a[i, k] * p + a[i, k + 1] * q
            low[i, k + 1] = a[i, k] * q + a[i, k + 1] * r
            for j in range(k + 2, i + 1):
                a[i, j] = a[i, j] - (low[i, k] * a[j, k] + low[i, k + 1] * a[j, k + 1])
            right[i] = [
                right[i][h] - (low[i, k] * right[k][h] + low[i, k + 1] * right[k + 1][h])
                for h in range(2)
            ]
    out = [None] * cols
    for k in range(cols - 2, -1, -2):
        p, q, r = inverse[k // 2]
        halves = []
        for h in range(2):
            first = right[k][h] * p + right[k + 1][h] * q
            second = right[k][h] * q + right[k + 1][h] * r
            for i in range(cols - 1, k + 1, -1):
                first = first - low[i, k] * out[i][h]
                second = second - low[i, k + 1] * out[i][h]
            halves.append((first, second))
        out[k] = [halves[0][0], halves[1][0]]
        out[k + 1] = [halves[0][1], halves[1][1]]
    return [
        jnp.concatenate([out[k][0] * scale[k], out[k][1] * scale[k]], 0) for k in range(cols)
    ]


def kernel(
    sizes, groups, dims,
    off_ref, ext_ref, count_ref, proj_ref, d_in, x_in, hx_in, p_in, hp_in, v_in, beta_in,
    w_out, hw_out, gram_out, ray_out, red1_ref, w_ref, hw_ref, gram_ref, ray_ref,
    acol, d_ref, v_ref, beta_ref,
    stack, zext, ybuf, plow, phigh, xr, xl, edges, inner, nf,
    shared, offs, lines, bnear, bfar, parts4, parts_in,
    *rest,
):
    cz, cy, cx, slots, nproj, cols = dims
    nz, ny, nx = sizes
    n_red = len(groups)
    bufs = (rest[:n_red], rest[n_red : 2 * n_red], rest[2 * n_red : 3 * n_red])
    rest = rest[3 * n_red :]
    red_send, red_recv, halo_send, halo_recv, atom_send, atom_recv, part_sem = rest[:7]
    load_sem, out_sem, x_ref, hx_ref, p_ref, hp_ref = rest[7:]
    loads = []
    for i, (source, target) in enumerate(
        (
            (x_in, x_ref), (hx_in, hx_ref), (v_in, v_ref), (beta_in, beta_ref),
            (p_in, p_ref), (hp_in, hp_ref), (d_in, d_ref),
        )
    ):
        loads.append(pltpu.make_async_copy(source, target, load_sem.at[i]))
        loads[-1].start()
    zi, yi, xi = (lax.axis_index(a) for a in AXES)
    size_of = dict(zip(AXES, sizes))
    here = dict(zip(AXES, (zi, yi, xi)))
    more_z, more_y = BZ - 1, BY - 1
    own = cz * cy
    lane = lax.broadcasted_iota(jnp.int32, (cols, 128), 1)

    def neighbour(dz, dy, dx):
        step = dict(zip(AXES, (dz, dy, dx)))
        return {a: lax.rem(here[a] + step[a] + size_of[a], size_of[a]) for a in AXES}

    def member(group, offset):
        total = 1
        index = 0
        for a in group:
            total *= size_of[a]
            index = index * size_of[a] + here[a]
        target = lax.rem(index + offset, total)
        device = {}
        for a in reversed(group):
            device[a] = lax.rem(target, size_of[a])
            target = target // size_of[a]
        return {a: device.get(a, here[a]) for a in AXES}, index, total

    octant = [(o // 4, o // 2 % 2, o % 2) for o in range(8)]
    around = [
        (dz, dy, dx)
        for dx in (-1, 0, 1) for dz in (-1, 0, 1) for dy in (-1, 0, 1)
        if (dz, dy, dx) != (0, 0, 0)
    ]
    barrier = pltpu.get_barrier_semaphore()
    greeted = 0
    for group in groups:
        total = member(group, 0)[2]
        for offset in range(1, total):
            pl.semaphore_signal(
                barrier, inc=1, device_id=member(group, offset)[0], device_id_type=MESH
            )
            greeted += 1
    for where in around:
        pl.semaphore_signal(
            barrier, inc=1, device_id=neighbour(*where), device_id_type=MESH
        )
        greeted += 1

    def split_store(kind, cell, value):
        high = value.astype(BF16)
        low = (value - high.astype(F32)).astype(BF16)
        start = cell * 128 if isinstance(cell, int) else pl.multiple_of(cell * 128, 128)
        stack[kind * 32 : kind * 32 + 32, pl.ds(start, 128)] = jnp.concatenate([high, low], 0)

    def split_all(*kinds):
        @pl.loop(0, cz)
        def _(z):
            for y in range(cy):
                cell = z * cy + y
                for kind, ref in kinds:
                    split_store(kind, cell, ref[cell])

    for load in loads[:2]:
        load.wait()
    split_all((HX, hx_ref), (XX, x_ref))

    def products(left, right_from, right_to, count=1):
        m = lax.dot_general(
            stack[left * 32 : (left + count) * 32, :],
            stack[right_from * 32 : right_to * 32, :],
            (((1,), (1,)), ((), ())),
            preferred_element_type=F32,
        )
        parts = [m[32 * i : 32 * i + cols] + m[32 * i + cols : 32 * i + 32] for i in range(count)]
        return parts if count > 1 else parts[0]

    def reduced(which, payload):
        for phase, group in enumerate(groups):
            buf = bufs[which][phase]
            _, index, total = member(group, 0)
            send_sem, recv_sem = (sem.at[which * n_red + phase] for sem in (red_send, red_recv))
            buf[index] = payload
            if phase == 0 and which == 2:
                pl.semaphore_wait(barrier, greeted)
            for offset in range(1, total):
                pltpu.make_async_remote_copy(
                    src_ref=buf.at[index],
                    dst_ref=buf.at[index],
                    send_sem=send_sem,
                    recv_sem=recv_sem,
                    device_id=member(group, offset)[0],
                    device_id_type=MESH,
                ).start()
            yield None
            most = buf.at[pl.ds(0, total - 1)]
            for sem in (recv_sem, send_sem):
                pltpu.make_async_copy(most, most, sem).wait()
            payload = buf[0]
            for slot in range(1, total):
                payload = payload + buf[slot]
        yield payload

    def finish(steps):
        out = None
        for out in steps:
            pass
        return out

    both = lax.dot_general(
        stack[HX * 32 : XX * 32 + 32, :], stack[XX * 32 : XX * 32 + 32, :],
        (((1,), (1,)), ((), ())), preferred_element_type=F32,
    )
    both = jnp.concatenate([both, jnp.zeros((64, 96), F32)], 1)
    turn_hx = both[:cols] + both[cols:32]
    corr = both[32 : 32 + cols] + both[32 + cols :]
    narrow = lax.broadcasted_iota(jnp.int32, (8, 128), 1)

    def merged(tile):
        return tile + pltpu.roll(tile, 128 - cols, 1)

    payload0 = jnp.where(narrow < cols, merged(turn_hx[:8]), 0.0)
    for at, tile in ((1, turn_hx[8:]), (2, corr[:8]), (3, corr[8:])):
        moved = pltpu.roll(merged(tile), at * cols, 1)
        payload0 = jnp.where((narrow >= at * cols) & (narrow < at * cols + cols), moved, payload0)
    solving = reduced(2, payload0)
    next(solving)
    for load in loads[2:]:
        load.wait()
    rows = slots * nproj
    pairs = rows // 8
    box_lane = lax.broadcasted_iota(jnp.int32, (nproj, BZ * BY * BX), 1)
    box_row = lax.broadcasted_iota(jnp.int32, (nproj, BZ * BY * BX), 0)
    box_a, box_b, box_c = box_lane // (BY * BX), box_lane // BX % BY, box_lane % BX
    for s in range(slots):
        kept = jnp.where(s < count_ref[0, 0, 0], proj_ref[0, s], 0)
        inside = (
            (box_row < kept)
            & (box_a < ext_ref[0, 0, 0, 0, s])
            & (box_b < ext_ref[1, 0, 0, 0, s])
            & (box_c < ext_ref[2, 0, 0, 0, s])
        )
        at = s * nproj
        shared[0, at // 8, at % 8 : at % 8 + nproj, :] = jnp.where(inside, beta_ref[s], 0.0)
    lane1 = lax.broadcasted_iota(jnp.int32, (1, 128), 1)
    lane16 = lax.broadcasted_iota(jnp.int32, (nproj, 128), 1)
    slot_at = lane16 % 64 // 16 * (8 // nproj) + lane16 % 8 // nproj
    table = []
    for p in range(nproj):
        mirrored = jnp.concatenate([d_ref[q, p : p + 1, :] for q in range(nproj)], 0)
        sym = 0.5 * (d_ref[p] + mirrored)
        spread = jnp.zeros((nproj, 128), F32)
        for s in range(slots):
            value = jnp.broadcast_to(sym[:, s : s + 1], (nproj, 128))
            spread = jnp.where(slot_at == s, value, spread)
        table.append(spread)
    for d in range(-nproj + 1, nproj):
        row = jnp.zeros((1, 128), F32)
        for p in range(max(0, -d), min(nproj, nproj - d)):
            row = jnp.where(lane1 % nproj == p, table[p][p + d : p + d + 1, :], row)
        shared[0, pairs, d + nproj - 1 : d + nproj, 0:128] = row
    atom_copies = {}
    for o in (4, 2, 1, 6, 5, 3, 7):
        atom_copies[o] = [
            pltpu.make_async_remote_copy(
                src_ref=source,
                dst_ref=target,
                send_sem=atom_send.at[2 * (o - 1) + i],
                recv_sem=atom_recv.at[2 * (o - 1) + i],
                device_id=neighbour(*octant[o]),
                device_id_type=MESH,
            )
            for i, (source, target) in enumerate(
                ((off_ref, offs.at[o - 1]), (shared.at[0], shared.at[o]))
            )
        ]
        for copy in atom_copies[o]:
            copy.start()
    split_all((HP, hp_ref), (PP, p_ref))
    hx_row, x_row, p_row = products(HX, HP, WW, 3)
    first = jnp.where((lane >= 32) & (lane < 64), pltpu.roll(hx_row, 96, 1), x_row)

    def paired(upper, lower):
        upper = upper + pltpu.roll(upper, 112, 1)
        lower = lower + pltpu.roll(lower, 112, 1)
        return jnp.where(lane % 32 < 16, upper, pltpu.roll(lower, 16, 1))

    reduction = reduced(0, paired(first, p_row))

    lane8 = lax.broadcasted_iota(jnp.int32, (8, 128), 1)
    row8 = lax.broadcasted_iota(jnp.int32, (8, 128), 0)
    in_tile = 128 // BX
    width = BY + cy - 1
    ahead = cy - 1
    nothing = ahead + slots * BZ * width + ahead
    blank = jnp.zeros((16, 128), BF16)
    blank_line = jnp.zeros((8, 128), F32)

    @pl.loop(0, slots * BZ)
    def _(block):
        for b in range(BY, width):
            lines[ahead + block * width + b] = blank_line

    for at in [*range(ahead), *range(nothing - ahead, nothing + width)]:
        lines[at] = blank_line

    def build(o):
        dz, dy, dx = octant[o]

        def expand(pair):
            tiles = shared[o, pair]
            for half in range(8 // nproj):
                s = pair * (8 // nproj) + half
                ox = offset(2, s)
                along = (lane8 - ox + 128) & 127
                side = lane8 < ox if dx else lane8 >= ox
                keep = (along < BX) & side & (row8 // nproj == half)
                for k in range(in_tile):
                    shift = (ox + 128 - BX * k) & 127
                    for at in range(k, BZ * BY, in_tile):
                        part = tiles[:, at // in_tile * 128 : at // in_tile * 128 + 128]
                        part = jnp.where(keep, pltpu.roll(part, shift, 1), 0.0)
                        lines[ahead + (s * BZ + at // BY) * width + at % BY] = part

        def offset(axis, s):
            return off_ref[axis, 0, 0, 0, s] if o == 0 else offs[o - 1, axis, 0, 0, 0, s]

        for pair in range(pairs):
            expand(pair)

        target = bfar if dz else bnear
        top = o % 4 * 64
        ys = more_y if dy else cy

        @pl.loop(0, more_z if dz else cz)
        def _(z):
            starts = []
            for s in range(slots):
                a = z + dz * cz - offset(0, s)
                ok = (a >= 0) & (a < BZ)
                start = jnp.where(ok, ahead + (s * BZ + a) * width - offset(1, s), nothing - offset(1, s))
                starts.append(start)
            for y in range(cy):
                column = pl.ds(pl.multiple_of((z * cy + y) * 128, 128), 128)
                for pair in range(pairs):
                    at = top + pair * 16
                    if y >= ys:
                        target[at : at + 16, column] = blank
                        continue
                    total = None
                    for half in range(8 // nproj):
                        start = starts[pair * (8 // nproj) + half] + (y + dy * cy)
                        part = lines[start]
                        total = part if total is None else total + part
                    high = total.astype(BF16)
                    low = (total - high.astype(F32)).astype(BF16)
                    target[at : at + 16, column] = jnp.concatenate([high, low], 0)

    for z in range(cz):
        for y in range(cy):
            inner[z, y] = jnp.zeros((cols, 128), F32)
            inner[2 * cz + z, y] = jnp.zeros((cols, 128), F32)
    build(0)
    next(solving)
    next(reduction)
    for o in (4, 1, 2, 5, 6, 3, 7):
        for copy in atom_copies[o]:
            copy.wait()
        build(o)
    sums0 = finish(solving)
    next(reduction)
    sums0 = solved(sums0, cols, acol)
    theta_cols = sums0

    @pl.loop(0, cz)
    def _(z):
        for y in range(cy):
            cell = z * cy + y
            xs = x_ref[cell]
            value = hx_ref[cell]
            for k in range(cols):
                value = value - theta_cols[k] * xs[k : k + 1, :]
            vv = v_ref[z, y : y + 1, :]
            value = value * (1.0 / (1.0 + vv * vv))
            zext[cz + z, y] = value
            inner[cz + z, y] = value
            w_ref[cell] = value
            split_store(WW, cell, value)

    two_y = ny == 2
    split = cz // 2

    def some(ref, z, dz, y, dy):
        return ref.at[pl.ds(z, dz), pl.ds(y, dy)]

    def layers(target, base, z, dz, where):
        return some(zext, cz + z, dz, 0, cy), some(target, base + z, dz, 0, cy), where

    def bulk(z, dz):
        sends = [
            layers(zext, 2 * cz, z, dz, (-1, 0, 0)),
            layers(zext, 0, z, dz, (1, 0, 0)),
            layers(ybuf.at[1], 0, z, dz, (0, -1, 0)),
        ]
        if not two_y:
            sends.append(layers(ybuf.at[0], 0, z, dz, (0, 1, 0)))
        return sends

    early = bulk(0, split)
    late = bulk(split, cz - split)

    def launch(sends, send_sem, recv_sem, first=0):
        copies = []
        for i, (source, target, where) in enumerate(sends, start=first):
            copies.append(
                pltpu.make_async_remote_copy(
                    src_ref=source,
                    dst_ref=target,
                    send_sem=send_sem.at[i],
                    recv_sem=recv_sem.at[i],
                    device_id=neighbour(*where),
                    device_id_type=MESH,
                )
            )
            copies[-1].start()
        return copies

    copies = launch(early, halo_send, halo_recv)
    outs = [
        pltpu.make_async_copy(source, target, out_sem.at[i])
        for i, (source, target) in enumerate(
            ((w_ref, w_out), (hw_ref, hw_out), (gram_ref, gram_out), (ray_ref, ray_out))
        )
    ]
    outs[0].start()
    for q in range(tiles_of(own)):
        low = jnp.zeros((cols, 128), F32)
        high = low
        for j in range(min(8, own - 8 * q)):
            tile = zext[cz + (8 * q + j) // cy, (8 * q + j) % cy]
            keep = (lane >= 16 * j) & (lane < 16 * j + 16)
            low = jnp.where(keep, pltpu.roll(tile, 16 * j, 1) if j else tile, low)
            high = jnp.where(keep, pltpu.roll(tile, (16 * j + 16) % 128, 1) if j < 7 else tile, high)
        plow[q] = low
        phigh[q] = high

    x_copies = launch(
        [(plow, xr, (0, 0, -1)), (phigh, xl, (0, 0, 1))],
        halo_send, halo_recv, len(early) + len(late),
    )
    n_far = more_z * cy * 128

    def overlapped(values, table):
        m = lax.dot_general(
            values, table, (((1,), (1,)), ((), ())), preferred_element_type=F32
        )
        m = m[:cols] + m[cols:]
        return m + pltpu.roll(m, 256 - 8, 1)

    w_rows = stack.at[WW * 32 : WW * 32 + 32]
    for dz, tile in enumerate(
        (overlapped(w_rows[...], bnear[...]), overlapped(w_rows[:, :n_far], bfar[...]))
    ):
        for dy in range(2):
            upper, lower = tile[:8, dy * 128 : dy * 128 + 128], tile[8:, dy * 128 : dy * 128 + 128]
            parts4[dz, dy] = jnp.where(lane8 % 16 < 8, upper, pltpu.roll(lower, 8, 1))

    def span(step):
        return (max(0, -step), 2 - abs(step))

    slot_of = {}
    filled = 0
    for where in around:
        count = span(where[0])[1] * span(where[1])[1]
        slot_of[where] = filled
        filled += count
    part_copies = []
    for where in around:
        (z0, zn), (y0, yn) = span(where[0]), span(where[1])
        for z in range(z0, z0 + zn):
            at = slot_of[where] + (z - z0) * yn
            pltpu.make_async_remote_copy(
                src_ref=parts4.at[z, pl.ds(y0, yn)],
                dst_ref=parts_in.at[pl.ds(at, yn)],
                send_sem=part_sem.at[0],
                recv_sem=part_sem.at[1],
                device_id=neighbour(*where),
                device_id_type=MESH,
            ).start()
    late_copies = launch(late, halo_send, halo_recv, len(early))
    w_row = products(WW, HP, WW)
    w_row2 = products(WW, XX, HW)
    red1_ref[...] = finish(reduction)
    for copy in x_copies:
        copy.wait()
    for cell in range(own):
        left, right = xl[cell // 8], xr[cell // 8]
        turn = (112 - 16 * (cell % 8)) % 128
        left = pltpu.roll(left, turn, 1) if turn else left
        shift = (128 - 16 * (cell % 8)) % 128
        right = pltpu.roll(right, shift, 1) if shift else right
        edges[cell] = jnp.where(lane < 64, right, left)

    @pl.loop(0, cz)
    def _(z):
        for y in range(cy):
            cell = z * cy + y
            edge = edges[cell]
            centre = inner[cz + z, y]
            vv = v_ref[z, y : y + 1, :]
            total = centre * (vv - 1.5 * LAP_CENTER)
            for k, weight in enumerate(LAP_COEFFS, start=1):
                beside = pltpu.roll(jnp.where(lane < k, edge, centre), 128 - k, 1)
                beside = beside + pltpu.roll(jnp.where(lane >= 128 - k, edge, centre), k, 1)
                if k < cz:
                    beside = beside + (inner[cz + z + k, y] + inner[cz + z - k, y])
                for target in (y + k, y - k):
                    if 0 <= target < cy:
                        beside = beside + inner[cz + z, target]
                total = total - 0.5 * weight * beside
            hw_ref[cell] = total
    for sem in (part_sem.at[1], part_sem.at[0]):
        pltpu.make_async_copy(parts_in, parts_in, sem).wait()
    gathered = {}
    for dz in range(2):
        for dy in range(2):
            sums = {}
            for dx in (-1, 0, 1):
                total = None
                for from_z in range(2):
                    for from_y in range(2):
                        where = (dz - from_z, dy - from_y, dx)
                        if where == (0, 0, 0):
                            tile = parts4[dz, dy]
                        else:
                            (z0, _), (y0, yn) = span(where[0]), span(where[1])
                            tile = parts_in[slot_of[where] + (from_z - z0) * yn + from_y - y0]
                        total = tile if total is None else total + tile
                sums[dx] = total
            side = jnp.where(lane8 < 64, pltpu.roll(sums[-1], 64, 1), pltpu.roll(sums[1], 64, 1))
            gathered[dz, dy] = sums[0] + side
    lefts = []
    for dz in range(2):
        halves = []
        for dy in range(2):
            total = gathered[dz, dy]
            o = dz * 4 + dy * 2
            coefs = jnp.where(
                lane8 < 64, shared[o, pairs][:, :128], shared[o + 1, pairs][:, :128]
            )
            mixed = None
            for d in range(-nproj + 1, nproj):
                term = pltpu.roll(total, (128 - d) % 128, 1) if d else total
                term = term * coefs[d + nproj - 1 : d + nproj, :]
                mixed = term if mixed is None else mixed + term
            low_half = lane8 % 16 < 8
            mixed = jnp.concatenate(
                [
                    jnp.where(low_half, mixed, pltpu.roll(mixed, 8, 1)),
                    jnp.where(low_half, pltpu.roll(mixed, 120, 1), mixed),
                ],
                0,
            )
            high = mixed.astype(BF16)
            low = (mixed - high.astype(F32)).astype(BF16)
            halves.append(jnp.concatenate([high, low], 0))
        lefts.append(jnp.concatenate(halves, 1))

    def placed(left, table, z):
        m = lax.dot_general(
            left, table[:, z * cy * 128 : (z + 1) * cy * 128],
            (((1,), (0,)), ((), ())), preferred_element_type=F32,
        )
        return m[:cols] + m[cols:]

    for z in range(cz):
        total = placed(lefts[0], bnear, z)
        if z < more_z:
            total = total + placed(lefts[1], bfar, z)
        for y in range(cy):
            nf[z, y] = total[:, y * 128 : y * 128 + 128]
    for copy in copies + late_copies:
        copy.wait()
    for cell in range(own):
        z, y = cell // cy, cell % cy
        total = hw_ref[cell] + nf[z, y]
        weights = {}
        for k, weight in enumerate(LAP_COEFFS, start=1):
            keys = [("z", z + k), ("z", z - k), (1, y + k - cy), (1 if two_y else 0, y - k + cy)]
            for key, inside in zip(keys, (z + k < cz, z - k >= 0, y + k < cy, y - k >= 0)):
                if not inside:
                    weights[key] = weights.get(key, 0.0) - 0.5 * weight
        for (where, at), weight in weights.items():
            tile = zext[cz + at, y] if where == "z" else ybuf[where, z, at]
            total = total + weight * tile
        hw_ref[cell] = total
        split_store(HW, cell, total)
    outs[1].start()
    hw_row = products(HW, XX, HW + 1)
    second = jnp.where(lane < 96, hw_row, pltpu.roll(w_row2_pad(w_row2), 32, 1))
    sums2 = finish(reduced(1, paired(w_row, second)))
    weight = 1.0 / (own * cx * nz * ny * nx)
    sums1 = red1_ref[...]
    rows = jnp.concatenate([sums1, pltpu.roll(sums1, 112, 1), sums2, pltpu.roll(sums2, 112, 1)], 0)
    rows = rows * weight
    turned = jnp.transpose(jnp.concatenate([rows, jnp.zeros_like(rows)], 0))

    def direct(row, group, target):
        return rows[16 * row : 16 * row + 16, :], 32 * group, target

    def flipped(row, group, target):
        return turned[32 * group : 32 * group + 16, :], 16 * row, target

    def laid(parts):
        total = None
        for tile, begin, target in parts:
            shift = (16 * target - begin) % 128
            tile = pltpu.roll(tile, shift, 1) if shift else tile
            tile = jnp.where((lane >= 16 * target) & (lane < 16 * target + 16), tile, 0.0)
            total = tile if total is None else total + tile
        return total

    gram = [
        [direct(0, 2, 0), flipped(2, 2, 1), direct(0, 3, 2)],
        [direct(2, 2, 0), direct(3, 3, 1), direct(2, 3, 2)],
        [direct(1, 2, 0), flipped(2, 3, 1), direct(1, 3, 2)],
    ]
    rayleigh = [
        [flipped(0, 1, 0), flipped(3, 0, 1), direct(0, 0, 2)],
        [direct(2, 1, 0), flipped(3, 2, 1), direct(2, 0, 2)],
        [direct(1, 1, 0), flipped(3, 1, 1), direct(1, 0, 2)],
    ]
    for i in range(3):
        gram_ref[16 * i : 16 * i + 16, :] = laid(gram[i])[:, :48]
        ray_ref[16 * i : 16 * i + 16, :] = laid(rayleigh[i])[:, :48]
    for out in outs[2:]:
        out.start()
    for out in outs:
        out.wait()


def put_out(*refs):
    sems = refs[-1]
    half = len(refs) // 2
    copies = [
        pltpu.make_async_copy(source, target, sems.at[i])
        for i, (source, target) in enumerate(zip(refs[:half], refs[half : 2 * half]))
    ]
    for copy in copies:
        copy.start()
    for copy in copies:
        copy.wait()


def w_row2_pad(row):
    return jnp.concatenate([row, jnp.zeros((row.shape[0], 128 - row.shape[1]), row.dtype)], 1)


def per_device(
    sizes,
    block_x, block_hx, block_p, block_hp, potential, projectors, coupling,
    atom_count, proj_count, offsets, extents,
):
    cols, cz, cy, cx = block_x.shape
    slots, nproj = projectors.shape[-3], projectors.shape[-2]
    nz, ny, nx = sizes
    own = cz * cy
    turned = [
        jnp.transpose(b, (1, 2, 0, 3)).reshape(own, cols, cx)
        for b in (block_x, block_hx, block_p, block_hp)
    ]
    groups = (("gz", "gy"), ("gx",)) if nz * ny <= 16 else (("gz",), ("gy",), ("gx",))
    size_of = dict(zip(AXES, sizes))
    totals = []
    for group in groups:
        total = 1
        for a in group:
            total *= size_of[a]
        totals.append(total)
    tile = (cols, 128)
    rows = slots * nproj
    near, far = own * 128, (BZ - 1) * cy * 128
    scratch = [
        pltpu.VMEM((cols, 128), F32),
        pltpu.VMEM((own,) + tile, F32),
        pltpu.VMEM((own,) + tile, F32),
        pltpu.VMEM((3 * cols, 3 * cols), F32),
        pltpu.VMEM((3 * cols, 3 * cols), F32),
        pltpu.VMEM((cols, cols, 128), F32),
        pltpu.VMEM((nproj, nproj, slots), F32),
        pltpu.VMEM(potential.shape, F32),
        pltpu.VMEM(projectors.shape[3:], F32),
        pltpu.VMEM((192, own * 128), BF16),
        pltpu.VMEM((3 * cz, cy) + tile, F32),
        pltpu.VMEM((2, cz, cy) + tile, F32),
        pltpu.VMEM((tiles_of(own),) + tile, F32),
        pltpu.VMEM((tiles_of(own),) + tile, F32),
        pltpu.VMEM((tiles_of(own),) + tile, F32),
        pltpu.VMEM((tiles_of(own),) + tile, F32),
        pltpu.VMEM((own,) + tile, F32),
        pltpu.VMEM((3 * cz, cy) + tile, F32),
        pltpu.VMEM((cz, cy) + tile, F32),
        pltpu.VMEM((8, rows // 8 + 1, 8, BZ * BY * BX), F32),
        pltpu.SMEM((7,) + offsets.shape, jnp.int32),
        pltpu.VMEM((slots * BZ * (BY + cy - 1) + BY + 3 * (cy - 1), 8, 128), F32),
        pltpu.VMEM((256, near), BF16),
        pltpu.VMEM((256, far), BF16),
        pltpu.VMEM((2, 2, 8, 128), F32),
        pltpu.VMEM((44, 8, 128), F32),
    ]
    scratch += [pltpu.VMEM((t, cols, 128), F32) for t in totals] * 2
    scratch += [pltpu.VMEM((t, 8, 128), F32) for t in totals]
    scratch += [
        pltpu.SemaphoreType.DMA((3 * len(groups),)),
        pltpu.SemaphoreType.DMA((3 * len(groups),)),
        pltpu.SemaphoreType.DMA((10,)),
        pltpu.SemaphoreType.DMA((10,)),
        pltpu.SemaphoreType.DMA((14,)),
        pltpu.SemaphoreType.DMA((14,)),
        pltpu.SemaphoreType.DMA((2,)),
        pltpu.SemaphoreType.DMA((7,)),
        pltpu.SemaphoreType.DMA((4,)),
    ]
    scratch += [pltpu.VMEM((own,) + tile, F32)] * 4
    vmem = pl.BlockSpec(memory_space=pltpu.VMEM)
    smem = pl.BlockSpec(memory_space=pltpu.SMEM)
    w, hw, gram, rayleigh = pl.pallas_call(
        functools.partial(kernel, sizes, groups, (cz, cy, cx, slots, nproj, cols)),
        out_shape=(
            pltpu.VMEM((own,) + tile, F32),
            pltpu.VMEM((own,) + tile, F32),
            pltpu.VMEM((3 * cols, 3 * cols), F32),
            pltpu.VMEM((3 * cols, 3 * cols), F32),
        ),
        in_specs=[smem] * 4 + [pl.BlockSpec(memory_space=pltpu.HBM)] * 7,
        out_specs=(pl.BlockSpec(memory_space=pl.ANY),) * 4,
        scratch_shapes=scratch,
        compiler_params=pltpu.CompilerParams(
            collective_id=0, has_side_effects=True, vmem_limit_bytes=VMEM_LIMIT
        ),
    )(
        offsets, extents, atom_count, proj_count[0, 0],
        jnp.transpose(coupling[0, 0, 0], (1, 2, 0)),
        *turned, potential, projectors[0, 0, 0],
    )
    w, hw, gram, rayleigh = pl.pallas_call(
        put_out,
        out_shape=tuple(jax.ShapeDtypeStruct(b.shape, F32) for b in (w, hw, gram, rayleigh)),
        in_specs=[vmem] * 4,
        out_specs=(pl.BlockSpec(memory_space=pl.ANY),) * 4,
        scratch_shapes=[pltpu.SemaphoreType.DMA((4,))],
        compiler_params=pltpu.CompilerParams(vmem_limit_bytes=4 << 20),
    )(w, hw, gram, rayleigh)
    w, hw = (jnp.transpose(b.reshape(cz, cy, cols, cx), (2, 0, 1, 3)) for b in (w, hw))
    return (w, hw, gram, rayleigh)


def solution(mesh):
    sizes = tuple(mesh.shape[a] for a in AXES)
    in_specs = (
        P(None, "gz", "gy", "gx"),
        P(None, "gz", "gy", "gx"),
        P(None, "gz", "gy", "gx"),
        P(None, "gz", "gy", "gx"),
        P("gz", "gy", "gx"),
        P("gz", "gy", "gx", None, None, None),
        P("gz", "gy", "gx", None, None, None),
        P("gz", "gy", "gx"),
        P("gz", "gy", "gx", None),
        P(None, "gz", "gy", "gx", None),
        P(None, "gz", "gy", "gx", None),
    )
    out_specs = (P(None, "gz", "gy", "gx"), P(None, "gz", "gy", "gx"), P(), P())
    return jax.shard_map(
        functools.partial(per_device, sizes),
        mesh=mesh, in_specs=in_specs, out_specs=out_specs, check_vma=False,
    )
```

```python
import functools

import jax
import jax.numpy as jnp
from jax import lax
from jax.experimental import pallas as pl
from jax.experimental.pallas import tpu as pltpu
from jax.sharding import PartitionSpec as P

BZ, BY, BX = 4, 4, 16
LAP_CENTER = -5369.0 / 1800.0
LAP_COEFFS = (12.0 / 7.0, -15.0 / 56.0, 10.0 / 189.0, -1.0 / 112.0, 2.0 / 1925.0, -1.0 / 16632.0)
MESH = pl.DeviceIdType.MESH
VMEM_LIMIT = (63 << 20) - (64 << 10)
AXES = ("gz", "gy", "gx")
F32 = jnp.float32
BF16 = jnp.bfloat16
HP, HX, XX, PP, WW, HW = range(6)


def tiles_of(count):
    return -(-count // 8)


def solved(packed, cols, acol):
    shape = (8, 128)

    def spread(lane_at):
        return jnp.broadcast_to(packed[:, lane_at : lane_at + 1], shape)

    for j in range(cols):
        if j < 8:
            acol[j, 0:8] = spread(2 * cols + j)
        acol[j, 8:16] = spread(3 * cols + j)
    a = {}
    for j in range(cols):
        for i in range(j, cols):
            a[i, j] = jnp.broadcast_to(acol[j, i : i + 1, :], shape)
    scale = [lax.rsqrt(a[i, i]) for i in range(cols)]
    for i, j in a:
        a[i, j] = a[i, j] * scale[i] * scale[j]
    right = [
        [spread(half * cols + k) * scale[k] for half in range(2)] for k in range(cols)
    ]
    low = {}
    inverse = []
    for k in range(0, cols, 2):
        p, q, r = a[k, k], a[k + 1, k], a[k + 1, k + 1]
        det = 1.0 / (p * r - q * q)
        p, q, r = r * det, -q * det, p * det
        inverse.append((p, q, r))
        for i in range(k + 2, cols):
            low[i, k] = a[i, k] * p + a[i, k + 1] * q
            low[i, k + 1] = a[i, k] * q + a[i, k + 1] * r
            for j in range(k + 2, i + 1):
                a[i, j] = a[i, j] - (low[i, k] * a[j, k] + low[i, k + 1] * a[j, k + 1])
            right[i] = [
                right[i][h] - (low[i, k] * right[k][h] + low[i, k + 1] * right[k + 1][h])
                for h in range(2)
            ]
    out = [None] * cols
    for k in range(cols - 2, -1, -2):
        p, q, r = inverse[k // 2]
        halves = []
        for h in range(2):
            first = right[k][h] * p + right[k + 1][h] * q
            second = right[k][h] * q + right[k + 1][h] * r
            for i in range(cols - 1, k + 1, -1):
                first = first - low[i, k] * out[i][h]
                second = second - low[i, k + 1] * out[i][h]
            halves.append((first, second))
        out[k] = [halves[0][0], halves[1][0]]
        out[k + 1] = [halves[0][1], halves[1][1]]
    return [
        jnp.concatenate([out[k][0] * scale[k], out[k][1] * scale[k]], 0) for k in range(cols)
    ]


def kernel(
    sizes, groups, dims,
    off_in, ext_in, count_in, proj_in, d_in, x_in, hx_in, p_in, hp_in, v_in, beta_in,
    w_out, hw_out, sums_out, red1_ref, w_ref, hw_ref, sums_ref,
    off_ref, ext_ref, count_ref, proj_ref, acol, d_ref, v_ref, beta_ref,
    stack, zext, ybuf, plow, phigh, xr, xl, edges, inner, nf,
    shared, offs, lines, bnear, bfar, parts4, parts_in,
    *rest,
):
    cz, cy, cx, slots, nproj, cols = dims
    nz, ny, nx = sizes
    n_red = len(groups)
    bufs = (rest[:n_red], rest[n_red : 2 * n_red], rest[2 * n_red : 3 * n_red])
    rest = rest[3 * n_red :]
    red_send, red_recv, halo_send, halo_recv, atom_send, atom_recv, part_sem = rest[:7]
    load_sem, out_sem, xh, p_ref, hp_ref, raw, raw_v, raw_send, raw_recv = rest[7:]
    x_ref, hx_ref = xh.at[0], xh.at[1]
    loads = []
    for i, (source, target) in enumerate(
        (
            (x_in, x_ref), (hx_in, hx_ref), (off_in, off_ref), (ext_in, ext_ref),
            (count_in, count_ref), (proj_in, proj_ref), (v_in, v_ref), (beta_in, beta_ref),
            (p_in, p_ref), (hp_in, hp_ref), (d_in, d_ref),
        )
    ):
        loads.append(pltpu.make_async_copy(source, target, load_sem.at[i]))
        loads[-1].start()
    zi, yi, xi = (lax.axis_index(a) for a in AXES)
    size_of = dict(zip(AXES, sizes))
    here = dict(zip(AXES, (zi, yi, xi)))
    more_z, more_y = BZ - 1, BY - 1
    own = cz * cy
    lane = lax.broadcasted_iota(jnp.int32, (cols, 128), 1)

    def neighbour(dz, dy, dx):
        step = dict(zip(AXES, (dz, dy, dx)))
        return {a: lax.rem(here[a] + step[a] + size_of[a], size_of[a]) for a in AXES}

    def member(group, offset):
        total = 1
        index = 0
        for a in group:
            total *= size_of[a]
            index = index * size_of[a] + here[a]
        target = lax.rem(index + offset, total)
        device = {}
        for a in reversed(group):
            device[a] = lax.rem(target, size_of[a])
            target = target // size_of[a]
        return {a: device.get(a, here[a]) for a in AXES}, index, total

    octant = [(o // 4, o // 2 % 2, o % 2) for o in range(8)]
    around = [
        (dz, dy, dx)
        for dx in (-1, 0, 1) for dz in (-1, 0, 1) for dy in (-1, 0, 1)
        if (dz, dy, dx) != (0, 0, 0)
    ]
    barrier = pltpu.get_barrier_semaphore()
    greeted = 0
    for group in groups:
        total = member(group, 0)[2]
        for offset in range(1, total):
            pl.semaphore_signal(
                barrier, inc=1, device_id=member(group, offset)[0], device_id_type=MESH
            )
            greeted += 1
    for where in around:
        pl.semaphore_signal(
            barrier, inc=1, device_id=neighbour(*where), device_id_type=MESH
        )
        greeted += 1

    def split_store(kind, cell, value):
        high = value.astype(BF16)
        low = (value - high.astype(F32)).astype(BF16)
        start = cell * 128 if isinstance(cell, int) else pl.multiple_of(cell * 128, 128)
        stack[kind * 32 : kind * 32 + 32, pl.ds(start, 128)] = jnp.concatenate([high, low], 0)

    def split_all(*kinds):
        @pl.loop(0, cz)
        def _(z):
            for y in range(cy):
                cell = z * cy + y
                for kind, ref in kinds:
                    split_store(kind, cell, ref[cell])

    for load in loads[:2]:
        load.wait()
    split_all((HX, hx_ref), (XX, x_ref))

    def products(left, right_from, right_to, count=1):
        m = lax.dot_general(
            stack[left * 32 : (left + count) * 32, :],
            stack[right_from * 32 : right_to * 32, :],
            (((1,), (1,)), ((), ())),
            preferred_element_type=F32,
        )
        parts = [m[32 * i : 32 * i + cols] + m[32 * i + cols : 32 * i + 32] for i in range(count)]
        return parts if count > 1 else parts[0]

    def reduced(which, payload):
        for phase, group in enumerate(groups):
            buf = bufs[which][phase]
            _, index, total = member(group, 0)
            send_sem, recv_sem = (sem.at[which * n_red + phase] for sem in (red_send, red_recv))
            buf[index] = payload
            if phase == 0 and which == 2:
                pl.semaphore_wait(barrier, greeted)
            for offset in range(1, total):
                pltpu.make_async_remote_copy(
                    src_ref=buf.at[index],
                    dst_ref=buf.at[index],
                    send_sem=send_sem,
                    recv_sem=recv_sem,
                    device_id=member(group, offset)[0],
                    device_id_type=MESH,
                ).start()
            yield None
            most = buf.at[pl.ds(0, total - 1)]
            for sem in (recv_sem, send_sem):
                pltpu.make_async_copy(most, most, sem).wait()
            payload = buf[0]
            for slot in range(1, total):
                payload = payload + buf[slot]
        yield payload

    def finish(steps):
        out = None
        for out in steps:
            pass
        return out

    both = lax.dot_general(
        stack[HX * 32 : XX * 32 + 32, :], stack[XX * 32 : XX * 32 + 32, :],
        (((1,), (1,)), ((), ())), preferred_element_type=F32,
    )
    both = jnp.concatenate([both, jnp.zeros((64, 96), F32)], 1)
    turn_hx = both[:cols] + both[cols:32]
    corr = both[32 : 32 + cols] + both[32 + cols :]
    narrow = lax.broadcasted_iota(jnp.int32, (8, 128), 1)

    def merged(tile):
        return tile + pltpu.roll(tile, 128 - cols, 1)

    payload0 = jnp.where(narrow < cols, merged(turn_hx[:8]), 0.0)
    for at, tile in ((1, turn_hx[8:]), (2, corr[:8]), (3, corr[8:])):
        moved = pltpu.roll(merged(tile), at * cols, 1)
        payload0 = jnp.where((narrow >= at * cols) & (narrow < at * cols + cols), moved, payload0)
    solving = reduced(2, payload0)
    next(solving)
    for load in loads[2:]:
        load.wait()
    rows = slots * nproj
    pairs = rows // 8
    columns = BZ * BY * BX // 128
    box_lane = lax.broadcasted_iota(jnp.int32, (nproj, BZ * BY * BX), 1)
    box_row = lax.broadcasted_iota(jnp.int32, (nproj, BZ * BY * BX), 0)
    box_a, box_b, box_c = box_lane // (BY * BX), box_lane // BX % BY, box_lane % BX
    for s in range(slots):
        kept = jnp.where(s < count_ref[0, 0, 0], proj_ref[0, s], 0)
        inside = (
            (box_row < kept)
            & (box_a < ext_ref[0, 0, 0, 0, s])
            & (box_b < ext_ref[1, 0, 0, 0, s])
            & (box_c < ext_ref[2, 0, 0, 0, s])
        )
        at = s * nproj
        kept = jnp.where(inside, beta_ref[s], 0.0)
        for c in range(columns):
            where = (0, at // 8 * columns + c, slice(at % 8, at % 8 + nproj), slice(None))
            shared[where] = kept[:, c * 128 : c * 128 + 128]
    lane1 = lax.broadcasted_iota(jnp.int32, (1, 128), 1)
    lane16 = lax.broadcasted_iota(jnp.int32, (nproj, 128), 1)
    slot_at = lane16 % 64 // 16 * (8 // nproj) + lane16 % 8 // nproj
    table = []
    for p in range(nproj):
        mirrored = jnp.concatenate([d_ref[q, p : p + 1, :] for q in range(nproj)], 0)
        sym = 0.5 * (d_ref[p] + mirrored)
        spread = jnp.zeros((nproj, 128), F32)
        for s in range(slots):
            value = jnp.broadcast_to(sym[:, s : s + 1], (nproj, 128))
            spread = jnp.where(slot_at == s, value, spread)
        table.append(spread)
    for d in range(-nproj + 1, nproj):
        row = jnp.zeros((1, 128), F32)
        for p in range(max(0, -d), min(nproj, nproj - d)):
            row = jnp.where(lane1 % nproj == p, table[p][p + d : p + d + 1, :], row)
        shared[0, pairs * columns, d + nproj - 1 : d + nproj, :] = row
    atom_copies = {}
    for o in (4, 2, 1, 6, 5, 3, 7):
        atom_copies[o] = [
            pltpu.make_async_remote_copy(
                src_ref=source,
                dst_ref=target,
                send_sem=atom_send.at[2 * (o - 1) + i],
                recv_sem=atom_recv.at[2 * (o - 1) + i],
                device_id=neighbour(*octant[o]),
                device_id_type=MESH,
            )
            for i, (source, target) in enumerate(
                ((off_ref, offs.at[o - 1]), (shared.at[0], shared.at[o]))
            )
        ]
        for copy in atom_copies[o]:
            copy.start()
    split_all((HP, hp_ref), (PP, p_ref))
    hx_row, x_row, p_row = products(HX, HP, WW, 3)
    first = jnp.where((lane >= 32) & (lane < 64), pltpu.roll(hx_row, 96, 1), x_row)

    def paired(upper, lower):
        upper = upper + pltpu.roll(upper, 112, 1)
        lower = lower + pltpu.roll(lower, 112, 1)
        return jnp.where(lane % 32 < 16, upper, pltpu.roll(lower, 16, 1))

    reduction = reduced(0, paired(first, p_row))

    lane8 = lax.broadcasted_iota(jnp.int32, (8, 128), 1)
    row8 = lax.broadcasted_iota(jnp.int32, (8, 128), 0)
    in_tile = 128 // BX
    width = BY + cy - 1
    ahead = cy - 1
    nothing = ahead + slots * BZ * width + ahead
    blank = jnp.zeros((16, 128), BF16)
    blank_line = jnp.zeros((8, 128), F32)

    @pl.loop(0, slots * BZ)
    def _(block):
        for b in range(BY, width):
            lines[ahead + block * width + b] = blank_line

    for at in [*range(ahead), *range(nothing - ahead, nothing + width)]:
        lines[at] = blank_line

    def build(o):
        dz, dy, dx = octant[o]

        def expand(pair):
            tiles = [shared[o, pair * columns + c] for c in range(columns)]
            for half in range(8 // nproj):
                s = pair * (8 // nproj) + half
                ox = offset(2, s)
                along = (lane8 - ox + 128) & 127
                side = lane8 < ox if dx else lane8 >= ox
                keep = (along < BX) & side & (row8 // nproj == half)
                for k in range(in_tile):
                    shift = (ox + 128 - BX * k) & 127
                    for at in range(k, BZ * BY, in_tile):
                        part = jnp.where(keep, pltpu.roll(tiles[at // in_tile], shift, 1), 0.0)
                        lines[ahead + (s * BZ + at // BY) * width + at % BY] = part

        def offset(axis, s):
            return off_ref[axis, 0, 0, 0, s] if o == 0 else offs[o - 1, axis, 0, 0, 0, s]

        for pair in range(pairs):
            expand(pair)

        target = bfar if dz else bnear
        top = o % 4 * 64
        ys = more_y if dy else cy

        @pl.loop(0, more_z if dz else cz)
        def _(z):
            starts = []
            for s in range(slots):
                a = z + dz * cz - offset(0, s)
                ok = (a >= 0) & (a < BZ)
                start = jnp.where(ok, ahead + (s * BZ + a) * width - offset(1, s), nothing - offset(1, s))
                starts.append(start)
            for y in range(cy):
                column = pl.ds(pl.multiple_of((z * cy + y) * 128, 128), 128)
                for pair in range(pairs):
                    at = top + pair * 16
                    if y >= ys:
                        target[at : at + 16, column] = blank
                        continue
                    total = None
                    for half in range(8 // nproj):
                        start = starts[pair * (8 // nproj) + half] + (y + dy * cy)
                        part = lines[start]
                        total = part if total is None else total + part
                    high = total.astype(BF16)
                    low = (total - high.astype(F32)).astype(BF16)
                    target[at : at + 16, column] = jnp.concatenate([high, low], 0)

    for z in range(cz):
        for y in range(cy):
            inner[z, y] = jnp.zeros((cols, 128), F32)
            inner[2 * cz + z, y] = jnp.zeros((cols, 128), F32)
    build(0)
    next(solving)
    next(reduction)
    early_z = cz // 3
    early_to = [(-1, 0, 0), (1, 0, 0), (0, -1, 0)] + ([] if ny == 2 else [(0, 1, 0)])
    raw_copies = []
    for d, where in enumerate(early_to):
        for i, (source, target) in enumerate(
            (
                (xh.at[:, pl.ds(0, early_z * cy)], raw.at[d]),
                (v_ref.at[pl.ds(0, early_z)], raw_v.at[d]),
            )
        ):
            raw_copies.append(
                pltpu.make_async_remote_copy(
                    src_ref=source,
                    dst_ref=target,
                    send_sem=raw_send.at[2 * d + i],
                    recv_sem=raw_recv.at[2 * d + i],
                    device_id=neighbour(*where),
                    device_id_type=MESH,
                )
            )
            raw_copies[-1].start()
    for o in (4, 1, 2, 5, 6, 3, 7):
        for copy in atom_copies[o]:
            copy.wait()
        build(o)
    sums0 = finish(solving)
    next(reduction)
    sums0 = solved(sums0, cols, acol)
    theta_cols = sums0

    @pl.loop(0, cz)
    def _(z):
        for y in range(cy):
            cell = z * cy + y
            xs = x_ref[cell]
            value = hx_ref[cell]
            for k in range(cols):
                value = value - theta_cols[k] * xs[k : k + 1, :]
            vv = v_ref[z, y : y + 1, :]
            value = value * (1.0 / (1.0 + vv * vv))
            zext[cz + z, y] = value
            inner[cz + z, y] = value
            w_ref[cell] = value
            split_store(WW, cell, value)

    two_y = ny == 2
    split = early_z + (cz - early_z) // 2

    def some(ref, z, dz, y, dy):
        return ref.at[pl.ds(z, dz), pl.ds(y, dy)]

    def layers(target, base, z, dz, where):
        return some(zext, cz + z, dz, 0, cy), some(target, base + z, dz, 0, cy), where

    def bulk(z, dz):
        sends = [
            layers(zext, 2 * cz, z, dz, (-1, 0, 0)),
            layers(zext, 0, z, dz, (1, 0, 0)),
            layers(ybuf.at[1], 0, z, dz, (0, -1, 0)),
        ]
        if not two_y:
            sends.append(layers(ybuf.at[0], 0, z, dz, (0, 1, 0)))
        return sends

    early = bulk(early_z, split - early_z)
    late = bulk(split, cz - split)

    def launch(sends, send_sem, recv_sem, first=0):
        copies = []
        for i, (source, target, where) in enumerate(sends, start=first):
            copies.append(
                pltpu.make_async_remote_copy(
                    src_ref=source,
                    dst_ref=target,
                    send_sem=send_sem.at[i],
                    recv_sem=recv_sem.at[i],
                    device_id=neighbour(*where),
                    device_id_type=MESH,
                )
            )
            copies[-1].start()
        return copies

    copies = launch(early, halo_send, halo_recv)
    outs = [
        pltpu.make_async_copy(source, target, out_sem.at[i])
        for i, (source, target) in enumerate(
            ((w_ref, w_out), (hw_ref, hw_out), (sums_ref, sums_out))
        )
    ]
    outs[0].start()
    for q in range(tiles_of(own)):
        low = jnp.zeros((cols, 128), F32)
        high = low
        for j in range(min(8, own - 8 * q)):
            tile = zext[cz + (8 * q + j) // cy, (8 * q + j) % cy]
            keep = (lane >= 16 * j) & (lane < 16 * j + 16)
            low = jnp.where(keep, pltpu.roll(tile, 16 * j, 1) if j else tile, low)
            high = jnp.where(keep, pltpu.roll(tile, (16 * j + 16) % 128, 1) if j < 7 else tile, high)
        plow[q] = low
        phigh[q] = high

    x_copies = launch(
        [(plow, xr, (0, 0, -1)), (phigh, xl, (0, 0, 1))],
        halo_send, halo_recv, len(early) + len(late),
    )
    n_far = more_z * cy * 128

    def overlapped(values, table):
        m = lax.dot_general(
            values, table, (((1,), (1,)), ((), ())), preferred_element_type=F32
        )
        m = m[:cols] + m[cols:]
        return m + pltpu.roll(m, 256 - 8, 1)

    lane4 = lax.broadcasted_iota(jnp.int32, (4, 128), 1)
    w_rows = stack.at[WW * 32 : WW * 32 + 32]
    for dz, tile in enumerate(
        (overlapped(w_rows[...], bnear[...]), overlapped(w_rows[:, :n_far], bfar[...]))
    ):
        for dy in range(2):
            upper, lower = tile[:8, dy * 128 : dy * 128 + 128], tile[8:, dy * 128 : dy * 128 + 128]
            both = jnp.where(lane8 % 16 < 8, upper, pltpu.roll(lower, 8, 1))
            moved = pltpu.roll(both, 64, 1)
            parts4[dz, dy, 0] = jnp.where(lane4 < 64, both[:4], moved[4:])
            parts4[dz, dy, 1] = jnp.where(lane4 < 64, moved[:4], both[4:])

    def span(step):
        return (max(0, -step), 2 - abs(step))

    slot_of = {}
    filled = 0
    for where in around:
        slot_of[where] = filled
        filled += span(where[0])[1] * span(where[1])[1] * span(where[2])[1]
    for where in around:
        (z0, zn), (y0, yn), (x0, xn) = (span(step) for step in where)
        for z in range(z0, z0 + zn):
            for y in range(y0, y0 + yn):
                at = slot_of[where] + ((z - z0) * yn + y - y0) * xn
                pltpu.make_async_remote_copy(
                    src_ref=parts4.at[z, y, pl.ds(x0, xn)],
                    dst_ref=parts_in.at[pl.ds(at, xn)],
                    send_sem=part_sem.at[0],
                    recv_sem=part_sem.at[1],
                    device_id=neighbour(*where),
                    device_id_type=MESH,
                ).start()
    late_copies = launch(late, halo_send, halo_recv, len(early))
    w_row = products(WW, HP, WW)
    w_row2 = products(WW, XX, HW)
    red1_ref[...] = finish(reduction)
    for copy in raw_copies:
        copy.wait()
    for d in range(len(early_to)):
        target, base = ((zext, 2 * cz), (zext, 0), (ybuf.at[1], 0), (ybuf.at[0], 0))[d]

        @pl.loop(0, early_z)
        def _(z):
            for y in range(cy):
                cell = z * cy + y
                xs = raw[d, 0, cell]
                value = raw[d, 1, cell]
                for k in range(cols):
                    value = value - theta_cols[k] * xs[k : k + 1, :]
                vv = raw_v[d, z, y : y + 1, :]
                target[base + z, y] = value * (1.0 / (1.0 + vv * vv))

    for copy in x_copies:
        copy.wait()
    for cell in range(own):
        left, right = xl[cell // 8], xr[cell // 8]
        turn = (112 - 16 * (cell % 8)) % 128
        left = pltpu.roll(left, turn, 1) if turn else left
        shift = (128 - 16 * (cell % 8)) % 128
        right = pltpu.roll(right, shift, 1) if shift else right
        edges[cell] = jnp.where(lane < 64, right, left)

    @pl.loop(0, cz)
    def _(z):
        for y in range(cy):
            cell = z * cy + y
            edge = edges[cell]
            centre = inner[cz + z, y]
            vv = v_ref[z, y : y + 1, :]
            total = centre * (vv - 1.5 * LAP_CENTER)
            for k, weight in enumerate(LAP_COEFFS, start=1):
                beside = pltpu.roll(jnp.where(lane < k, edge, centre), 128 - k, 1)
                beside = beside + pltpu.roll(jnp.where(lane >= 128 - k, edge, centre), k, 1)
                if k < cz:
                    beside = beside + (inner[cz + z + k, y] + inner[cz + z - k, y])
                for target in (y + k, y - k):
                    if 0 <= target < cy:
                        beside = beside + inner[cz + z, target]
                total = total - 0.5 * weight * beside
            hw_ref[cell] = total
    for sem in (part_sem.at[1], part_sem.at[0]):
        pltpu.make_async_copy(parts_in, parts_in, sem).wait()
    gathered = {}
    for dz in range(2):
        for dy in range(2):
            sums = []
            for dx in range(2):
                total = None
                for from_z in range(2):
                    for from_y in range(2):
                        for from_x in range(2):
                            where = (dz - from_z, dy - from_y, dx - from_x)
                            if where == (0, 0, 0):
                                tile = parts4[dz, dy, dx]
                            else:
                                (z0, _), (y0, yn), (x0, xn) = (span(step) for step in where)
                                at = ((from_z - z0) * yn + from_y - y0) * xn + from_x - x0
                                tile = parts_in[slot_of[where] + at]
                            total = tile if total is None else total + tile
                sums.append(total)
            turned = [pltpu.roll(total, 64, 1) for total in sums]
            gathered[dz, dy] = jnp.concatenate(
                [
                    jnp.where(lane4 < 64, sums[0], turned[1]),
                    jnp.where(lane4 < 64, turned[0], sums[1]),
                ],
                0,
            )
    lefts = []
    for dz in range(2):
        halves = []
        for dy in range(2):
            total = gathered[dz, dy]
            o = dz * 4 + dy * 2
            coefs = jnp.where(
                lane8 < 64, shared[o, pairs * columns], shared[o + 1, pairs * columns]
            )
            mixed = None
            for d in range(-nproj + 1, nproj):
                term = pltpu.roll(total, (128 - d) % 128, 1) if d else total
                term = term * coefs[d + nproj - 1 : d + nproj, :]
                mixed = term if mixed is None else mixed + term
            low_half = lane8 % 16 < 8
            mixed = jnp.concatenate(
                [
                    jnp.where(low_half, mixed, pltpu.roll(mixed, 8, 1)),
                    jnp.where(low_half, pltpu.roll(mixed, 120, 1), mixed),
                ],
                0,
            )
            high = mixed.astype(BF16)
            low = (mixed - high.astype(F32)).astype(BF16)
            halves.append(jnp.concatenate([high, low], 0))
        lefts.append(jnp.concatenate(halves, 1))

    def placed(left, table, z):
        m = lax.dot_general(
            left, table[:, z * cy * 128 : (z + 1) * cy * 128],
            (((1,), (0,)), ((), ())), preferred_element_type=F32,
        )
        return m[:cols] + m[cols:]

    for z in range(cz):
        total = placed(lefts[0], bnear, z)
        if z < more_z:
            total = total + placed(lefts[1], bfar, z)
        for y in range(cy):
            nf[z, y] = total[:, y * 128 : y * 128 + 128]
    for copy in copies + late_copies:
        copy.wait()
    hw_sum = None
    for cell in range(own):
        z, y = cell // cy, cell % cy
        total = hw_ref[cell] + nf[z, y]
        weights = {}
        for k, weight in enumerate(LAP_COEFFS, start=1):
            keys = [("z", z + k), ("z", z - k), (1, y + k - cy), (1 if two_y else 0, y - k + cy)]
            for key, inside in zip(keys, (z + k < cz, z - k >= 0, y + k < cy, y - k >= 0)):
                if not inside:
                    weights[key] = weights.get(key, 0.0) - 0.5 * weight
        for (where, at), weight in weights.items():
            tile = zext[cz + at, y] if where == "z" else ybuf[where, z, at]
            total = total + weight * tile
        hw_ref[cell] = total
        split_store(HW, cell, total)
        if y == cy - 1:
            plane = slice(z * cy * 128, (z + 1) * cy * 128)
            part = lax.dot_general(
                stack[HW * 32 : HW * 32 + 32, plane], stack[XX * 32 : HW * 32, plane],
                (((1,), (1,)), ((), ())), preferred_element_type=F32,
            )
            hw_sum = part if hw_sum is None else hw_sum + part
    outs[1].start()
    hw_row = w_row2_pad(hw_sum[:cols] + hw_sum[cols:])
    second = jnp.where(lane < 96, hw_row, pltpu.roll(w_row2_pad(w_row2), 32, 1))
    sums2 = finish(reduced(1, paired(w_row, second)))
    sums_ref[...] = jnp.concatenate([red1_ref[...], sums2], 0)
    outs[2].start()
    for out in outs:
        out.wait()


def finish_out(weight, w_ref, hw_ref, sums_ref, w_out, hw_out, gram_out, ray_out, gram_ref, ray_ref, sems):
    copies = [
        pltpu.make_async_copy(source, target, sems.at[i])
        for i, (source, target) in enumerate(
            ((w_ref, w_out), (hw_ref, hw_out), (gram_ref, gram_out), (ray_ref, ray_out))
        )
    ]
    for copy in copies[:2]:
        copy.start()
    sums1, sums2 = sums_ref[:16], sums_ref[16:]
    lane = lax.broadcasted_iota(jnp.int32, (16, 128), 1)
    rows = jnp.concatenate([sums1, pltpu.roll(sums1, 112, 1), sums2, pltpu.roll(sums2, 112, 1)], 0)
    rows = rows * weight
    turned = jnp.transpose(jnp.concatenate([rows, jnp.zeros_like(rows)], 0))

    def direct(row, group, target):
        return rows[16 * row : 16 * row + 16, :], 32 * group, target

    def flipped(row, group, target):
        return turned[32 * group : 32 * group + 16, :], 16 * row, target

    def laid(parts):
        total = None
        for tile, begin, target in parts:
            shift = (16 * target - begin) % 128
            tile = pltpu.roll(tile, shift, 1) if shift else tile
            tile = jnp.where((lane >= 16 * target) & (lane < 16 * target + 16), tile, 0.0)
            total = tile if total is None else total + tile
        return total

    gram = [
        [direct(0, 2, 0), flipped(2, 2, 1), direct(0, 3, 2)],
        [direct(2, 2, 0), direct(3, 3, 1), direct(2, 3, 2)],
        [direct(1, 2, 0), flipped(2, 3, 1), direct(1, 3, 2)],
    ]
    rayleigh = [
        [flipped(0, 1, 0), flipped(3, 0, 1), direct(0, 0, 2)],
        [direct(2, 1, 0), flipped(3, 2, 1), direct(2, 0, 2)],
        [direct(1, 1, 0), flipped(3, 1, 1), direct(1, 0, 2)],
    ]
    for i in range(3):
        gram_ref[16 * i : 16 * i + 16, :] = laid(gram[i])[:, :48]
        ray_ref[16 * i : 16 * i + 16, :] = laid(rayleigh[i])[:, :48]
    for copy in copies[2:]:
        copy.start()
    for copy in copies:
        copy.wait()


def w_row2_pad(row):
    return jnp.concatenate([row, jnp.zeros((row.shape[0], 128 - row.shape[1]), row.dtype)], 1)


def per_device(
    sizes,
    block_x, block_hx, block_p, block_hp, potential, projectors, coupling,
    atom_count, proj_count, offsets, extents,
):
    cols, cz, cy, cx = block_x.shape
    slots, nproj = projectors.shape[-3], projectors.shape[-2]
    nz, ny, nx = sizes
    own = cz * cy
    turned = [
        jnp.transpose(b, (1, 2, 0, 3)).reshape(own, cols, cx)
        for b in (block_x, block_hx, block_p, block_hp)
    ]
    groups = (("gz", "gy"), ("gx",)) if nz * ny <= 16 else (("gz",), ("gy",), ("gx",))
    size_of = dict(zip(AXES, sizes))
    totals = []
    for group in groups:
        total = 1
        for a in group:
            total *= size_of[a]
        totals.append(total)
    tile = (cols, 128)
    rows = slots * nproj
    near, far = own * 128, (BZ - 1) * cy * 128
    scratch = [
        pltpu.VMEM((cols, 128), F32),
        pltpu.VMEM((own,) + tile, F32),
        pltpu.VMEM((own,) + tile, F32),
        pltpu.VMEM((2 * cols, 128), F32),
        pltpu.SMEM(offsets.shape, jnp.int32),
        pltpu.SMEM(extents.shape, jnp.int32),
        pltpu.SMEM(atom_count.shape, jnp.int32),
        pltpu.SMEM(proj_count.shape[2:], jnp.int32),
        pltpu.VMEM((cols, cols, 128), F32),
        pltpu.VMEM((nproj, nproj, slots), F32),
        pltpu.VMEM(potential.shape, F32),
        pltpu.VMEM(projectors.shape[3:], F32),
        pltpu.VMEM((192, own * 128), BF16),
        pltpu.VMEM((3 * cz, cy) + tile, F32),
        pltpu.VMEM((2, cz, cy) + tile, F32),
        pltpu.VMEM((tiles_of(own),) + tile, F32),
        pltpu.VMEM((tiles_of(own),) + tile, F32),
        pltpu.VMEM((tiles_of(own),) + tile, F32),
        pltpu.VMEM((tiles_of(own),) + tile, F32),
        pltpu.VMEM((own,) + tile, F32),
        pltpu.VMEM((3 * cz, cy) + tile, F32),
        pltpu.VMEM((cz, cy) + tile, F32),
        pltpu.VMEM((8, rows // 8 * (BZ * BY * BX // 128) + 1, 8, 128), F32),
        pltpu.SMEM((7,) + offsets.shape, jnp.int32),
        pltpu.VMEM((slots * BZ * (BY + cy - 1) + BY + 3 * (cy - 1), 8, 128), F32),
        pltpu.VMEM((256, near), BF16),
        pltpu.VMEM((256, far), BF16),
        pltpu.VMEM((2, 2, 2, 4, 128), F32),
        pltpu.VMEM((56, 4, 128), F32),
    ]
    scratch += [pltpu.VMEM((t, cols, 128), F32) for t in totals] * 2
    scratch += [pltpu.VMEM((t, 8, 128), F32) for t in totals]
    scratch += [
        pltpu.SemaphoreType.DMA((3 * len(groups),)),
        pltpu.SemaphoreType.DMA((3 * len(groups),)),
        pltpu.SemaphoreType.DMA((10,)),
        pltpu.SemaphoreType.DMA((10,)),
        pltpu.SemaphoreType.DMA((14,)),
        pltpu.SemaphoreType.DMA((14,)),
        pltpu.SemaphoreType.DMA((2,)),
        pltpu.SemaphoreType.DMA((11,)),
        pltpu.SemaphoreType.DMA((3,)),
    ]
    ways = 3 if ny == 2 else 4
    early_z = cz // 3
    scratch += [
        pltpu.VMEM((2, own) + tile, F32),
        pltpu.VMEM((own,) + tile, F32),
        pltpu.VMEM((own,) + tile, F32),
        pltpu.VMEM((ways, 2, early_z * cy) + tile, F32),
        pltpu.VMEM((ways, early_z, cy, 128), F32),
        pltpu.SemaphoreType.DMA((2 * ways,)),
        pltpu.SemaphoreType.DMA((2 * ways,)),
    ]
    vmem = pl.BlockSpec(memory_space=pltpu.VMEM)
    w, hw, sums = pl.pallas_call(
        functools.partial(kernel, sizes, groups, (cz, cy, cx, slots, nproj, cols)),
        out_shape=(
            pltpu.VMEM((own,) + tile, F32),
            pltpu.VMEM((own,) + tile, F32),
            pltpu.VMEM((2 * cols, 128), F32),
        ),
        in_specs=[pl.BlockSpec(memory_space=pltpu.HBM)] * 11,
        out_specs=(pl.BlockSpec(memory_space=pl.ANY),) * 3,
        scratch_shapes=scratch,
        compiler_params=pltpu.CompilerParams(
            collective_id=0, has_side_effects=True, vmem_limit_bytes=VMEM_LIMIT
        ),
    )(
        offsets, extents, atom_count, proj_count[0, 0],
        jnp.transpose(coupling[0, 0, 0], (1, 2, 0)),
        *turned, potential, projectors[0, 0, 0],
    )
    square = jax.ShapeDtypeStruct((3 * cols, 3 * cols), F32)
    field = jax.ShapeDtypeStruct((own,) + tile, F32)
    w, hw, gram, rayleigh = pl.pallas_call(
        functools.partial(finish_out, 1.0 / (own * cx * nz * ny * nx)),
        out_shape=(field, field, square, square),
        in_specs=[vmem] * 3,
        out_specs=(pl.BlockSpec(memory_space=pl.ANY),) * 4,
        scratch_shapes=[
            pltpu.VMEM(square.shape, F32),
            pltpu.VMEM(square.shape, F32),
            pltpu.SemaphoreType.DMA((4,)),
        ],
        compiler_params=pltpu.CompilerParams(vmem_limit_bytes=4 << 20),
    )(w, hw, sums)
    w, hw = (jnp.transpose(b.reshape(cz, cy, cols, cx), (2, 0, 1, 3)) for b in (w, hw))
    return (w, hw, gram, rayleigh)


def solution(mesh):
    sizes = tuple(mesh.shape[a] for a in AXES)
    in_specs = (
        P(None, "gz", "gy", "gx"),
        P(None, "gz", "gy", "gx"),
        P(None, "gz", "gy", "gx"),
        P(None, "gz", "gy", "gx"),
        P("gz", "gy", "gx"),
        P("gz", "gy", "gx", None, None, None),
        P("gz", "gy", "gx", None, None, None),
        P("gz", "gy", "gx"),
        P("gz", "gy", "gx", None),
        P(None, "gz", "gy", "gx", None),
        P(None, "gz", "gy", "gx", None),
    )
    out_specs = (P(None, "gz", "gy", "gx"), P(None, "gz", "gy", "gx"), P(), P())
    return jax.shard_map(
        functools.partial(per_device, sizes),
        mesh=mesh, in_specs=in_specs, out_specs=out_specs, check_vma=False,
    )
```

```python
import functools

import jax
import jax.numpy as jnp
from jax import lax
from jax.experimental import pallas as pl
from jax.experimental.pallas import tpu as pltpu
from jax.sharding import PartitionSpec as P

BZ, BY, BX = 4, 4, 16
LAP_CENTER = -5369.0 / 1800.0
LAP_COEFFS = (12.0 / 7.0, -15.0 / 56.0, 10.0 / 189.0, -1.0 / 112.0, 2.0 / 1925.0, -1.0 / 16632.0)
MESH = pl.DeviceIdType.MESH
VMEM_LIMIT = (63 << 20) - (64 << 10)
AXES = ("gz", "gy", "gx")
F32 = jnp.float32
BF16 = jnp.bfloat16
HP, HX, XX, PP, WW, HW = range(6)


EDGE = 8
PER_TILE = 128 // EDGE


def tiles_of(count):
    return -(-count // PER_TILE)


def solved(packed, cols, acol):
    shape = (8, 128)

    def spread(lane_at):
        return jnp.broadcast_to(packed[:, lane_at : lane_at + 1], shape)

    for j in range(cols):
        if j < 8:
            acol[j, 0:8] = spread(2 * cols + j)
        acol[j, 8:16] = spread(3 * cols + j)
    a = {}
    for j in range(cols):
        for i in range(j, cols):
            a[i, j] = jnp.broadcast_to(acol[j, i : i + 1, :], shape)
    scale = [lax.rsqrt(a[i, i]) for i in range(cols)]
    for i, j in a:
        a[i, j] = a[i, j] * scale[i] * scale[j]
    right = [
        [spread(half * cols + k) * scale[k] for half in range(2)] for k in range(cols)
    ]
    low = {}
    inverse = []
    for k in range(0, cols, 2):
        p, q, r = a[k, k], a[k + 1, k], a[k + 1, k + 1]
        det = 1.0 / (p * r - q * q)
        p, q, r = r * det, -q * det, p * det
        inverse.append((p, q, r))
        for i in range(k + 2, cols):
            low[i, k] = a[i, k] * p + a[i, k + 1] * q
            low[i, k + 1] = a[i, k] * q + a[i, k + 1] * r
            for j in range(k + 2, i + 1):
                a[i, j] = a[i, j] - (low[i, k] * a[j, k] + low[i, k + 1] * a[j, k + 1])
            right[i] = [
                right[i][h] - (low[i, k] * right[k][h] + low[i, k + 1] * right[k + 1][h])
                for h in range(2)
            ]
    out = [None] * cols
    for k in range(cols - 2, -1, -2):
        p, q, r = inverse[k // 2]
        halves = []
        for h in range(2):
            first = right[k][h] * p + right[k + 1][h] * q
            second = right[k][h] * q + right[k + 1][h] * r
            for i in range(cols - 1, k + 1, -1):
                first = first - low[i, k] * out[i][h]
                second = second - low[i, k + 1] * out[i][h]
            halves.append((first, second))
        out[k] = [halves[0][0], halves[1][0]]
        out[k + 1] = [halves[0][1], halves[1][1]]
    return [
        jnp.concatenate([out[k][0] * scale[k], out[k][1] * scale[k]], 0) for k in range(cols)
    ]


def kernel(
    sizes, groups, dims,
    off_in, ext_in, count_in, proj_in, d_in, x_in, hx_in, p_in, hp_in, v_in, beta_in,
    w_out, hw_out, sums_out, w_ref, hw_ref, sums_ref,
    off_ref, ext_ref, count_ref, proj_ref, acol, d_ref, v_ref, beta_ref,
    stack, zext, ybuf, xr, xl, edge_out, edge_in, edge_v, edge_v_in, edges, inner, nf,
    shared, trim, offs, lines, near0, near1, far0, far1, wside, parts4, parts_in,
    *rest,
):
    cz, cy, cx, slots, nproj, cols = dims
    nz, ny, nx = sizes
    n_red = len(groups)
    slow = (("gx",), ("gz",), ("gy",))
    n_slow = len(slow)
    bufs = (rest[:n_slow], rest[n_slow : n_slow + n_red], rest[n_slow + n_red : n_slow + 2 * n_red])
    rest = rest[n_slow + 2 * n_red :]
    red_send, red_recv, halo_send, halo_recv, atom_send, atom_recv, part_sem = rest[:7]
    load_sem, out_sem, xh, p_ref, hp_ref, raw, raw_v, raw_send, raw_recv, edge_send, edge_recv = rest[7:]
    x_ref, hx_ref = xh.at[0], xh.at[1]
    loads = []
    for i, (source, target) in enumerate(
        (
            (x_in, x_ref), (hx_in, hx_ref), (off_in, off_ref), (ext_in, ext_ref),
            (count_in, count_ref), (proj_in, proj_ref), (v_in, v_ref), (beta_in, beta_ref),
            (p_in, p_ref), (hp_in, hp_ref), (d_in, d_ref),
        )
    ):
        loads.append(pltpu.make_async_copy(source, target, load_sem.at[i]))
        loads[-1].start()
    zi, yi, xi = (lax.axis_index(a) for a in AXES)
    size_of = dict(zip(AXES, sizes))
    here = dict(zip(AXES, (zi, yi, xi)))
    more_z, more_y = BZ - 1, BY - 1
    own = cz * cy
    lane = lax.broadcasted_iota(jnp.int32, (cols, 128), 1)

    def neighbour(dz, dy, dx):
        step = dict(zip(AXES, (dz, dy, dx)))
        return {a: lax.rem(here[a] + step[a] + size_of[a], size_of[a]) for a in AXES}

    def member(group, offset):
        total = 1
        index = 0
        for a in group:
            total *= size_of[a]
            index = index * size_of[a] + here[a]
        target = lax.rem(index + offset, total)
        device = {}
        for a in reversed(group):
            device[a] = lax.rem(target, size_of[a])
            target = target // size_of[a]
        return {a: device.get(a, here[a]) for a in AXES}, index, total

    octant = [(o // 4, o // 2 % 2, o % 2) for o in range(8)]
    around = [
        (dz, dy, dx)
        for dx in (-1, 0, 1) for dz in (-1, 0, 1) for dy in (-1, 0, 1)
        if (dz, dy, dx) != (0, 0, 0)
    ]
    barrier = pltpu.get_barrier_semaphore()
    greeted = 0
    for group in groups:
        total = member(group, 0)[2]
        for offset in range(1, total):
            pl.semaphore_signal(
                barrier, inc=1, device_id=member(group, offset)[0], device_id_type=MESH
            )
            greeted += 1
    for where in around:
        pl.semaphore_signal(
            barrier, inc=1, device_id=neighbour(*where), device_id_type=MESH
        )
        greeted += 1

    def split_store(kind, cell, value):
        high = value.astype(BF16)
        low = (value - high.astype(F32)).astype(BF16)
        start = cell * 128 if isinstance(cell, int) else pl.multiple_of(cell * 128, 128)
        stack[kind * 32 : kind * 32 + 32, pl.ds(start, 128)] = jnp.concatenate([high, low], 0)

    def split_all(*kinds):
        @pl.loop(0, cz)
        def _(z):
            for y in range(cy):
                cell = z * cy + y
                for kind, ref in kinds:
                    split_store(kind, cell, ref[cell])

    for load in loads[:2]:
        load.wait()
    split_all((HX, hx_ref), (XX, x_ref))

    def products(left, right_from, right_to, count=1):
        m = lax.dot_general(
            stack[left * 32 : (left + count) * 32, :],
            stack[right_from * 32 : right_to * 32, :],
            (((1,), (1,)), ((), ())),
            preferred_element_type=F32,
        )
        parts = [m[32 * i : 32 * i + cols] + m[32 * i + cols : 32 * i + 32] for i in range(count)]
        return parts if count > 1 else parts[0]

    def reduced(which, payload):
        for phase, group in enumerate(slow if which == 0 else groups):
            buf = bufs[which][phase]
            _, index, total = member(group, 0)
            at = phase + (which and len(slow) + (which - 1) * n_red)
            send_sem, recv_sem = red_send.at[at], red_recv.at[at]
            buf[index] = payload
            if phase == 0 and which == 2:
                pl.semaphore_wait(barrier, greeted)
            for offset in range(1, total):
                pltpu.make_async_remote_copy(
                    src_ref=buf.at[index],
                    dst_ref=buf.at[index],
                    send_sem=send_sem,
                    recv_sem=recv_sem,
                    device_id=member(group, offset)[0],
                    device_id_type=MESH,
                ).start()
            yield None
            most = buf.at[pl.ds(0, total - 1)]
            for sem in (recv_sem, send_sem):
                pltpu.make_async_copy(most, most, sem).wait()
            payload = buf[0]
            for slot in range(1, total):
                payload = payload + buf[slot]
        yield payload

    def finish(steps):
        out = None
        for out in steps:
            pass
        return out

    both = lax.dot_general(
        stack[HX * 32 : XX * 32 + 32, :], stack[XX * 32 : XX * 32 + 32, :],
        (((1,), (1,)), ((), ())), preferred_element_type=F32,
    )
    both = jnp.concatenate([both, jnp.zeros((64, 96), F32)], 1)
    turn_hx = both[:cols] + both[cols:32]
    corr = both[32 : 32 + cols] + both[32 + cols :]
    narrow = lax.broadcasted_iota(jnp.int32, (8, 128), 1)

    def merged(tile):
        return tile + pltpu.roll(tile, 128 - cols, 1)

    payload0 = jnp.where(narrow < cols, merged(turn_hx[:8]), 0.0)
    for at, tile in ((1, turn_hx[8:]), (2, corr[:8]), (3, corr[8:])):
        moved = pltpu.roll(merged(tile), at * cols, 1)
        payload0 = jnp.where((narrow >= at * cols) & (narrow < at * cols + cols), moved, payload0)
    solving = reduced(2, payload0)
    next(solving)
    for load in loads[2:]:
        load.wait()
    lane8 = lax.broadcasted_iota(jnp.int32, (8, 128), 1)
    rows = slots * nproj
    pairs = rows // 8
    columns = BZ * BY * BX // 128
    box_lane = lax.broadcasted_iota(jnp.int32, (nproj, BZ * BY * BX), 1)
    box_row = lax.broadcasted_iota(jnp.int32, (nproj, BZ * BY * BX), 0)
    box_a, box_b, box_c = box_lane // (BY * BX), box_lane // BX % BY, box_lane % BX
    for s in range(slots):
        kept = jnp.where(s < count_ref[0, 0, 0], proj_ref[0, s], 0)
        inside = (
            (box_row < kept)
            & (box_a < ext_ref[0, 0, 0, 0, s])
            & (box_b < ext_ref[1, 0, 0, 0, s])
            & (box_c < ext_ref[2, 0, 0, 0, s])
        )
        at = s * nproj
        kept = jnp.where(inside, beta_ref[s], 0.0)
        for c in range(columns):
            where = (0, at // 8 * columns + c, slice(at % 8, at % 8 + nproj), slice(None))
            shared[where] = kept[:, c * 128 : c * 128 + 128]
    lane1 = lax.broadcasted_iota(jnp.int32, (1, 128), 1)
    lane16 = lax.broadcasted_iota(jnp.int32, (nproj, 128), 1)
    slot_at = lane16 % 64 // 16 * (8 // nproj) + lane16 % 8 // nproj
    table = []
    for p in range(nproj):
        mirrored = jnp.concatenate([d_ref[q, p : p + 1, :] for q in range(nproj)], 0)
        sym = 0.5 * (d_ref[p] + mirrored)
        spread = jnp.zeros((nproj, 128), F32)
        for s in range(slots):
            value = jnp.broadcast_to(sym[:, s : s + 1], (nproj, 128))
            spread = jnp.where(slot_at == s, value, spread)
        table.append(spread)
    for d in range(-nproj + 1, nproj):
        row = jnp.zeros((1, 128), F32)
        for p in range(max(0, -d), min(nproj, nproj - d)):
            row = jnp.where(lane1 % nproj == p, table[p][p + d : p + d + 1, :], row)
        shared[0, pairs * columns, d + nproj - 1 : d + nproj, :] = row
    for pair in range(0, pairs, 2):
        lasts = []
        for p in (pair, pair + 1):
            first, last = shared[0, p * columns], shared[0, p * columns + 1]
            lasts.append(last)
            trim[p] = jnp.where(
                lane8 < 48, pltpu.roll(first, 112, 1),
                jnp.where(lane8 < 96, pltpu.roll(first, 96, 1), pltpu.roll(last, 80, 1)),
            )
        trim[pairs + pair // 2] = jnp.where(
            lane8 < 64,
            jnp.where(lane8 < 16, pltpu.roll(lasts[0], 80, 1), pltpu.roll(lasts[0], 64, 1)),
            jnp.where(lane8 < 80, pltpu.roll(lasts[1], 16, 1), lasts[1]),
        )
    trim[pairs + pairs // 2] = shared[0, pairs * columns]
    atom_copies = {}
    for o in (4, 2, 1, 6, 5, 3, 7):
        atom_copies[o] = [
            pltpu.make_async_remote_copy(
                src_ref=source,
                dst_ref=target,
                send_sem=atom_send.at[2 * (o - 1) + i],
                recv_sem=atom_recv.at[2 * (o - 1) + i],
                device_id=neighbour(*octant[o]),
                device_id_type=MESH,
            )
            for i, (source, target) in enumerate(
                (
                    (off_ref, offs.at[o - 1]),
                    (trim, shared.at[o, pl.ds(0, pairs + pairs // 2 + 1)])
                    if octant[o][1] else (shared.at[0], shared.at[o]),
                )
            )
        ]
        for copy in atom_copies[o]:
            copy.start()
    split_all((HP, hp_ref), (PP, p_ref))
    hx_row, x_row, p_row = products(HX, HP, WW, 3)
    first = jnp.where((lane >= 32) & (lane < 64), pltpu.roll(hx_row, 96, 1), x_row)

    def paired(upper, lower):
        upper = upper + pltpu.roll(upper, 112, 1)
        lower = lower + pltpu.roll(lower, 112, 1)
        return jnp.where(lane % 32 < 16, upper, pltpu.roll(lower, 16, 1))

    reduction = reduced(0, paired(first, p_row))

    row8 = lax.broadcasted_iota(jnp.int32, (8, 128), 0)
    in_tile = 128 // BX
    width = BY + cy - 1
    ahead = cy - 1
    nothing = ahead + slots * BZ * width + ahead
    tables = {(0, 0): near0, (0, 1): near1, (1, 0): far0, (1, 1): far1}
    blank_line = jnp.zeros((8, 128), F32)

    @pl.loop(0, slots * BZ)
    def _(block):
        for b in range(BY, width):
            lines[ahead + block * width + b] = blank_line

    for at in [*range(ahead), *range(nothing - ahead, nothing + width)]:
        lines[at] = blank_line

    def build(o):
        dz, dy, dx = octant[o]

        def expand(pair):
            if dy:
                tiles = [shared[o, pair], shared[o, pairs + pair // 2]]
            else:
                tiles = [shared[o, pair * columns + c] for c in range(columns)]
            places = {}
            for at in range(BZ * BY):
                a, b = at // BY, at % BY
                if not dy:
                    places[at] = at // in_tile, at % in_tile
                elif b and a * (BY - 1) + b - 1 < in_tile:
                    places[at] = 0, a * (BY - 1) + b - 1
                elif b:
                    places[at] = 1, pair % 2 * (in_tile // 2) + a * (BY - 1) + b - 1 - in_tile
            for half in range(8 // nproj):
                s = pair * (8 // nproj) + half
                ox = offset(2, s)
                along = (lane8 - ox + 128) & 127
                side = lane8 < ox if dx else lane8 >= ox
                keep = (along < BX) & side & (row8 // nproj == half)
                for at, (tile, k) in places.items():
                    shift = (ox + 128 - BX * k) & 127
                    part = jnp.where(keep, pltpu.roll(tiles[tile], shift, 1), 0.0)
                    lines[ahead + (s * BZ + at // BY) * width + at % BY] = part

        def offset(axis, s):
            return off_ref[axis, 0, 0, 0, s] if o == 0 else offs[o - 1, axis, 0, 0, 0, s]

        for pair in range(pairs):
            expand(pair)

        target = tables[dz, dy]
        top = dx * 64
        ys = more_y if dy else cy

        @pl.loop(0, more_z if dz else cz)
        def _(z):
            starts = []
            for s in range(slots):
                a = z + dz * cz - offset(0, s)
                ok = (a >= 0) & (a < BZ)
                start = jnp.where(ok, ahead + (s * BZ + a) * width - offset(1, s), nothing - offset(1, s))
                starts.append(start)
            for y in range(ys):
                column = pl.ds(pl.multiple_of((z * ys + y) * 128, 128), 128)
                for pair in range(pairs):
                    at = top + pair * 16
                    total = None
                    for half in range(8 // nproj):
                        start = starts[pair * (8 // nproj) + half] + (y + dy * cy)
                        part = lines[start]
                        total = part if total is None else total + part
                    high = total.astype(BF16)
                    low = (total - high.astype(F32)).astype(BF16)
                    target[at : at + 16, column] = jnp.concatenate([high, low], 0)

    for z in range(cz):
        for y in range(cy):
            inner[z, y] = jnp.zeros((cols, 128), F32)
            inner[2 * cz + z, y] = jnp.zeros((cols, 128), F32)
    def build_all(owners):
        for o in owners:
            for copy in atom_copies[o]:
                copy.wait()
            build(o)

    build(0)
    early_z = cz // 3
    early_to = [(-1, 0, 0), (1, 0, 0), (0, -1, 0)] + ([] if ny == 2 else [(0, 1, 0)])
    raw_copies = []
    for d, where in enumerate(early_to):
        for i, (source, target) in enumerate(
            (
                (xh.at[:, pl.ds(0, early_z * cy)], raw.at[d]),
                (v_ref.at[pl.ds(0, early_z)], raw_v.at[d]),
            )
        ):
            raw_copies.append(
                pltpu.make_async_remote_copy(
                    src_ref=source,
                    dst_ref=target,
                    send_sem=raw_send.at[2 * d + i],
                    recv_sem=raw_recv.at[2 * d + i],
                    device_id=neighbour(*where),
                    device_id_type=MESH,
                )
            )
            raw_copies[-1].start()
    def packed(read, rows_of):
        at_lane = lax.broadcasted_iota(jnp.int32, (rows_of, 128), 1)
        for q in range(tiles_of(own)):
            low = jnp.zeros((rows_of, 128), F32)
            high = low
            for j in range(min(PER_TILE, own - PER_TILE * q)):
                tile = read(PER_TILE * q + j)
                keep = (at_lane >= EDGE * j) & (at_lane < EDGE * j + EDGE)
                low = jnp.where(keep, pltpu.roll(tile, EDGE * j, 1) if j else tile, low)
                turn = (EDGE * j + EDGE) % 128
                high = jnp.where(keep, pltpu.roll(tile, turn, 1) if turn else tile, high)
            yield q, low, high

    edge_v[...] = jnp.zeros(edge_v.shape, F32)
    for kind in range(2):
        for q, low, high in packed(lambda cell: xh[kind, cell], cols):
            edge_out[0, kind, q] = low
            edge_out[1, kind, q] = high
    for q, low, high in packed(lambda cell: v_ref[cell // cy, cell % cy : cell % cy + 1, :], 1):
        edge_v[0, q : q + 1, :] = low
        edge_v[1, q : q + 1, :] = high
    next(solving)
    next(reduction)
    edge_copies = []
    for side, step in enumerate((-1, 1)):
        for i, (source, target) in enumerate(
            ((edge_out.at[side], edge_in.at[side]), (edge_v.at[side], edge_v_in.at[side]))
        ):
            edge_copies.append(
                pltpu.make_async_remote_copy(
                    src_ref=source,
                    dst_ref=target,
                    send_sem=edge_send.at[2 * side + i],
                    recv_sem=edge_recv.at[2 * side + i],
                    device_id=neighbour(0, 0, step),
                    device_id_type=MESH,
                )
            )
            edge_copies[-1].start()
    build_all((4, 2, 6, 1, 5, 3, 7))
    sums0 = finish(solving)
    sums0 = solved(sums0, cols, acol)
    theta_cols = sums0

    @pl.loop(0, cz)
    def _(z):
        for y in range(cy):
            cell = z * cy + y
            xs = x_ref[cell]
            value = hx_ref[cell]
            for k in range(cols):
                value = value - theta_cols[k] * xs[k : k + 1, :]
            vv = v_ref[z, y : y + 1, :]
            value = value * (1.0 / (1.0 + vv * vv))
            zext[cz + z, y] = value
            inner[cz + z, y] = value
            w_ref[cell] = value
            split_store(WW, cell, value)
            if y < more_y:
                place = pl.ds(pl.multiple_of((z * more_y + y) * 128, 128), 128)
                high = value.astype(BF16)
                low = (value - high.astype(F32)).astype(BF16)
                wside[:, place] = jnp.concatenate([high, low], 0)

    two_y = ny == 2
    split = early_z + (cz - early_z) // 2

    def some(ref, z, dz, y, dy):
        return ref.at[pl.ds(z, dz), pl.ds(y, dy)]

    def layers(target, base, z, dz, where):
        return some(zext, cz + z, dz, 0, cy), some(target, base + z, dz, 0, cy), where

    def bulk(z, dz):
        sends = [
            layers(zext, 2 * cz, z, dz, (-1, 0, 0)),
            layers(zext, 0, z, dz, (1, 0, 0)),
            layers(ybuf.at[1], 0, z, dz, (0, -1, 0)),
        ]
        if not two_y:
            sends.append(layers(ybuf.at[0], 0, z, dz, (0, 1, 0)))
        return sends

    early = bulk(early_z, split - early_z)
    late = bulk(split, cz - split)

    def launch(sends, send_sem, recv_sem, first=0):
        copies = []
        for i, (source, target, where) in enumerate(sends, start=first):
            copies.append(
                pltpu.make_async_remote_copy(
                    src_ref=source,
                    dst_ref=target,
                    send_sem=send_sem.at[i],
                    recv_sem=recv_sem.at[i],
                    device_id=neighbour(*where),
                    device_id_type=MESH,
                )
            )
            copies[-1].start()
        return copies

    copies = launch(early, halo_send, halo_recv)
    outs = [
        pltpu.make_async_copy(source, target, out_sem.at[i])
        for i, (source, target) in enumerate(
            ((w_ref, w_out), (hw_ref, hw_out), (sums_ref, sums_out))
        )
    ]
    outs[0].start()
    w_rows = stack.at[WW * 32 : WW * 32 + 32]
    lane4 = lax.broadcasted_iota(jnp.int32, (4, 128), 1)
    for dz in range(2):
        for dy in range(2):
            table = tables[dz, dy]
            source = wside if dy else w_rows
            m = lax.dot_general(
                table[...], source[:, : table.shape[1]],
                (((1,), (1,)), ((), ())), preferred_element_type=F32,
            )
            m = jnp.concatenate([m, jnp.zeros((128, 128 - 2 * cols), F32)], 1)
            m = jnp.transpose(m)
            m = m[:cols] + m[cols : 2 * cols]
            m = m + pltpu.roll(m, 128 - 8, 1)
            upper, lower = m[:8], m[8:]
            both = jnp.where(lane8 % 16 < 8, upper, pltpu.roll(lower, 8, 1))
            moved = pltpu.roll(both, 64, 1)
            parts4[dz, dy, 0] = jnp.where(lane4 < 64, both[:4], moved[4:])
            parts4[dz, dy, 1] = jnp.where(lane4 < 64, moved[:4], both[4:])

    def span(step):
        return (max(0, -step), 2 - abs(step))

    slot_of = {}
    filled = 0
    for where in around:
        slot_of[where] = filled
        filled += span(where[0])[1] * span(where[1])[1] * span(where[2])[1]
    for where in around:
        (z0, zn), (y0, yn), (x0, xn) = (span(step) for step in where)
        for z in range(z0, z0 + zn):
            for y in range(y0, y0 + yn):
                at = slot_of[where] + ((z - z0) * yn + y - y0) * xn
                pltpu.make_async_remote_copy(
                    src_ref=parts4.at[z, y, pl.ds(x0, xn)],
                    dst_ref=parts_in.at[pl.ds(at, xn)],
                    send_sem=part_sem.at[0],
                    recv_sem=part_sem.at[1],
                    device_id=neighbour(*where),
                    device_id_type=MESH,
                ).start()
    late_copies = launch(late, halo_send, halo_recv, len(early))
    w_row = products(WW, HP, WW)
    w_row2 = products(WW, XX, HW)
    for copy in edge_copies:
        copy.wait()
    for side, target in enumerate((xr, xl)):
        for q in range(tiles_of(own)):
            value = edge_in[side, 1, q]
            xs = edge_in[side, 0, q]
            for k in range(cols):
                value = value - theta_cols[k] * xs[k : k + 1, :]
            vv = edge_v_in[side, q : q + 1, :]
            target[q] = value * (1.0 / (1.0 + vv * vv))
    for copy in raw_copies:
        copy.wait()
    for d in range(len(early_to)):
        target, base = ((zext, 2 * cz), (zext, 0), (ybuf.at[1], 0), (ybuf.at[0], 0))[d]

        @pl.loop(0, early_z)
        def _(z):
            for y in range(cy):
                cell = z * cy + y
                xs = raw[d, 0, cell]
                value = raw[d, 1, cell]
                for k in range(cols):
                    value = value - theta_cols[k] * xs[k : k + 1, :]
                vv = raw_v[d, z, y : y + 1, :]
                target[base + z, y] = value * (1.0 / (1.0 + vv * vv))

    next(reduction)
    @pl.loop(0, cz)
    def _(z):
        for y in range(cy):
            centre = inner[cz + z, y]
            vv = v_ref[z, y : y + 1, :]
            total = centre * (vv - 1.5 * LAP_CENTER)
            for k, weight in enumerate(LAP_COEFFS, start=1):
                tiles = [inner[cz + z, t] for t in (y + k, y - k) if 0 <= t < cy]
                if k < cz:
                    tiles += [inner[cz + z + k, y], inner[cz + z - k, y]]
                beside = None
                for tile in tiles:
                    beside = tile if beside is None else beside + tile
                if beside is not None:
                    total = total - 0.5 * weight * beside
            hw_ref[z * cy + y] = total

    for cell in range(own):
        left, right = xl[cell // PER_TILE], xr[cell // PER_TILE]
        turn = (256 - EDGE - EDGE * (cell % PER_TILE)) % 128
        left = pltpu.roll(left, turn, 1) if turn else left
        shift = (128 - EDGE * (cell % PER_TILE)) % 128
        right = pltpu.roll(right, shift, 1) if shift else right
        edges[cell] = jnp.where(lane < 64, right, left)

    @pl.loop(0, cz)
    def _(z):
        for y in range(cy):
            cell = z * cy + y
            edge = edges[cell]
            centre = inner[cz + z, y]
            total = hw_ref[cell]
            for k, weight in enumerate(LAP_COEFFS, start=1):
                beside = pltpu.roll(jnp.where(lane < k, edge, centre), 128 - k, 1)
                beside = beside + pltpu.roll(jnp.where(lane >= 128 - k, edge, centre), k, 1)
                total = total - 0.5 * weight * beside
            hw_ref[cell] = total
    for sem in (part_sem.at[1], part_sem.at[0]):
        pltpu.make_async_copy(parts_in, parts_in, sem).wait()
    gathered = {}
    for dz in range(2):
        for dy in range(2):
            sums = []
            for dx in range(2):
                total = None
                for from_z in range(2):
                    for from_y in range(2):
                        for from_x in range(2):
                            where = (dz - from_z, dy - from_y, dx - from_x)
                            if where == (0, 0, 0):
                                tile = parts4[dz, dy, dx]
                            else:
                                (z0, _), (y0, yn), (x0, xn) = (span(step) for step in where)
                                at = ((from_z - z0) * yn + from_y - y0) * xn + from_x - x0
                                tile = parts_in[slot_of[where] + at]
                            total = tile if total is None else total + tile
                sums.append(total)
            turned = [pltpu.roll(total, 64, 1) for total in sums]
            gathered[dz, dy] = jnp.concatenate(
                [
                    jnp.where(lane4 < 64, sums[0], turned[1]),
                    jnp.where(lane4 < 64, turned[0], sums[1]),
                ],
                0,
            )
    coef_at = (pairs * columns, pairs + pairs // 2)
    lefts = {}
    for dz in range(2):
        for dy in range(2):
            total = gathered[dz, dy]
            o = dz * 4 + dy * 2
            coefs = jnp.where(
                lane8 < 64, shared[o, coef_at[dy]], shared[o + 1, coef_at[dy]]
            )
            mixed = None
            for d in range(-nproj + 1, nproj):
                term = pltpu.roll(total, (128 - d) % 128, 1) if d else total
                term = term * coefs[d + nproj - 1 : d + nproj, :]
                mixed = term if mixed is None else mixed + term
            low_half = lane8 % 16 < 8
            mixed = jnp.concatenate(
                [
                    jnp.where(low_half, mixed, pltpu.roll(mixed, 8, 1)),
                    jnp.where(low_half, pltpu.roll(mixed, 120, 1), mixed),
                ],
                0,
            )
            high = mixed.astype(BF16)
            low = (mixed - high.astype(F32)).astype(BF16)
            lefts[dz, dy] = jnp.concatenate([high, low], 0)

    for z in range(cz):
        sums = {}
        for dz in range(2 if z < more_z else 1):
            for dy in range(2):
                ys = more_y if dy else cy
                m = lax.dot_general(
                    lefts[dz, dy], tables[dz, dy][:, z * ys * 128 : (z + 1) * ys * 128],
                    (((1,), (0,)), ((), ())), preferred_element_type=F32,
                )
                m = m[:cols] + m[cols:]
                for y in range(ys):
                    part = m[:, y * 128 : y * 128 + 128]
                    sums[y] = sums[y] + part if y in sums else part
        for y in range(cy):
            nf[z, y] = sums[y]
    next(reduction)
    for copy in copies + late_copies:
        copy.wait()
    hw_sum = None
    for cell in range(own):
        z, y = cell // cy, cell % cy
        total = hw_ref[cell] + nf[z, y]
        weights = {}
        for k, weight in enumerate(LAP_COEFFS, start=1):
            keys = [("z", z + k), ("z", z - k), (1, y + k - cy), (1 if two_y else 0, y - k + cy)]
            for key, inside in zip(keys, (z + k < cz, z - k >= 0, y + k < cy, y - k >= 0)):
                if not inside:
                    weights[key] = weights.get(key, 0.0) - 0.5 * weight
        for (where, at), weight in weights.items():
            tile = zext[cz + at, y] if where == "z" else ybuf[where, z, at]
            total = total + weight * tile
        hw_ref[cell] = total
        split_store(HW, cell, total)
        if y == cy - 1:
            plane = slice(z * cy * 128, (z + 1) * cy * 128)
            part = lax.dot_general(
                stack[HW * 32 : HW * 32 + 32, plane], stack[XX * 32 : HW * 32, plane],
                (((1,), (1,)), ((), ())), preferred_element_type=F32,
            )
            hw_sum = part if hw_sum is None else hw_sum + part
    outs[1].start()
    hw_row = w_row2_pad(hw_sum[:cols] + hw_sum[cols:])
    second = jnp.where(lane < 96, hw_row, pltpu.roll(w_row2_pad(w_row2), 32, 1))
    closing = reduced(1, paired(w_row, second))
    next(closing)
    sums1 = next(reduction)
    next(closing)
    sums2 = finish(closing)
    sums_ref[...] = jnp.concatenate([sums1, sums2], 0)
    outs[2].start()
    for out in outs:
        out.wait()


def finish_out(weight, w_ref, hw_ref, sums_ref, w_out, hw_out, gram_out, ray_out, gram_ref, ray_ref, sems):
    copies = [
        pltpu.make_async_copy(source, target, sems.at[i])
        for i, (source, target) in enumerate(
            ((w_ref, w_out), (hw_ref, hw_out), (gram_ref, gram_out), (ray_ref, ray_out))
        )
    ]
    for copy in copies[:2]:
        copy.start()
    sums1, sums2 = sums_ref[:16], sums_ref[16:]
    lane = lax.broadcasted_iota(jnp.int32, (16, 128), 1)
    rows = jnp.concatenate([sums1, pltpu.roll(sums1, 112, 1), sums2, pltpu.roll(sums2, 112, 1)], 0)
    rows = rows * weight
    turned = jnp.transpose(jnp.concatenate([rows, jnp.zeros_like(rows)], 0))

    def direct(row, group, target):
        return rows[16 * row : 16 * row + 16, :], 32 * group, target

    def flipped(row, group, target):
        return turned[32 * group : 32 * group + 16, :], 16 * row, target

    def laid(parts):
        total = None
        for tile, begin, target in parts:
            shift = (16 * target - begin) % 128
            tile = pltpu.roll(tile, shift, 1) if shift else tile
            tile = jnp.where((lane >= 16 * target) & (lane < 16 * target + 16), tile, 0.0)
            total = tile if total is None else total + tile
        return total

    gram = [
        [direct(0, 2, 0), flipped(2, 2, 1), direct(0, 3, 2)],
        [direct(2, 2, 0), direct(3, 3, 1), direct(2, 3, 2)],
        [direct(1, 2, 0), flipped(2, 3, 1), direct(1, 3, 2)],
    ]
    rayleigh = [
        [flipped(0, 1, 0), flipped(3, 0, 1), direct(0, 0, 2)],
        [direct(2, 1, 0), flipped(3, 2, 1), direct(2, 0, 2)],
        [direct(1, 1, 0), flipped(3, 1, 1), direct(1, 0, 2)],
    ]
    for i in range(3):
        gram_ref[16 * i : 16 * i + 16, :] = laid(gram[i])[:, :48]
        ray_ref[16 * i : 16 * i + 16, :] = laid(rayleigh[i])[:, :48]
    for copy in copies[2:]:
        copy.start()
    for copy in copies:
        copy.wait()


def w_row2_pad(row):
    return jnp.concatenate([row, jnp.zeros((row.shape[0], 128 - row.shape[1]), row.dtype)], 1)


def per_device(
    sizes,
    block_x, block_hx, block_p, block_hp, potential, projectors, coupling,
    atom_count, proj_count, offsets, extents,
):
    cols, cz, cy, cx = block_x.shape
    slots, nproj = projectors.shape[-3], projectors.shape[-2]
    nz, ny, nx = sizes
    own = cz * cy
    turned = [
        jnp.transpose(b, (1, 2, 0, 3)).reshape(own, cols, cx)
        for b in (block_x, block_hx, block_p, block_hp)
    ]
    groups = (("gz", "gy"), ("gx",)) if nz * ny <= 16 else (("gz",), ("gy",), ("gx",))
    size_of = dict(zip(AXES, sizes))
    totals = []
    for group in groups:
        total = 1
        for a in group:
            total *= size_of[a]
        totals.append(total)
    tile = (cols, 128)
    rows = slots * nproj
    scratch = [
        pltpu.VMEM((own,) + tile, F32),
        pltpu.VMEM((own,) + tile, F32),
        pltpu.VMEM((2 * cols, 128), F32),
        pltpu.SMEM(offsets.shape, jnp.int32),
        pltpu.SMEM(extents.shape, jnp.int32),
        pltpu.SMEM(atom_count.shape, jnp.int32),
        pltpu.SMEM(proj_count.shape[2:], jnp.int32),
        pltpu.VMEM((cols, cols, 128), F32),
        pltpu.VMEM((nproj, nproj, slots), F32),
        pltpu.VMEM(potential.shape, F32),
        pltpu.VMEM(projectors.shape[3:], F32),
        pltpu.VMEM((192, own * 128), BF16),
        pltpu.VMEM((3 * cz, cy) + tile, F32),
        pltpu.VMEM((2, cz, cy) + tile, F32),
        pltpu.VMEM((tiles_of(own),) + tile, F32),
        pltpu.VMEM((tiles_of(own),) + tile, F32),
        pltpu.VMEM((2, 2, tiles_of(own)) + tile, F32),
        pltpu.VMEM((2, 2, tiles_of(own)) + tile, F32),
        pltpu.VMEM((2, 8 * (-(-tiles_of(own) // 8)), 128), F32),
        pltpu.VMEM((2, 8 * (-(-tiles_of(own) // 8)), 128), F32),
        pltpu.VMEM((own,) + tile, F32),
        pltpu.VMEM((3 * cz, cy) + tile, F32),
        pltpu.VMEM((cz, cy) + tile, F32),
        pltpu.VMEM((8, rows // 8 * (BZ * BY * BX // 128) + 1, 8, 128), F32),
        pltpu.VMEM((rows // 8 + rows // 16 + 1, 8, 128), F32),
        pltpu.SMEM((7,) + offsets.shape, jnp.int32),
        pltpu.VMEM((slots * BZ * (BY + cy - 1) + BY + 3 * (cy - 1), 8, 128), F32),
        pltpu.VMEM((128, own * 128), BF16),
        pltpu.VMEM((128, cz * (BY - 1) * 128), BF16),
        pltpu.VMEM((128, (BZ - 1) * cy * 128), BF16),
        pltpu.VMEM((128, (BZ - 1) * (BY - 1) * 128), BF16),
        pltpu.VMEM((2 * cols, cz * (BY - 1) * 128), BF16),
        pltpu.VMEM((2, 2, 2, 4, 128), F32),
        pltpu.VMEM((56, 4, 128), F32),
    ]
    scratch += [pltpu.VMEM((size_of[a], cols, 128), F32) for a in ("gx", "gz", "gy")]
    scratch += [pltpu.VMEM((t, cols, 128), F32) for t in totals]
    scratch += [pltpu.VMEM((t, 8, 128), F32) for t in totals]
    scratch += [
        pltpu.SemaphoreType.DMA((3 + 2 * len(groups),)),
        pltpu.SemaphoreType.DMA((3 + 2 * len(groups),)),
        pltpu.SemaphoreType.DMA((8,)),
        pltpu.SemaphoreType.DMA((8,)),
        pltpu.SemaphoreType.DMA((14,)),
        pltpu.SemaphoreType.DMA((14,)),
        pltpu.SemaphoreType.DMA((2,)),
        pltpu.SemaphoreType.DMA((11,)),
        pltpu.SemaphoreType.DMA((3,)),
    ]
    ways = 3 if ny == 2 else 4
    early_z = cz // 3
    scratch += [
        pltpu.VMEM((2, own) + tile, F32),
        pltpu.VMEM((own,) + tile, F32),
        pltpu.VMEM((own,) + tile, F32),
        pltpu.VMEM((ways, 2, early_z * cy) + tile, F32),
        pltpu.VMEM((ways, early_z, cy, 128), F32),
        pltpu.SemaphoreType.DMA((2 * ways,)),
        pltpu.SemaphoreType.DMA((2 * ways,)),
        pltpu.SemaphoreType.DMA((4,)),
        pltpu.SemaphoreType.DMA((4,)),
    ]
    vmem = pl.BlockSpec(memory_space=pltpu.VMEM)
    w, hw, sums = pl.pallas_call(
        functools.partial(kernel, sizes, groups, (cz, cy, cx, slots, nproj, cols)),
        out_shape=(
            pltpu.VMEM((own,) + tile, F32),
            pltpu.VMEM((own,) + tile, F32),
            pltpu.VMEM((2 * cols, 128), F32),
        ),
        in_specs=[pl.BlockSpec(memory_space=pltpu.HBM)] * 11,
        out_specs=(pl.BlockSpec(memory_space=pl.ANY),) * 3,
        scratch_shapes=scratch,
        compiler_params=pltpu.CompilerParams(
            collective_id=0, has_side_effects=True, vmem_limit_bytes=VMEM_LIMIT
        ),
    )(
        offsets, extents, atom_count, proj_count[0, 0],
        jnp.transpose(coupling[0, 0, 0], (1, 2, 0)),
        *turned, potential, projectors[0, 0, 0],
    )
    square = jax.ShapeDtypeStruct((3 * cols, 3 * cols), F32)
    field = jax.ShapeDtypeStruct((own,) + tile, F32)
    w, hw, gram, rayleigh = pl.pallas_call(
        functools.partial(finish_out, 1.0 / (own * cx * nz * ny * nx)),
        out_shape=(field, field, square, square),
        in_specs=[vmem] * 3,
        out_specs=(pl.BlockSpec(memory_space=pl.ANY),) * 4,
        scratch_shapes=[
            pltpu.VMEM(square.shape, F32),
            pltpu.VMEM(square.shape, F32),
            pltpu.SemaphoreType.DMA((4,)),
        ],
        compiler_params=pltpu.CompilerParams(vmem_limit_bytes=4 << 20),
    )(w, hw, sums)
    w, hw = (jnp.transpose(b.reshape(cz, cy, cols, cx), (2, 0, 1, 3)) for b in (w, hw))
    return (w, hw, gram, rayleigh)


def solution(mesh):
    sizes = tuple(mesh.shape[a] for a in AXES)
    in_specs = (
        P(None, "gz", "gy", "gx"),
        P(None, "gz", "gy", "gx"),
        P(None, "gz", "gy", "gx"),
        P(None, "gz", "gy", "gx"),
        P("gz", "gy", "gx"),
        P("gz", "gy", "gx", None, None, None),
        P("gz", "gy", "gx", None, None, None),
        P("gz", "gy", "gx"),
        P("gz", "gy", "gx", None),
        P(None, "gz", "gy", "gx", None),
        P(None, "gz", "gy", "gx", None),
    )
    out_specs = (P(None, "gz", "gy", "gx"), P(None, "gz", "gy", "gx"), P(), P())
    return jax.shard_map(
        functools.partial(per_device, sizes),
        mesh=mesh, in_specs=in_specs, out_specs=out_specs, check_vma=False,
    )
```

```python
import functools

import jax
import jax.numpy as jnp
from jax import lax
from jax.experimental import pallas as pl
from jax.experimental.pallas import tpu as pltpu
from jax.sharding import PartitionSpec as P

BZ, BY, BX = 4, 4, 16
LAP_CENTER = -5369.0 / 1800.0
LAP_COEFFS = (12.0 / 7.0, -15.0 / 56.0, 10.0 / 189.0, -1.0 / 112.0, 2.0 / 1925.0, -1.0 / 16632.0)
MESH = pl.DeviceIdType.MESH
VMEM_LIMIT = (63 << 20) - (64 << 10)
AXES = ("gz", "gy", "gx")
F32 = jnp.float32
BF16 = jnp.bfloat16
HP, HX, XX, PP, WW, HW = range(6)


EDGE = 8
PER_TILE = 128 // EDGE


def tiles_of(count):
    return -(-count // PER_TILE)


def solved(packed, cols, acol):
    shape = (8, 128)

    def spread(lane_at):
        return jnp.broadcast_to(packed[:, lane_at : lane_at + 1], shape)

    for j in range(cols):
        if j < 8:
            acol[j, 0:8] = spread(2 * cols + j)
        acol[j, 8:16] = spread(3 * cols + j)
    a = {}
    for j in range(cols):
        for i in range(j, cols):
            a[i, j] = jnp.broadcast_to(acol[j, i : i + 1, :], shape)
    scale = [lax.rsqrt(a[i, i]) for i in range(cols)]
    for i, j in a:
        a[i, j] = a[i, j] * scale[i] * scale[j]
    right = [
        [spread(half * cols + k) * scale[k] for half in range(2)] for k in range(cols)
    ]
    low = {}
    inverse = []
    for k in range(0, cols, 2):
        p, q, r = a[k, k], a[k + 1, k], a[k + 1, k + 1]
        det = 1.0 / (p * r - q * q)
        p, q, r = r * det, -q * det, p * det
        inverse.append((p, q, r))
        for i in range(k + 2, cols):
            low[i, k] = a[i, k] * p + a[i, k + 1] * q
            low[i, k + 1] = a[i, k] * q + a[i, k + 1] * r
            for j in range(k + 2, i + 1):
                a[i, j] = a[i, j] - (low[i, k] * a[j, k] + low[i, k + 1] * a[j, k + 1])
            right[i] = [
                right[i][h] - (low[i, k] * right[k][h] + low[i, k + 1] * right[k + 1][h])
                for h in range(2)
            ]
    out = [None] * cols
    for k in range(cols - 2, -1, -2):
        p, q, r = inverse[k // 2]
        halves = []
        for h in range(2):
            first = right[k][h] * p + right[k + 1][h] * q
            second = right[k][h] * q + right[k + 1][h] * r
            for i in range(cols - 1, k + 1, -1):
                first = first - low[i, k] * out[i][h]
                second = second - low[i, k + 1] * out[i][h]
            halves.append((first, second))
        out[k] = [halves[0][0], halves[1][0]]
        out[k + 1] = [halves[0][1], halves[1][1]]
    return [
        jnp.concatenate([out[k][0] * scale[k], out[k][1] * scale[k]], 0) for k in range(cols)
    ]


def kernel(
    sizes, groups, dims,
    off_in, ext_in, count_in, proj_in, d_in, x_in, hx_in, p_in, hp_in, v_in, beta_in,
    w_out, hw_out, sums_out, w_ref, hw_ref, sums_ref,
    off_ref, ext_ref, count_ref, proj_ref, acol, d_ref, v_ref, beta_ref,
    stack, zext, ybuf, xr, xl, edge_out, edge_in, edge_v, edge_v_in, edges, inner, nf,
    shared, trim, offs, lines, near0, near1, far0, far1, wside, parts4, parts_in,
    *rest,
):
    cz, cy, cx, slots, nproj, cols = dims
    nz, ny, nx = sizes
    n_red = len(groups)
    slow = (("gx",), ("gz",), ("gy",))
    n_slow = len(slow)
    bufs = (rest[:n_slow], rest[n_slow : n_slow + n_red], rest[n_slow + n_red : n_slow + 2 * n_red])
    rest = rest[n_slow + 2 * n_red :]
    red_send, red_recv, halo_send, halo_recv, atom_send, atom_recv, part_sem = rest[:7]
    load_sem, out_sem, xh, p_ref, hp_ref, raw, raw_v, raw_send, raw_recv, edge_send, edge_recv = rest[7:]
    x_ref, hx_ref = xh.at[0], xh.at[1]
    loads = []
    for i, (source, target) in enumerate(
        (
            (x_in, x_ref), (hx_in, hx_ref), (off_in, off_ref), (ext_in, ext_ref),
            (count_in, count_ref), (proj_in, proj_ref), (v_in, v_ref), (beta_in, beta_ref),
            (p_in, p_ref), (hp_in, hp_ref), (d_in, d_ref),
        )
    ):
        loads.append(pltpu.make_async_copy(source, target, load_sem.at[i]))
        loads[-1].start()
    zi, yi, xi = (lax.axis_index(a) for a in AXES)
    size_of = dict(zip(AXES, sizes))
    here = dict(zip(AXES, (zi, yi, xi)))
    more_z, more_y = BZ - 1, BY - 1
    own = cz * cy
    lane = lax.broadcasted_iota(jnp.int32, (cols, 128), 1)

    def neighbour(dz, dy, dx):
        step = dict(zip(AXES, (dz, dy, dx)))
        return {a: lax.rem(here[a] + step[a] + size_of[a], size_of[a]) for a in AXES}

    def member(group, offset):
        total = 1
        index = 0
        for a in group:
            total *= size_of[a]
            index = index * size_of[a] + here[a]
        target = lax.rem(index + offset, total)
        device = {}
        for a in reversed(group):
            device[a] = lax.rem(target, size_of[a])
            target = target // size_of[a]
        return {a: device.get(a, here[a]) for a in AXES}, index, total

    octant = [(o // 4, o // 2 % 2, o % 2) for o in range(8)]
    around = [
        (dz, dy, dx)
        for dx in (-1, 0, 1) for dz in (-1, 0, 1) for dy in (-1, 0, 1)
        if (dz, dy, dx) != (0, 0, 0)
    ]
    barrier = pltpu.get_barrier_semaphore()
    greeted = 0
    for group in groups:
        total = member(group, 0)[2]
        for offset in range(1, total):
            pl.semaphore_signal(
                barrier, inc=1, device_id=member(group, offset)[0], device_id_type=MESH
            )
            greeted += 1
    for where in around:
        pl.semaphore_signal(
            barrier, inc=1, device_id=neighbour(*where), device_id_type=MESH
        )
        greeted += 1

    def split_store(kind, cell, value):
        high = value.astype(BF16)
        low = (value - high.astype(F32)).astype(BF16)
        start = cell * 128 if isinstance(cell, int) else pl.multiple_of(cell * 128, 128)
        stack[kind * 32 : kind * 32 + 32, pl.ds(start, 128)] = jnp.concatenate([high, low], 0)

    def split_all(*kinds):
        @pl.loop(0, cz)
        def _(z):
            for y in range(cy):
                cell = z * cy + y
                for kind, ref in kinds:
                    split_store(kind, cell, ref[cell])

    for load in loads[:2]:
        load.wait()
    split_all((HX, hx_ref), (XX, x_ref))

    def products(left, right_from, right_to, count=1):
        m = lax.dot_general(
            stack[left * 32 : (left + count) * 32, :],
            stack[right_from * 32 : right_to * 32, :],
            (((1,), (1,)), ((), ())),
            preferred_element_type=F32,
        )
        parts = [m[32 * i : 32 * i + cols] + m[32 * i + cols : 32 * i + 32] for i in range(count)]
        return parts if count > 1 else parts[0]

    def reduced(which, payload):
        for phase, group in enumerate(slow if which == 0 else groups):
            buf = bufs[which][phase]
            _, index, total = member(group, 0)
            at = phase + (which and len(slow) + (which - 1) * n_red)
            send_sem, recv_sem = red_send.at[at], red_recv.at[at]
            buf[index] = payload
            if phase == 0 and which == 2:
                pl.semaphore_wait(barrier, greeted)
            for offset in range(1, total):
                pltpu.make_async_remote_copy(
                    src_ref=buf.at[index],
                    dst_ref=buf.at[index],
                    send_sem=send_sem,
                    recv_sem=recv_sem,
                    device_id=member(group, offset)[0],
                    device_id_type=MESH,
                ).start()
            yield None
            most = buf.at[pl.ds(0, total - 1)]
            for sem in (recv_sem, send_sem):
                pltpu.make_async_copy(most, most, sem).wait()
            payload = buf[0]
            for slot in range(1, total):
                payload = payload + buf[slot]
        yield payload

    def finish(steps):
        out = None
        for out in steps:
            pass
        return out

    both = lax.dot_general(
        stack[HX * 32 : XX * 32 + 32, :], stack[XX * 32 : XX * 32 + 32, :],
        (((1,), (1,)), ((), ())), preferred_element_type=F32,
    )
    both = jnp.concatenate([both, jnp.zeros((64, 96), F32)], 1)
    turn_hx = both[:cols] + both[cols:32]
    corr = both[32 : 32 + cols] + both[32 + cols :]
    narrow = lax.broadcasted_iota(jnp.int32, (8, 128), 1)

    def merged(tile):
        return tile + pltpu.roll(tile, 128 - cols, 1)

    payload0 = jnp.where(narrow < cols, merged(turn_hx[:8]), 0.0)
    for at, tile in ((1, turn_hx[8:]), (2, corr[:8]), (3, corr[8:])):
        moved = pltpu.roll(merged(tile), at * cols, 1)
        payload0 = jnp.where((narrow >= at * cols) & (narrow < at * cols + cols), moved, payload0)
    solving = reduced(2, payload0)
    next(solving)
    for load in loads[2:]:
        load.wait()
    lane8 = lax.broadcasted_iota(jnp.int32, (8, 128), 1)
    rows = slots * nproj
    pairs = rows // 8
    columns = BZ * BY * BX // 128
    box_lane = lax.broadcasted_iota(jnp.int32, (nproj, BZ * BY * BX), 1)
    box_row = lax.broadcasted_iota(jnp.int32, (nproj, BZ * BY * BX), 0)
    box_a, box_b, box_c = box_lane // (BY * BX), box_lane // BX % BY, box_lane % BX
    for s in range(slots):
        kept = jnp.where(s < count_ref[0, 0, 0], proj_ref[0, s], 0)
        inside = (
            (box_row < kept)
            & (box_a < ext_ref[0, 0, 0, 0, s])
            & (box_b < ext_ref[1, 0, 0, 0, s])
            & (box_c < ext_ref[2, 0, 0, 0, s])
        )
        at = s * nproj
        kept = jnp.where(inside, beta_ref[s], 0.0)
        for c in range(columns):
            where = (0, at // 8 * columns + c, slice(at % 8, at % 8 + nproj), slice(None))
            shared[where] = kept[:, c * 128 : c * 128 + 128]
    lane1 = lax.broadcasted_iota(jnp.int32, (1, 128), 1)
    lane16 = lax.broadcasted_iota(jnp.int32, (nproj, 128), 1)
    slot_at = lane16 % 64 // 16 * (8 // nproj) + lane16 % 8 // nproj
    table = []
    for p in range(nproj):
        mirrored = jnp.concatenate([d_ref[q, p : p + 1, :] for q in range(nproj)], 0)
        sym = 0.5 * (d_ref[p] + mirrored)
        spread = jnp.zeros((nproj, 128), F32)
        for s in range(slots):
            value = jnp.broadcast_to(sym[:, s : s + 1], (nproj, 128))
            spread = jnp.where(slot_at == s, value, spread)
        table.append(spread)
    for d in range(-nproj + 1, nproj):
        row = jnp.zeros((1, 128), F32)
        for p in range(max(0, -d), min(nproj, nproj - d)):
            row = jnp.where(lane1 % nproj == p, table[p][p + d : p + d + 1, :], row)
        shared[0, pairs * columns, d + nproj - 1 : d + nproj, :] = row
    for pair in range(0, pairs, 2):
        lasts = []
        for p in (pair, pair + 1):
            first, last = shared[0, p * columns], shared[0, p * columns + 1]
            lasts.append(last)
            trim[p] = jnp.where(
                lane8 < 48, pltpu.roll(first, 112, 1),
                jnp.where(lane8 < 96, pltpu.roll(first, 96, 1), pltpu.roll(last, 80, 1)),
            )
        trim[pairs + pair // 2] = jnp.where(
            lane8 < 64,
            jnp.where(lane8 < 16, pltpu.roll(lasts[0], 80, 1), pltpu.roll(lasts[0], 64, 1)),
            jnp.where(lane8 < 80, pltpu.roll(lasts[1], 16, 1), lasts[1]),
        )
    trim[pairs + pairs // 2] = shared[0, pairs * columns]
    atom_copies = {}
    for o in (4, 2, 1, 6, 5, 3, 7):
        atom_copies[o] = [
            pltpu.make_async_remote_copy(
                src_ref=source,
                dst_ref=target,
                send_sem=atom_send.at[2 * (o - 1) + i],
                recv_sem=atom_recv.at[2 * (o - 1) + i],
                device_id=neighbour(*octant[o]),
                device_id_type=MESH,
            )
            for i, (source, target) in enumerate(
                (
                    (off_ref, offs.at[o - 1]),
                    (trim, shared.at[o, pl.ds(0, pairs + pairs // 2 + 1)])
                    if octant[o][1] else (shared.at[0], shared.at[o]),
                )
            )
        ]
        for copy in atom_copies[o]:
            copy.start()
    split_all((HP, hp_ref), (PP, p_ref))
    hx_row, x_row, p_row = products(HX, HP, WW, 3)
    first = jnp.where((lane >= 32) & (lane < 64), pltpu.roll(hx_row, 96, 1), x_row)

    def paired(upper, lower):
        upper = upper + pltpu.roll(upper, 112, 1)
        lower = lower + pltpu.roll(lower, 112, 1)
        return jnp.where(lane % 32 < 16, upper, pltpu.roll(lower, 16, 1))

    reduction = reduced(0, paired(first, p_row))

    row8 = lax.broadcasted_iota(jnp.int32, (8, 128), 0)
    in_tile = 128 // BX
    width = BY + cy - 1
    ahead = cy - 1
    nothing = ahead + slots * BZ * width + ahead
    tables = {(0, 0): near0, (0, 1): near1, (1, 0): far0, (1, 1): far1}
    blank_line = jnp.zeros((8, 128), F32)

    @pl.loop(0, slots * BZ)
    def _(block):
        for b in range(BY, width):
            lines[ahead + block * width + b] = blank_line

    for at in [*range(ahead), *range(nothing - ahead, nothing + width)]:
        lines[at] = blank_line

    def build(o):
        dz, dy, dx = octant[o]

        def expand(pair):
            if dy:
                tiles = [shared[o, pair], shared[o, pairs + pair // 2]]
            else:
                tiles = [shared[o, pair * columns + c] for c in range(columns)]
            places = {}
            for at in range(BZ * BY):
                a, b = at // BY, at % BY
                if not dy:
                    places[at] = at // in_tile, at % in_tile
                elif b and a * (BY - 1) + b - 1 < in_tile:
                    places[at] = 0, a * (BY - 1) + b - 1
                elif b:
                    places[at] = 1, pair % 2 * (in_tile // 2) + a * (BY - 1) + b - 1 - in_tile
            for half in range(8 // nproj):
                s = pair * (8 // nproj) + half
                ox = offset(2, s)
                along = (lane8 - ox + 128) & 127
                side = lane8 < ox if dx else lane8 >= ox
                keep = (along < BX) & side & (row8 // nproj == half)
                for at, (tile, k) in places.items():
                    shift = (ox + 128 - BX * k) & 127
                    part = jnp.where(keep, pltpu.roll(tiles[tile], shift, 1), 0.0)
                    lines[ahead + (s * BZ + at // BY) * width + at % BY] = part

        def offset(axis, s):
            return off_ref[axis, 0, 0, 0, s] if o == 0 else offs[o - 1, axis, 0, 0, 0, s]

        for pair in range(pairs):
            expand(pair)

        target = tables[dz, dy]
        top = dx * 64
        ys = more_y if dy else cy

        @pl.loop(0, more_z if dz else cz)
        def _(z):
            starts = []
            for s in range(slots):
                a = z + dz * cz - offset(0, s)
                ok = (a >= 0) & (a < BZ)
                start = jnp.where(ok, ahead + (s * BZ + a) * width - offset(1, s), nothing - offset(1, s))
                starts.append(start)
            for y in range(ys):
                column = pl.ds(pl.multiple_of((z * ys + y) * 128, 128), 128)
                for pair in range(pairs):
                    at = top + pair * 16
                    total = None
                    for half in range(8 // nproj):
                        start = starts[pair * (8 // nproj) + half] + (y + dy * cy)
                        part = lines[start]
                        total = part if total is None else total + part
                    high = total.astype(BF16)
                    low = (total - high.astype(F32)).astype(BF16)
                    target[at : at + 16, column] = jnp.concatenate([high, low], 0)

    for z in range(cz):
        for y in range(cy):
            inner[z, y] = jnp.zeros((cols, 128), F32)
            inner[2 * cz + z, y] = jnp.zeros((cols, 128), F32)
    def build_all(owners):
        for o in owners:
            for copy in atom_copies[o]:
                copy.wait()
            build(o)

    build(0)
    early_z = cz // 3
    early_to = [(-1, 0, 0), (1, 0, 0), (0, -1, 0)] + ([] if ny == 2 else [(0, 1, 0)])
    raw_copies = []
    for d, where in enumerate(early_to):
        for i, (source, target) in enumerate(
            (
                (xh.at[:, pl.ds(0, early_z * cy)], raw.at[d]),
                (v_ref.at[pl.ds(0, early_z)], raw_v.at[d]),
            )
        ):
            raw_copies.append(
                pltpu.make_async_remote_copy(
                    src_ref=source,
                    dst_ref=target,
                    send_sem=raw_send.at[2 * d + i],
                    recv_sem=raw_recv.at[2 * d + i],
                    device_id=neighbour(*where),
                    device_id_type=MESH,
                )
            )
            raw_copies[-1].start()
    def packed(read, rows_of):
        at_lane = lax.broadcasted_iota(jnp.int32, (rows_of, 128), 1)
        for q in range(tiles_of(own)):
            low = jnp.zeros((rows_of, 128), F32)
            high = low
            for j in range(min(PER_TILE, own - PER_TILE * q)):
                tile = read(PER_TILE * q + j)
                keep = (at_lane >= EDGE * j) & (at_lane < EDGE * j + EDGE)
                low = jnp.where(keep, pltpu.roll(tile, EDGE * j, 1) if j else tile, low)
                turn = (EDGE * j + EDGE) % 128
                high = jnp.where(keep, pltpu.roll(tile, turn, 1) if turn else tile, high)
            yield q, low, high

    edge_v[...] = jnp.zeros(edge_v.shape, F32)
    for kind in range(2):
        for q, low, high in packed(lambda cell: xh[kind, cell], cols):
            edge_out[0, kind, q] = low
            edge_out[1, kind, q] = high
    for q, low, high in packed(lambda cell: v_ref[cell // cy, cell % cy : cell % cy + 1, :], 1):
        edge_v[0, q : q + 1, :] = low
        edge_v[1, q : q + 1, :] = high
    next(solving)
    next(reduction)
    edge_copies = []
    for side, step in enumerate((-1, 1)):
        for i, (source, target) in enumerate(
            ((edge_out.at[side], edge_in.at[side]), (edge_v.at[side], edge_v_in.at[side]))
        ):
            edge_copies.append(
                pltpu.make_async_remote_copy(
                    src_ref=source,
                    dst_ref=target,
                    send_sem=edge_send.at[2 * side + i],
                    recv_sem=edge_recv.at[2 * side + i],
                    device_id=neighbour(0, 0, step),
                    device_id_type=MESH,
                )
            )
            edge_copies[-1].start()
    build_all((4, 2, 6, 1, 5, 3, 7))
    sums0 = finish(solving)
    sums0 = solved(sums0, cols, acol)
    theta_cols = sums0

    @pl.loop(0, cz)
    def _(z):
        for y in range(cy):
            cell = z * cy + y
            xs = x_ref[cell]
            value = hx_ref[cell]
            for k in range(cols):
                value = value - theta_cols[k] * xs[k : k + 1, :]
            vv = v_ref[z, y : y + 1, :]
            value = value * (1.0 / (1.0 + vv * vv))
            zext[cz + z, y] = value
            inner[cz + z, y] = value
            w_ref[cell] = value
            split_store(WW, cell, value)
            if y < more_y:
                place = pl.ds(pl.multiple_of((z * more_y + y) * 128, 128), 128)
                high = value.astype(BF16)
                low = (value - high.astype(F32)).astype(BF16)
                wside[:, place] = jnp.concatenate([high, low], 0)

    two_y = ny == 2
    split = early_z + (cz - early_z) // 2

    def some(ref, z, dz, y, dy):
        return ref.at[pl.ds(z, dz), pl.ds(y, dy)]

    def layers(target, base, z, dz, where):
        return some(zext, cz + z, dz, 0, cy), some(target, base + z, dz, 0, cy), where

    def bulk(z, dz):
        sends = [
            layers(zext, 2 * cz, z, dz, (-1, 0, 0)),
            layers(zext, 0, z, dz, (1, 0, 0)),
            layers(ybuf.at[1], 0, z, dz, (0, -1, 0)),
        ]
        if not two_y:
            sends.append(layers(ybuf.at[0], 0, z, dz, (0, 1, 0)))
        return sends

    early = bulk(early_z, split - early_z)
    late = bulk(split, cz - split)

    def launch(sends, send_sem, recv_sem, first=0):
        copies = []
        for i, (source, target, where) in enumerate(sends, start=first):
            copies.append(
                pltpu.make_async_remote_copy(
                    src_ref=source,
                    dst_ref=target,
                    send_sem=send_sem.at[i],
                    recv_sem=recv_sem.at[i],
                    device_id=neighbour(*where),
                    device_id_type=MESH,
                )
            )
            copies[-1].start()
        return copies

    copies = launch(early, halo_send, halo_recv)
    outs = [
        pltpu.make_async_copy(source, target, out_sem.at[i])
        for i, (source, target) in enumerate(
            ((w_ref, w_out), (hw_ref, hw_out), (sums_ref, sums_out))
        )
    ]
    outs[0].start()
    def span(step):
        return (max(0, -step), 2 - abs(step))

    slot_of = {}
    filled = 0
    for where in around:
        slot_of[where] = filled
        filled += span(where[0])[1] * span(where[1])[1] * span(where[2])[1]
    def hand_out(z, y):
        for where in around:
            (z0, zn), (y0, yn), (x0, xn) = (span(step) for step in where)
            if z0 <= z < z0 + zn and y0 <= y < y0 + yn:
                at = slot_of[where] + ((z - z0) * yn + y - y0) * xn
                pltpu.make_async_remote_copy(
                    src_ref=parts4.at[z, y, pl.ds(x0, xn)],
                    dst_ref=parts_in.at[pl.ds(at, xn)],
                    send_sem=part_sem.at[0],
                    recv_sem=part_sem.at[1],
                    device_id=neighbour(*where),
                    device_id_type=MESH,
                ).start()

    w_rows = stack.at[WW * 32 : WW * 32 + 32]
    lane4 = lax.broadcasted_iota(jnp.int32, (4, 128), 1)
    for early_tiles in (((1, 1), (1, 0), (0, 1)), ((0, 0),)):
        for dz, dy in early_tiles:
            table = tables[dz, dy]
            source = wside if dy else w_rows
            m = lax.dot_general(
                table[...], source[:, : table.shape[1]],
                (((1,), (1,)), ((), ())), preferred_element_type=F32,
            )
            m = jnp.concatenate([m, jnp.zeros((128, 128 - 2 * cols), F32)], 1)
            m = jnp.transpose(m)
            m = m[:cols] + m[cols : 2 * cols]
            m = m + pltpu.roll(m, 128 - 8, 1)
            upper, lower = m[:8], m[8:]
            both = jnp.where(lane8 % 16 < 8, upper, pltpu.roll(lower, 8, 1))
            moved = pltpu.roll(both, 64, 1)
            parts4[dz, dy, 0] = jnp.where(lane4 < 64, both[:4], moved[4:])
            parts4[dz, dy, 1] = jnp.where(lane4 < 64, moved[:4], both[4:])
        for dz, dy in early_tiles:
            hand_out(dz, dy)

    late_copies = launch(late, halo_send, halo_recv, len(early))
    w_row = products(WW, HP, WW)
    w_row2 = products(WW, XX, HW)
    for copy in edge_copies:
        copy.wait()
    for side, target in enumerate((xr, xl)):
        for q in range(tiles_of(own)):
            value = edge_in[side, 1, q]
            xs = edge_in[side, 0, q]
            for k in range(cols):
                value = value - theta_cols[k] * xs[k : k + 1, :]
            vv = edge_v_in[side, q : q + 1, :]
            target[q] = value * (1.0 / (1.0 + vv * vv))
    for copy in raw_copies:
        copy.wait()
    for d in range(len(early_to)):
        target, base = ((zext, 2 * cz), (zext, 0), (ybuf.at[1], 0), (ybuf.at[0], 0))[d]

        @pl.loop(0, early_z)
        def _(z):
            for y in range(cy):
                cell = z * cy + y
                xs = raw[d, 0, cell]
                value = raw[d, 1, cell]
                for k in range(cols):
                    value = value - theta_cols[k] * xs[k : k + 1, :]
                vv = raw_v[d, z, y : y + 1, :]
                target[base + z, y] = value * (1.0 / (1.0 + vv * vv))

    @pl.loop(0, cz)
    def _(z):
        for y in range(cy):
            centre = inner[cz + z, y]
            vv = v_ref[z, y : y + 1, :]
            total = centre * (vv - 1.5 * LAP_CENTER)
            for k, weight in enumerate(LAP_COEFFS, start=1):
                tiles = [inner[cz + z, t] for t in (y + k, y - k) if 0 <= t < cy]
                if k < cz:
                    tiles += [inner[cz + z + k, y], inner[cz + z - k, y]]
                beside = None
                for tile in tiles:
                    beside = tile if beside is None else beside + tile
                if beside is not None:
                    total = total - 0.5 * weight * beside
            hw_ref[z * cy + y] = total

    for cell in range(own):
        left, right = xl[cell // PER_TILE], xr[cell // PER_TILE]
        turn = (256 - EDGE - EDGE * (cell % PER_TILE)) % 128
        left = pltpu.roll(left, turn, 1) if turn else left
        shift = (128 - EDGE * (cell % PER_TILE)) % 128
        right = pltpu.roll(right, shift, 1) if shift else right
        edges[cell] = jnp.where(lane < 64, right, left)

    @pl.loop(0, cz)
    def _(z):
        for y in range(cy):
            cell = z * cy + y
            edge = edges[cell]
            centre = inner[cz + z, y]
            total = hw_ref[cell]
            for k, weight in enumerate(LAP_COEFFS, start=1):
                beside = pltpu.roll(jnp.where(lane < k, edge, centre), 128 - k, 1)
                beside = beside + pltpu.roll(jnp.where(lane >= 128 - k, edge, centre), k, 1)
                total = total - 0.5 * weight * beside
            hw_ref[cell] = total
    next(reduction)
    for sem in (part_sem.at[1], part_sem.at[0]):
        pltpu.make_async_copy(parts_in, parts_in, sem).wait()
    gathered = {}
    for dz in range(2):
        for dy in range(2):
            sums = []
            for dx in range(2):
                total = None
                for from_z in range(2):
                    for from_y in range(2):
                        for from_x in range(2):
                            where = (dz - from_z, dy - from_y, dx - from_x)
                            if where == (0, 0, 0):
                                tile = parts4[dz, dy, dx]
                            else:
                                (z0, _), (y0, yn), (x0, xn) = (span(step) for step in where)
                                at = ((from_z - z0) * yn + from_y - y0) * xn + from_x - x0
                                tile = parts_in[slot_of[where] + at]
                            total = tile if total is None else total + tile
                sums.append(total)
            turned = [pltpu.roll(total, 64, 1) for total in sums]
            gathered[dz, dy] = jnp.concatenate(
                [
                    jnp.where(lane4 < 64, sums[0], turned[1]),
                    jnp.where(lane4 < 64, turned[0], sums[1]),
                ],
                0,
            )
    coef_at = (pairs * columns, pairs + pairs // 2)
    lefts = {}
    for dz in range(2):
        for dy in range(2):
            total = gathered[dz, dy]
            o = dz * 4 + dy * 2
            coefs = jnp.where(
                lane8 < 64, shared[o, coef_at[dy]], shared[o + 1, coef_at[dy]]
            )
            mixed = None
            for d in range(-nproj + 1, nproj):
                term = pltpu.roll(total, (128 - d) % 128, 1) if d else total
                term = term * coefs[d + nproj - 1 : d + nproj, :]
                mixed = term if mixed is None else mixed + term
            low_half = lane8 % 16 < 8
            mixed = jnp.concatenate(
                [
                    jnp.where(low_half, mixed, pltpu.roll(mixed, 8, 1)),
                    jnp.where(low_half, pltpu.roll(mixed, 120, 1), mixed),
                ],
                0,
            )
            high = mixed.astype(BF16)
            low = (mixed - high.astype(F32)).astype(BF16)
            lefts[dz, dy] = jnp.concatenate([high, low], 0)

    for z in range(cz):
        sums = {}
        for dz in range(2 if z < more_z else 1):
            for dy in range(2):
                ys = more_y if dy else cy
                m = lax.dot_general(
                    lefts[dz, dy], tables[dz, dy][:, z * ys * 128 : (z + 1) * ys * 128],
                    (((1,), (0,)), ((), ())), preferred_element_type=F32,
                )
                m = m[:cols] + m[cols:]
                for y in range(ys):
                    part = m[:, y * 128 : y * 128 + 128]
                    sums[y] = sums[y] + part if y in sums else part
        for y in range(cy):
            nf[z, y] = sums[y]
    for copy in copies + late_copies:
        copy.wait()
    hw_sum = None
    for cell in range(own):
        z, y = cell // cy, cell % cy
        total = hw_ref[cell] + nf[z, y]
        weights = {}
        for k, weight in enumerate(LAP_COEFFS, start=1):
            keys = [("z", z + k), ("z", z - k), (1, y + k - cy), (1 if two_y else 0, y - k + cy)]
            for key, inside in zip(keys, (z + k < cz, z - k >= 0, y + k < cy, y - k >= 0)):
                if not inside:
                    weights[key] = weights.get(key, 0.0) - 0.5 * weight
        for (where, at), weight in weights.items():
            tile = zext[cz + at, y] if where == "z" else ybuf[where, z, at]
            total = total + weight * tile
        hw_ref[cell] = total
        split_store(HW, cell, total)
        if y == cy - 1:
            plane = slice(z * cy * 128, (z + 1) * cy * 128)
            part = lax.dot_general(
                stack[HW * 32 : HW * 32 + 32, plane], stack[XX * 32 : HW * 32, plane],
                (((1,), (1,)), ((), ())), preferred_element_type=F32,
            )
            hw_sum = part if hw_sum is None else hw_sum + part
    outs[1].start()
    hw_row = w_row2_pad(hw_sum[:cols] + hw_sum[cols:])
    second = jnp.where(lane < 96, hw_row, pltpu.roll(w_row2_pad(w_row2), 32, 1))
    closing = reduced(1, paired(w_row, second))
    next(closing)
    next(reduction)
    next(closing)
    sums1 = next(reduction)
    sums2 = finish(closing)
    sums_ref[...] = jnp.concatenate([sums1, sums2], 0)
    outs[2].start()
    for out in outs:
        out.wait()


def finish_out(weight, w_ref, hw_ref, sums_ref, w_out, hw_out, gram_out, ray_out, gram_ref, ray_ref, sems):
    copies = [
        pltpu.make_async_copy(source, target, sems.at[i])
        for i, (source, target) in enumerate(
            ((w_ref, w_out), (hw_ref, hw_out), (gram_ref, gram_out), (ray_ref, ray_out))
        )
    ]
    for copy in copies[:2]:
        copy.start()
    sums1, sums2 = sums_ref[:16], sums_ref[16:]
    lane = lax.broadcasted_iota(jnp.int32, (16, 128), 1)
    rows = jnp.concatenate([sums1, pltpu.roll(sums1, 112, 1), sums2, pltpu.roll(sums2, 112, 1)], 0)
    rows = rows * weight
    turned = jnp.transpose(jnp.concatenate([rows, jnp.zeros_like(rows)], 0))

    def direct(row, group, target):
        return rows[16 * row : 16 * row + 16, :], 32 * group, target

    def flipped(row, group, target):
        return turned[32 * group : 32 * group + 16, :], 16 * row, target

    def laid(parts):
        total = None
        for tile, begin, target in parts:
            shift = (16 * target - begin) % 128
            tile = pltpu.roll(tile, shift, 1) if shift else tile
            tile = jnp.where((lane >= 16 * target) & (lane < 16 * target + 16), tile, 0.0)
            total = tile if total is None else total + tile
        return total

    gram = [
        [direct(0, 2, 0), flipped(2, 2, 1), direct(0, 3, 2)],
        [direct(2, 2, 0), direct(3, 3, 1), direct(2, 3, 2)],
        [direct(1, 2, 0), flipped(2, 3, 1), direct(1, 3, 2)],
    ]
    rayleigh = [
        [flipped(0, 1, 0), flipped(3, 0, 1), direct(0, 0, 2)],
        [direct(2, 1, 0), flipped(3, 2, 1), direct(2, 0, 2)],
        [direct(1, 1, 0), flipped(3, 1, 1), direct(1, 0, 2)],
    ]
    for i in range(3):
        gram_ref[16 * i : 16 * i + 16, :] = laid(gram[i])[:, :48]
        ray_ref[16 * i : 16 * i + 16, :] = laid(rayleigh[i])[:, :48]
    for copy in copies[2:]:
        copy.start()
    for copy in copies:
        copy.wait()


def w_row2_pad(row):
    return jnp.concatenate([row, jnp.zeros((row.shape[0], 128 - row.shape[1]), row.dtype)], 1)


def per_device(
    sizes,
    block_x, block_hx, block_p, block_hp, potential, projectors, coupling,
    atom_count, proj_count, offsets, extents,
):
    cols, cz, cy, cx = block_x.shape
    slots, nproj = projectors.shape[-3], projectors.shape[-2]
    nz, ny, nx = sizes
    own = cz * cy
    turned = [
        jnp.transpose(b, (1, 2, 0, 3)).reshape(own, cols, cx)
        for b in (block_x, block_hx, block_p, block_hp)
    ]
    groups = (("gz", "gy"), ("gx",)) if nz * ny <= 16 else (("gz",), ("gy",), ("gx",))
    size_of = dict(zip(AXES, sizes))
    totals = []
    for group in groups:
        total = 1
        for a in group:
            total *= size_of[a]
        totals.append(total)
    tile = (cols, 128)
    rows = slots * nproj
    scratch = [
        pltpu.VMEM((own,) + tile, F32),
        pltpu.VMEM((own,) + tile, F32),
        pltpu.VMEM((2 * cols, 128), F32),
        pltpu.SMEM(offsets.shape, jnp.int32),
        pltpu.SMEM(extents.shape, jnp.int32),
        pltpu.SMEM(atom_count.shape, jnp.int32),
        pltpu.SMEM(proj_count.shape[2:], jnp.int32),
        pltpu.VMEM((cols, cols, 128), F32),
        pltpu.VMEM((nproj, nproj, slots), F32),
        pltpu.VMEM(potential.shape, F32),
        pltpu.VMEM(projectors.shape[3:], F32),
        pltpu.VMEM((192, own * 128), BF16),
        pltpu.VMEM((3 * cz, cy) + tile, F32),
        pltpu.VMEM((2, cz, cy) + tile, F32),
        pltpu.VMEM((tiles_of(own),) + tile, F32),
        pltpu.VMEM((tiles_of(own),) + tile, F32),
        pltpu.VMEM((2, 2, tiles_of(own)) + tile, F32),
        pltpu.VMEM((2, 2, tiles_of(own)) + tile, F32),
        pltpu.VMEM((2, 8 * (-(-tiles_of(own) // 8)), 128), F32),
        pltpu.VMEM((2, 8 * (-(-tiles_of(own) // 8)), 128), F32),
        pltpu.VMEM((own,) + tile, F32),
        pltpu.VMEM((3 * cz, cy) + tile, F32),
        pltpu.VMEM((cz, cy) + tile, F32),
        pltpu.VMEM((8, rows // 8 * (BZ * BY * BX // 128) + 1, 8, 128), F32),
        pltpu.VMEM((rows // 8 + rows // 16 + 1, 8, 128), F32),
        pltpu.SMEM((7,) + offsets.shape, jnp.int32),
        pltpu.VMEM((slots * BZ * (BY + cy - 1) + BY + 3 * (cy - 1), 8, 128), F32),
        pltpu.VMEM((128, own * 128), BF16),
        pltpu.VMEM((128, cz * (BY - 1) * 128), BF16),
        pltpu.VMEM((128, (BZ - 1) * cy * 128), BF16),
        pltpu.VMEM((128, (BZ - 1) * (BY - 1) * 128), BF16),
        pltpu.VMEM((2 * cols, cz * (BY - 1) * 128), BF16),
        pltpu.VMEM((2, 2, 2, 4, 128), F32),
        pltpu.VMEM((56, 4, 128), F32),
    ]
    scratch += [pltpu.VMEM((size_of[a], cols, 128), F32) for a in ("gx", "gz", "gy")]
    scratch += [pltpu.VMEM((t, cols, 128), F32) for t in totals]
    scratch += [pltpu.VMEM((t, 8, 128), F32) for t in totals]
    scratch += [
        pltpu.SemaphoreType.DMA((3 + 2 * len(groups),)),
        pltpu.SemaphoreType.DMA((3 + 2 * len(groups),)),
        pltpu.SemaphoreType.DMA((8,)),
        pltpu.SemaphoreType.DMA((8,)),
        pltpu.SemaphoreType.DMA((14,)),
        pltpu.SemaphoreType.DMA((14,)),
        pltpu.SemaphoreType.DMA((2,)),
        pltpu.SemaphoreType.DMA((11,)),
        pltpu.SemaphoreType.DMA((3,)),
    ]
    ways = 3 if ny == 2 else 4
    early_z = cz // 3
    scratch += [
        pltpu.VMEM((2, own) + tile, F32),
        pltpu.VMEM((own,) + tile, F32),
        pltpu.VMEM((own,) + tile, F32),
        pltpu.VMEM((ways, 2, early_z * cy) + tile, F32),
        pltpu.VMEM((ways, early_z, cy, 128), F32),
        pltpu.SemaphoreType.DMA((2 * ways,)),
        pltpu.SemaphoreType.DMA((2 * ways,)),
        pltpu.SemaphoreType.DMA((4,)),
        pltpu.SemaphoreType.DMA((4,)),
    ]
    vmem = pl.BlockSpec(memory_space=pltpu.VMEM)
    w, hw, sums = pl.pallas_call(
        functools.partial(kernel, sizes, groups, (cz, cy, cx, slots, nproj, cols)),
        out_shape=(
            pltpu.VMEM((own,) + tile, F32),
            pltpu.VMEM((own,) + tile, F32),
            pltpu.VMEM((2 * cols, 128), F32),
        ),
        in_specs=[pl.BlockSpec(memory_space=pltpu.HBM)] * 11,
        out_specs=(pl.BlockSpec(memory_space=pl.ANY),) * 3,
        scratch_shapes=scratch,
        compiler_params=pltpu.CompilerParams(
            collective_id=0, has_side_effects=True, vmem_limit_bytes=VMEM_LIMIT
        ),
    )(
        offsets, extents, atom_count, proj_count[0, 0],
        jnp.transpose(coupling[0, 0, 0], (1, 2, 0)),
        *turned, potential, projectors[0, 0, 0],
    )
    square = jax.ShapeDtypeStruct((3 * cols, 3 * cols), F32)
    field = jax.ShapeDtypeStruct((own,) + tile, F32)
    w, hw, gram, rayleigh = pl.pallas_call(
        functools.partial(finish_out, 1.0 / (own * cx * nz * ny * nx)),
        out_shape=(field, field, square, square),
        in_specs=[vmem] * 3,
        out_specs=(pl.BlockSpec(memory_space=pl.ANY),) * 4,
        scratch_shapes=[
            pltpu.VMEM(square.shape, F32),
            pltpu.VMEM(square.shape, F32),
            pltpu.SemaphoreType.DMA((4,)),
        ],
        compiler_params=pltpu.CompilerParams(vmem_limit_bytes=4 << 20),
    )(w, hw, sums)
    w, hw = (jnp.transpose(b.reshape(cz, cy, cols, cx), (2, 0, 1, 3)) for b in (w, hw))
    return (w, hw, gram, rayleigh)


def solution(mesh):
    sizes = tuple(mesh.shape[a] for a in AXES)
    in_specs = (
        P(None, "gz", "gy", "gx"),
        P(None, "gz", "gy", "gx"),
        P(None, "gz", "gy", "gx"),
        P(None, "gz", "gy", "gx"),
        P("gz", "gy", "gx"),
        P("gz", "gy", "gx", None, None, None),
        P("gz", "gy", "gx", None, None, None),
        P("gz", "gy", "gx"),
        P("gz", "gy", "gx", None),
        P(None, "gz", "gy", "gx", None),
        P(None, "gz", "gy", "gx", None),
    )
    out_specs = (P(None, "gz", "gy", "gx"), P(None, "gz", "gy", "gx"), P(), P())
    return jax.shard_map(
        functools.partial(per_device, sizes),
        mesh=mesh, in_specs=in_specs, out_specs=out_specs, check_vma=False,
    )
```

```python
import functools

import jax
import jax.numpy as jnp
from jax import lax
from jax.experimental import pallas as pl
from jax.experimental.pallas import tpu as pltpu
from jax.sharding import PartitionSpec as P

BZ, BY, BX = 4, 4, 16
LAP_CENTER = -5369.0 / 1800.0
LAP_COEFFS = (12.0 / 7.0, -15.0 / 56.0, 10.0 / 189.0, -1.0 / 112.0, 2.0 / 1925.0, -1.0 / 16632.0)
MESH = pl.DeviceIdType.MESH
VMEM_LIMIT = (63 << 20) - (64 << 10)
AXES = ("gz", "gy", "gx")
F32 = jnp.float32
BF16 = jnp.bfloat16
HP, HX, XX, PP, WW, HW = range(6)


EDGE = 8
PER_TILE = 128 // EDGE


def tiles_of(count):
    return -(-count // PER_TILE)


def solved(packed, cols, acol):
    shape = (8, 128)

    def spread(lane_at):
        return jnp.broadcast_to(packed[:, lane_at : lane_at + 1], shape)

    for j in range(cols):
        if j < 8:
            acol[j, 0:8] = spread(2 * cols + j)
        acol[j, 8:16] = spread(3 * cols + j)
    a = {}
    for j in range(cols):
        for i in range(j, cols):
            a[i, j] = jnp.broadcast_to(acol[j, i : i + 1, :], shape)
    scale = [lax.rsqrt(a[i, i]) for i in range(cols)]
    for i, j in a:
        a[i, j] = a[i, j] * scale[i] * scale[j]
    right = [
        [spread(half * cols + k) * scale[k] for half in range(2)] for k in range(cols)
    ]
    low = {}
    inverse = []
    for k in range(0, cols, 2):
        p, q, r = a[k, k], a[k + 1, k], a[k + 1, k + 1]
        det = 1.0 / (p * r - q * q)
        p, q, r = r * det, -q * det, p * det
        inverse.append((p, q, r))
        for i in range(k + 2, cols):
            low[i, k] = a[i, k] * p + a[i, k + 1] * q
            low[i, k + 1] = a[i, k] * q + a[i, k + 1] * r
            for j in range(k + 2, i + 1):
                a[i, j] = a[i, j] - (low[i, k] * a[j, k] + low[i, k + 1] * a[j, k + 1])
            right[i] = [
                right[i][h] - (low[i, k] * right[k][h] + low[i, k + 1] * right[k + 1][h])
                for h in range(2)
            ]
    out = [None] * cols
    for k in range(cols - 2, -1, -2):
        p, q, r = inverse[k // 2]
        halves = []
        for h in range(2):
            first = right[k][h] * p + right[k + 1][h] * q
            second = right[k][h] * q + right[k + 1][h] * r
            for i in range(cols - 1, k + 1, -1):
                first = first - low[i, k] * out[i][h]
                second = second - low[i, k + 1] * out[i][h]
            halves.append((first, second))
        out[k] = [halves[0][0], halves[1][0]]
        out[k + 1] = [halves[0][1], halves[1][1]]
    return [
        jnp.concatenate([out[k][0] * scale[k], out[k][1] * scale[k]], 0) for k in range(cols)
    ]


def kernel(
    sizes, groups, dims,
    off_in, ext_in, count_in, proj_in, d_in, x_in, hx_in, p_in, hp_in, v_in, beta_in,
    w_out, hw_out, sums_out, w_ref, hw_ref, sums_ref,
    off_ref, ext_ref, count_ref, proj_ref, acol, d_ref, v_ref, beta_ref,
    stack, zext, ybuf, xr, xl, edge_out, edge_in, edge_v, edge_v_in, edges, inner, nf,
    shared, trim, offs, lines, near0, near1, far0, far1, wside, parts4, parts_in,
    *rest,
):
    cz, cy, cx, slots, nproj, cols = dims
    nz, ny, nx = sizes
    n_red = len(groups)
    slow = (("gx",), ("gz",), ("gy",))
    n_slow = len(slow)
    bufs = (rest[:n_slow], rest[n_slow : n_slow + n_red], rest[n_slow + n_red : n_slow + 2 * n_red])
    rest = rest[n_slow + 2 * n_red :]
    red_send, red_recv, halo_send, halo_recv, atom_send, atom_recv, part_sem = rest[:7]
    load_sem, out_sem, xh, p_ref, hp_ref, raw, raw_v, raw_send, raw_recv, edge_send, edge_recv = rest[7:]
    x_ref, hx_ref = xh.at[0], xh.at[1]
    loads = []
    for i, (source, target) in enumerate(
        (
            (x_in, x_ref), (hx_in, hx_ref), (off_in, off_ref), (ext_in, ext_ref),
            (count_in, count_ref), (proj_in, proj_ref), (v_in, v_ref), (beta_in, beta_ref),
            (p_in, p_ref), (hp_in, hp_ref), (d_in, d_ref),
        )
    ):
        loads.append(pltpu.make_async_copy(source, target, load_sem.at[i]))
        loads[-1].start()
    zi, yi, xi = (lax.axis_index(a) for a in AXES)
    size_of = dict(zip(AXES, sizes))
    here = dict(zip(AXES, (zi, yi, xi)))
    more_z, more_y = BZ - 1, BY - 1
    own = cz * cy
    lane = lax.broadcasted_iota(jnp.int32, (cols, 128), 1)

    def neighbour(dz, dy, dx):
        step = dict(zip(AXES, (dz, dy, dx)))
        return {a: lax.rem(here[a] + step[a] + size_of[a], size_of[a]) for a in AXES}

    def member(group, offset):
        total = 1
        index = 0
        for a in group:
            total *= size_of[a]
            index = index * size_of[a] + here[a]
        target = lax.rem(index + offset, total)
        device = {}
        for a in reversed(group):
            device[a] = lax.rem(target, size_of[a])
            target = target // size_of[a]
        return {a: device.get(a, here[a]) for a in AXES}, index, total

    octant = [(o // 4, o // 2 % 2, o % 2) for o in range(8)]
    around = [
        (dz, dy, dx)
        for dx in (-1, 0, 1) for dz in (-1, 0, 1) for dy in (-1, 0, 1)
        if (dz, dy, dx) != (0, 0, 0)
    ]
    barrier = pltpu.get_barrier_semaphore()
    greeted = 0
    for group in groups:
        total = member(group, 0)[2]
        for offset in range(1, total):
            pl.semaphore_signal(
                barrier, inc=1, device_id=member(group, offset)[0], device_id_type=MESH
            )
            greeted += 1
    for where in around:
        pl.semaphore_signal(
            barrier, inc=1, device_id=neighbour(*where), device_id_type=MESH
        )
        greeted += 1

    def split_store(kind, cell, value):
        high = value.astype(BF16)
        low = (value - high.astype(F32)).astype(BF16)
        start = cell * 128 if isinstance(cell, int) else pl.multiple_of(cell * 128, 128)
        stack[kind * 32 : kind * 32 + 32, pl.ds(start, 128)] = jnp.concatenate([high, low], 0)

    def split_all(*kinds):
        @pl.loop(0, cz)
        def _(z):
            for y in range(cy):
                cell = z * cy + y
                for kind, ref in kinds:
                    split_store(kind, cell, ref[cell])

    for load in loads[:2]:
        load.wait()
    split_all((HX, hx_ref), (XX, x_ref))

    def products(left, right_from, right_to, count=1):
        m = lax.dot_general(
            stack[left * 32 : (left + count) * 32, :],
            stack[right_from * 32 : right_to * 32, :],
            (((1,), (1,)), ((), ())),
            preferred_element_type=F32,
        )
        parts = [m[32 * i : 32 * i + cols] + m[32 * i + cols : 32 * i + 32] for i in range(count)]
        return parts if count > 1 else parts[0]

    def reduced(which, payload):
        for phase, group in enumerate(slow if which == 0 else groups):
            buf = bufs[which][phase]
            _, index, total = member(group, 0)
            at = phase + (which and len(slow) + (which - 1) * n_red)
            send_sem, recv_sem = red_send.at[at], red_recv.at[at]
            buf[index] = payload
            if phase == 0 and which == 2:
                pl.semaphore_wait(barrier, greeted)
            for offset in range(1, total):
                pltpu.make_async_remote_copy(
                    src_ref=buf.at[index],
                    dst_ref=buf.at[index],
                    send_sem=send_sem,
                    recv_sem=recv_sem,
                    device_id=member(group, offset)[0],
                    device_id_type=MESH,
                ).start()
            yield None
            most = buf.at[pl.ds(0, total - 1)]
            for sem in (recv_sem, send_sem):
                pltpu.make_async_copy(most, most, sem).wait()
            payload = buf[0]
            for slot in range(1, total):
                payload = payload + buf[slot]
        yield payload

    def finish(steps):
        out = None
        for out in steps:
            pass
        return out

    both = lax.dot_general(
        stack[HX * 32 : XX * 32 + 32, :], stack[XX * 32 : XX * 32 + 32, :],
        (((1,), (1,)), ((), ())), preferred_element_type=F32,
    )
    both = jnp.concatenate([both, jnp.zeros((64, 96), F32)], 1)
    turn_hx = both[:cols] + both[cols:32]
    corr = both[32 : 32 + cols] + both[32 + cols :]
    narrow = lax.broadcasted_iota(jnp.int32, (8, 128), 1)

    def merged(tile):
        return tile + pltpu.roll(tile, 128 - cols, 1)

    payload0 = jnp.where(narrow < cols, merged(turn_hx[:8]), 0.0)
    for at, tile in ((1, turn_hx[8:]), (2, corr[:8]), (3, corr[8:])):
        moved = pltpu.roll(merged(tile), at * cols, 1)
        payload0 = jnp.where((narrow >= at * cols) & (narrow < at * cols + cols), moved, payload0)
    solving = reduced(2, payload0)
    next(solving)
    for load in loads[2:]:
        load.wait()
    lane8 = lax.broadcasted_iota(jnp.int32, (8, 128), 1)
    rows = slots * nproj
    pairs = rows // 8
    columns = BZ * BY * BX // 128
    box_lane = lax.broadcasted_iota(jnp.int32, (nproj, BZ * BY * BX), 1)
    box_row = lax.broadcasted_iota(jnp.int32, (nproj, BZ * BY * BX), 0)
    box_a, box_b, box_c = box_lane // (BY * BX), box_lane // BX % BY, box_lane % BX
    for s in range(slots):
        kept = jnp.where(s < count_ref[0, 0, 0], proj_ref[0, s], 0)
        inside = (
            (box_row < kept)
            & (box_a < ext_ref[0, 0, 0, 0, s])
            & (box_b < ext_ref[1, 0, 0, 0, s])
            & (box_c < ext_ref[2, 0, 0, 0, s])
        )
        at = s * nproj
        kept = jnp.where(inside, beta_ref[s], 0.0)
        for c in range(columns):
            where = (0, at // 8 * columns + c, slice(at % 8, at % 8 + nproj), slice(None))
            shared[where] = kept[:, c * 128 : c * 128 + 128]
    lane1 = lax.broadcasted_iota(jnp.int32, (1, 128), 1)
    lane16 = lax.broadcasted_iota(jnp.int32, (nproj, 128), 1)
    slot_at = lane16 % 64 // 16 * (8 // nproj) + lane16 % 8 // nproj
    table = []
    for p in range(nproj):
        mirrored = jnp.concatenate([d_ref[q, p : p + 1, :] for q in range(nproj)], 0)
        sym = 0.5 * (d_ref[p] + mirrored)
        spread = jnp.zeros((nproj, 128), F32)
        for s in range(slots):
            value = jnp.broadcast_to(sym[:, s : s + 1], (nproj, 128))
            spread = jnp.where(slot_at == s, value, spread)
        table.append(spread)
    for d in range(-nproj + 1, nproj):
        row = jnp.zeros((1, 128), F32)
        for p in range(max(0, -d), min(nproj, nproj - d)):
            row = jnp.where(lane1 % nproj == p, table[p][p + d : p + d + 1, :], row)
        shared[0, pairs * columns, d + nproj - 1 : d + nproj, :] = row
    for pair in range(0, pairs, 2):
        lasts = []
        for p in (pair, pair + 1):
            first, last = shared[0, p * columns], shared[0, p * columns + 1]
            lasts.append(last)
            trim[p] = jnp.where(
                lane8 < 48, pltpu.roll(first, 112, 1),
                jnp.where(lane8 < 96, pltpu.roll(first, 96, 1), pltpu.roll(last, 80, 1)),
            )
        trim[pairs + pair // 2] = jnp.where(
            lane8 < 64,
            jnp.where(lane8 < 16, pltpu.roll(lasts[0], 80, 1), pltpu.roll(lasts[0], 64, 1)),
            jnp.where(lane8 < 80, pltpu.roll(lasts[1], 16, 1), lasts[1]),
        )
    trim[pairs + pairs // 2] = shared[0, pairs * columns]
    atom_copies = {}
    for o in (4, 2, 1, 6, 5, 3, 7):
        atom_copies[o] = [
            pltpu.make_async_remote_copy(
                src_ref=source,
                dst_ref=target,
                send_sem=atom_send.at[2 * (o - 1) + i],
                recv_sem=atom_recv.at[2 * (o - 1) + i],
                device_id=neighbour(*octant[o]),
                device_id_type=MESH,
            )
            for i, (source, target) in enumerate(
                (
                    (off_ref, offs.at[o - 1]),
                    (trim, shared.at[o, pl.ds(0, pairs + pairs // 2 + 1)])
                    if octant[o][1] else (shared.at[0], shared.at[o]),
                )
            )
        ]
        for copy in atom_copies[o]:
            copy.start()
    split_all((HP, hp_ref), (PP, p_ref))
    hx_row, x_row, p_row = products(HX, HP, WW, 3)
    first = jnp.where((lane >= 32) & (lane < 64), pltpu.roll(hx_row, 96, 1), x_row)

    def paired(upper, lower):
        upper = upper + pltpu.roll(upper, 112, 1)
        lower = lower + pltpu.roll(lower, 112, 1)
        return jnp.where(lane % 32 < 16, upper, pltpu.roll(lower, 16, 1))

    reduction = reduced(0, paired(first, p_row))

    row8 = lax.broadcasted_iota(jnp.int32, (8, 128), 0)
    in_tile = 128 // BX
    width = BY + cy - 1
    ahead = cy - 1
    nothing = ahead + slots * BZ * width + ahead
    tables = {(0, 0): near0, (0, 1): near1, (1, 0): far0, (1, 1): far1}
    blank_line = jnp.zeros((8, 128), F32)

    @pl.loop(0, slots * BZ)
    def _(block):
        for b in range(BY, width):
            lines[ahead + block * width + b] = blank_line

    for at in [*range(ahead), *range(nothing - ahead, nothing + width)]:
        lines[at] = blank_line

    def build(o):
        dz, dy, dx = octant[o]

        def expand(pair):
            if dy:
                tiles = [shared[o, pair], shared[o, pairs + pair // 2]]
            else:
                tiles = [shared[o, pair * columns + c] for c in range(columns)]
            places = {}
            for at in range(BZ * BY):
                a, b = at // BY, at % BY
                if not dy:
                    places[at] = at // in_tile, at % in_tile
                elif b and a * (BY - 1) + b - 1 < in_tile:
                    places[at] = 0, a * (BY - 1) + b - 1
                elif b:
                    places[at] = 1, pair % 2 * (in_tile // 2) + a * (BY - 1) + b - 1 - in_tile
            for half in range(8 // nproj):
                s = pair * (8 // nproj) + half
                ox = offset(2, s)
                along = (lane8 - ox + 128) & 127
                side = lane8 < ox if dx else lane8 >= ox
                keep = (along < BX) & side & (row8 // nproj == half)
                for at, (tile, k) in places.items():
                    shift = (ox + 128 - BX * k) & 127
                    part = jnp.where(keep, pltpu.roll(tiles[tile], shift, 1), 0.0)
                    lines[ahead + (s * BZ + at // BY) * width + at % BY] = part

        def offset(axis, s):
            return off_ref[axis, 0, 0, 0, s] if o == 0 else offs[o - 1, axis, 0, 0, 0, s]

        for pair in range(pairs):
            expand(pair)

        target = tables[dz, dy]
        top = dx * 64
        ys = more_y if dy else cy

        @pl.loop(0, more_z if dz else cz)
        def _(z):
            starts = []
            for s in range(slots):
                a = z + dz * cz - offset(0, s)
                ok = (a >= 0) & (a < BZ)
                start = jnp.where(ok, ahead + (s * BZ + a) * width - offset(1, s), nothing - offset(1, s))
                starts.append(start)
            for y in range(ys):
                column = pl.ds(pl.multiple_of((z * ys + y) * 128, 128), 128)
                for pair in range(pairs):
                    at = top + pair * 16
                    total = None
                    for half in range(8 // nproj):
                        start = starts[pair * (8 // nproj) + half] + (y + dy * cy)
                        part = lines[start]
                        total = part if total is None else total + part
                    high = total.astype(BF16)
                    low = (total - high.astype(F32)).astype(BF16)
                    target[at : at + 16, column] = jnp.concatenate([high, low], 0)

    for z in range(cz):
        for y in range(cy):
            inner[z, y] = jnp.zeros((cols, 128), F32)
            inner[2 * cz + z, y] = jnp.zeros((cols, 128), F32)
    def build_all(owners):
        for o in owners:
            for copy in atom_copies[o]:
                copy.wait()
            build(o)

    build(0)
    early_z = cz // 3
    early_to = [(-1, 0, 0), (1, 0, 0), (0, -1, 0)] + ([] if ny == 2 else [(0, 1, 0)])
    raw_copies = []
    for d, where in enumerate(early_to):
        for i, (source, target) in enumerate(
            (
                (xh.at[:, pl.ds(0, early_z * cy)], raw.at[d]),
                (v_ref.at[pl.ds(0, early_z)], raw_v.at[d]),
            )
        ):
            raw_copies.append(
                pltpu.make_async_remote_copy(
                    src_ref=source,
                    dst_ref=target,
                    send_sem=raw_send.at[2 * d + i],
                    recv_sem=raw_recv.at[2 * d + i],
                    device_id=neighbour(*where),
                    device_id_type=MESH,
                )
            )
            raw_copies[-1].start()
    def packed(read, rows_of):
        at_lane = lax.broadcasted_iota(jnp.int32, (rows_of, 128), 1)
        for q in range(tiles_of(own)):
            low = jnp.zeros((rows_of, 128), F32)
            high = low
            for j in range(min(PER_TILE, own - PER_TILE * q)):
                tile = read(PER_TILE * q + j)
                keep = (at_lane >= EDGE * j) & (at_lane < EDGE * j + EDGE)
                low = jnp.where(keep, pltpu.roll(tile, EDGE * j, 1) if j else tile, low)
                turn = (EDGE * j + EDGE) % 128
                high = jnp.where(keep, pltpu.roll(tile, turn, 1) if turn else tile, high)
            yield q, low, high

    edge_v[...] = jnp.zeros(edge_v.shape, F32)
    for kind in range(2):
        for q, low, high in packed(lambda cell: xh[kind, cell], cols):
            edge_out[0, kind, q] = low
            edge_out[1, kind, q] = high
    for q, low, high in packed(lambda cell: v_ref[cell // cy, cell % cy : cell % cy + 1, :], 1):
        edge_v[0, q : q + 1, :] = low
        edge_v[1, q : q + 1, :] = high
    next(solving)
    next(reduction)
    edge_copies = []
    for side, step in enumerate((-1, 1)):
        for i, (source, target) in enumerate(
            ((edge_out.at[side], edge_in.at[side]), (edge_v.at[side], edge_v_in.at[side]))
        ):
            edge_copies.append(
                pltpu.make_async_remote_copy(
                    src_ref=source,
                    dst_ref=target,
                    send_sem=edge_send.at[2 * side + i],
                    recv_sem=edge_recv.at[2 * side + i],
                    device_id=neighbour(0, 0, step),
                    device_id_type=MESH,
                )
            )
            edge_copies[-1].start()
    build_all((4, 2, 6, 1, 5, 3))
    sums0 = finish(solving)
    sums0 = solved(sums0, cols, acol)
    theta_cols = sums0

    @pl.loop(0, cz)
    def _(z):
        for y in range(cy):
            cell = z * cy + y
            xs = x_ref[cell]
            value = hx_ref[cell]
            for k in range(cols):
                value = value - theta_cols[k] * xs[k : k + 1, :]
            vv = v_ref[z, y : y + 1, :]
            value = value * (1.0 / (1.0 + vv * vv))
            zext[cz + z, y] = value
            inner[cz + z, y] = value
            w_ref[cell] = value
            split_store(WW, cell, value)
            if y < more_y:
                place = pl.ds(pl.multiple_of((z * more_y + y) * 128, 128), 128)
                high = value.astype(BF16)
                low = (value - high.astype(F32)).astype(BF16)
                wside[:, place] = jnp.concatenate([high, low], 0)

    two_y = ny == 2
    split = early_z + (cz - early_z) // 2

    def some(ref, z, dz, y, dy):
        return ref.at[pl.ds(z, dz), pl.ds(y, dy)]

    def layers(target, base, z, dz, where):
        return some(zext, cz + z, dz, 0, cy), some(target, base + z, dz, 0, cy), where

    def bulk(z, dz):
        sends = [
            layers(zext, 2 * cz, z, dz, (-1, 0, 0)),
            layers(zext, 0, z, dz, (1, 0, 0)),
            layers(ybuf.at[1], 0, z, dz, (0, -1, 0)),
        ]
        if not two_y:
            sends.append(layers(ybuf.at[0], 0, z, dz, (0, 1, 0)))
        return sends

    early = bulk(early_z, split - early_z)
    late = bulk(split, cz - split)

    def launch(sends, send_sem, recv_sem, first=0):
        copies = []
        for i, (source, target, where) in enumerate(sends, start=first):
            copies.append(
                pltpu.make_async_remote_copy(
                    src_ref=source,
                    dst_ref=target,
                    send_sem=send_sem.at[i],
                    recv_sem=recv_sem.at[i],
                    device_id=neighbour(*where),
                    device_id_type=MESH,
                )
            )
            copies[-1].start()
        return copies

    copies = launch(early, halo_send, halo_recv)
    outs = [
        pltpu.make_async_copy(source, target, out_sem.at[i])
        for i, (source, target) in enumerate(
            ((w_ref, w_out), (hw_ref, hw_out), (sums_ref, sums_out))
        )
    ]
    outs[0].start()
    build_all((7,))
    def span(step):
        return (max(0, -step), 2 - abs(step))

    slot_of = {}
    filled = 0
    for where in around:
        slot_of[where] = filled
        filled += span(where[0])[1] * span(where[1])[1] * span(where[2])[1]
    def hand_out(z, y):
        for where in around:
            (z0, zn), (y0, yn), (x0, xn) = (span(step) for step in where)
            if z0 <= z < z0 + zn and y0 <= y < y0 + yn:
                at = slot_of[where] + ((z - z0) * yn + y - y0) * xn
                pltpu.make_async_remote_copy(
                    src_ref=parts4.at[z, y, pl.ds(x0, xn)],
                    dst_ref=parts_in.at[pl.ds(at, xn)],
                    send_sem=part_sem.at[0],
                    recv_sem=part_sem.at[1],
                    device_id=neighbour(*where),
                    device_id_type=MESH,
                ).start()

    w_rows = stack.at[WW * 32 : WW * 32 + 32]
    lane4 = lax.broadcasted_iota(jnp.int32, (4, 128), 1)
    for early_tiles in (((1, 1), (1, 0), (0, 1)), ((0, 0),)):
        for dz, dy in early_tiles:
            table = tables[dz, dy]
            source = wside if dy else w_rows
            m = lax.dot_general(
                table[...], source[:, : table.shape[1]],
                (((1,), (1,)), ((), ())), preferred_element_type=F32,
            )
            m = jnp.concatenate([m, jnp.zeros((128, 128 - 2 * cols), F32)], 1)
            m = jnp.transpose(m)
            m = m[:cols] + m[cols : 2 * cols]
            m = m + pltpu.roll(m, 128 - 8, 1)
            upper, lower = m[:8], m[8:]
            both = jnp.where(lane8 % 16 < 8, upper, pltpu.roll(lower, 8, 1))
            moved = pltpu.roll(both, 64, 1)
            parts4[dz, dy, 0] = jnp.where(lane4 < 64, both[:4], moved[4:])
            parts4[dz, dy, 1] = jnp.where(lane4 < 64, moved[:4], both[4:])
        for dz, dy in early_tiles:
            hand_out(dz, dy)

    late_copies = launch(late, halo_send, halo_recv, len(early))
    w_row = products(WW, HP, WW)
    w_row2 = products(WW, XX, HW)
    for copy in edge_copies:
        copy.wait()
    for side, target in enumerate((xr, xl)):
        for q in range(tiles_of(own)):
            value = edge_in[side, 1, q]
            xs = edge_in[side, 0, q]
            for k in range(cols):
                value = value - theta_cols[k] * xs[k : k + 1, :]
            vv = edge_v_in[side, q : q + 1, :]
            target[q] = value * (1.0 / (1.0 + vv * vv))
    for copy in raw_copies:
        copy.wait()
    for d in range(len(early_to)):
        target, base = ((zext, 2 * cz), (zext, 0), (ybuf.at[1], 0), (ybuf.at[0], 0))[d]

        @pl.loop(0, early_z)
        def _(z):
            for y in range(cy):
                cell = z * cy + y
                xs = raw[d, 0, cell]
                value = raw[d, 1, cell]
                for k in range(cols):
                    value = value - theta_cols[k] * xs[k : k + 1, :]
                vv = raw_v[d, z, y : y + 1, :]
                target[base + z, y] = value * (1.0 / (1.0 + vv * vv))

    @pl.loop(0, cz)
    def _(z):
        for y in range(cy):
            centre = inner[cz + z, y]
            vv = v_ref[z, y : y + 1, :]
            total = centre * (vv - 1.5 * LAP_CENTER)
            for k, weight in enumerate(LAP_COEFFS, start=1):
                tiles = [inner[cz + z, t] for t in (y + k, y - k) if 0 <= t < cy]
                if k < cz:
                    tiles += [inner[cz + z + k, y], inner[cz + z - k, y]]
                beside = None
                for tile in tiles:
                    beside = tile if beside is None else beside + tile
                if beside is not None:
                    total = total - 0.5 * weight * beside
            hw_ref[z * cy + y] = total

    for cell in range(own):
        left, right = xl[cell // PER_TILE], xr[cell // PER_TILE]
        turn = (256 - EDGE - EDGE * (cell % PER_TILE)) % 128
        left = pltpu.roll(left, turn, 1) if turn else left
        shift = (128 - EDGE * (cell % PER_TILE)) % 128
        right = pltpu.roll(right, shift, 1) if shift else right
        edges[cell] = jnp.where(lane < 64, right, left)

    @pl.loop(0, cz)
    def _(z):
        for y in range(cy):
            cell = z * cy + y
            edge = edges[cell]
            centre = inner[cz + z, y]
            total = hw_ref[cell]
            for k, weight in enumerate(LAP_COEFFS, start=1):
                beside = pltpu.roll(jnp.where(lane < k, edge, centre), 128 - k, 1)
                beside = beside + pltpu.roll(jnp.where(lane >= 128 - k, edge, centre), k, 1)
                total = total - 0.5 * weight * beside
            hw_ref[cell] = total
    next(reduction)
    for sem in (part_sem.at[1], part_sem.at[0]):
        pltpu.make_async_copy(parts_in, parts_in, sem).wait()
    gathered = {}
    for dz in range(2):
        for dy in range(2):
            sums = []
            for dx in range(2):
                total = None
                for from_z in range(2):
                    for from_y in range(2):
                        for from_x in range(2):
                            where = (dz - from_z, dy - from_y, dx - from_x)
                            if where == (0, 0, 0):
                                tile = parts4[dz, dy, dx]
                            else:
                                (z0, _), (y0, yn), (x0, xn) = (span(step) for step in where)
                                at = ((from_z - z0) * yn + from_y - y0) * xn + from_x - x0
                                tile = parts_in[slot_of[where] + at]
                            total = tile if total is None else total + tile
                sums.append(total)
            turned = [pltpu.roll(total, 64, 1) for total in sums]
            gathered[dz, dy] = jnp.concatenate(
                [
                    jnp.where(lane4 < 64, sums[0], turned[1]),
                    jnp.where(lane4 < 64, turned[0], sums[1]),
                ],
                0,
            )
    coef_at = (pairs * columns, pairs + pairs // 2)
    lefts = {}
    for dz in range(2):
        for dy in range(2):
            total = gathered[dz, dy]
            o = dz * 4 + dy * 2
            coefs = jnp.where(
                lane8 < 64, shared[o, coef_at[dy]], shared[o + 1, coef_at[dy]]
            )
            mixed = None
            for d in range(-nproj + 1, nproj):
                term = pltpu.roll(total, (128 - d) % 128, 1) if d else total
                term = term * coefs[d + nproj - 1 : d + nproj, :]
                mixed = term if mixed is None else mixed + term
            low_half = lane8 % 16 < 8
            mixed = jnp.concatenate(
                [
                    jnp.where(low_half, mixed, pltpu.roll(mixed, 8, 1)),
                    jnp.where(low_half, pltpu.roll(mixed, 120, 1), mixed),
                ],
                0,
            )
            high = mixed.astype(BF16)
            low = (mixed - high.astype(F32)).astype(BF16)
            lefts[dz, dy] = jnp.concatenate([high, low], 0)

    for z in range(cz):
        sums = {}
        for dz in range(2 if z < more_z else 1):
            for dy in range(2):
                ys = more_y if dy else cy
                m = lax.dot_general(
                    lefts[dz, dy], tables[dz, dy][:, z * ys * 128 : (z + 1) * ys * 128],
                    (((1,), (0,)), ((), ())), preferred_element_type=F32,
                )
                m = m[:cols] + m[cols:]
                for y in range(ys):
                    part = m[:, y * 128 : y * 128 + 128]
                    sums[y] = sums[y] + part if y in sums else part
        for y in range(cy):
            nf[z, y] = sums[y]
    for copy in copies + late_copies:
        copy.wait()
    hw_sum = None
    for cell in range(own):
        z, y = cell // cy, cell % cy
        total = hw_ref[cell] + nf[z, y]
        weights = {}
        for k, weight in enumerate(LAP_COEFFS, start=1):
            keys = [("z", z + k), ("z", z - k), (1, y + k - cy), (1 if two_y else 0, y - k + cy)]
            for key, inside in zip(keys, (z + k < cz, z - k >= 0, y + k < cy, y - k >= 0)):
                if not inside:
                    weights[key] = weights.get(key, 0.0) - 0.5 * weight
        for (where, at), weight in weights.items():
            tile = zext[cz + at, y] if where == "z" else ybuf[where, z, at]
            total = total + weight * tile
        hw_ref[cell] = total
        split_store(HW, cell, total)
        if y == cy - 1:
            plane = slice(z * cy * 128, (z + 1) * cy * 128)
            part = lax.dot_general(
                stack[HW * 32 : HW * 32 + 32, plane], stack[XX * 32 : HW * 32, plane],
                (((1,), (1,)), ((), ())), preferred_element_type=F32,
            )
            hw_sum = part if hw_sum is None else hw_sum + part
    outs[1].start()
    hw_row = w_row2_pad(hw_sum[:cols] + hw_sum[cols:])
    second = jnp.where(lane < 96, hw_row, pltpu.roll(w_row2_pad(w_row2), 32, 1))
    closing = reduced(1, paired(w_row, second))
    next(closing)
    next(reduction)
    next(closing)
    sums1 = next(reduction)
    sums2 = finish(closing)
    sums_ref[...] = jnp.concatenate([sums1, sums2], 0)
    outs[2].start()
    for out in outs:
        out.wait()


def finish_out(weight, w_ref, hw_ref, sums_ref, w_out, hw_out, gram_out, ray_out, gram_ref, ray_ref, sems):
    copies = [
        pltpu.make_async_copy(source, target, sems.at[i])
        for i, (source, target) in enumerate(
            ((w_ref, w_out), (hw_ref, hw_out), (gram_ref, gram_out), (ray_ref, ray_out))
        )
    ]
    for copy in copies[:2]:
        copy.start()
    sums1, sums2 = sums_ref[:16], sums_ref[16:]
    lane = lax.broadcasted_iota(jnp.int32, (16, 128), 1)
    rows = jnp.concatenate([sums1, pltpu.roll(sums1, 112, 1), sums2, pltpu.roll(sums2, 112, 1)], 0)
    rows = rows * weight
    turned = jnp.transpose(jnp.concatenate([rows, jnp.zeros_like(rows)], 0))

    def direct(row, group, target):
        return rows[16 * row : 16 * row + 16, :], 32 * group, target

    def flipped(row, group, target):
        return turned[32 * group : 32 * group + 16, :], 16 * row, target

    def laid(parts):
        total = None
        for tile, begin, target in parts:
            shift = (16 * target - begin) % 128
            tile = pltpu.roll(tile, shift, 1) if shift else tile
            tile = jnp.where((lane >= 16 * target) & (lane < 16 * target + 16), tile, 0.0)
            total = tile if total is None else total + tile
        return total

    gram = [
        [direct(0, 2, 0), flipped(2, 2, 1), direct(0, 3, 2)],
        [direct(2, 2, 0), direct(3, 3, 1), direct(2, 3, 2)],
        [direct(1, 2, 0), flipped(2, 3, 1), direct(1, 3, 2)],
    ]
    rayleigh = [
        [flipped(0, 1, 0), flipped(3, 0, 1), direct(0, 0, 2)],
        [direct(2, 1, 0), flipped(3, 2, 1), direct(2, 0, 2)],
        [direct(1, 1, 0), flipped(3, 1, 1), direct(1, 0, 2)],
    ]
    for i in range(3):
        gram_ref[16 * i : 16 * i + 16, :] = laid(gram[i])[:, :48]
        ray_ref[16 * i : 16 * i + 16, :] = laid(rayleigh[i])[:, :48]
    for copy in copies[2:]:
        copy.start()
    for copy in copies:
        copy.wait()


def w_row2_pad(row):
    return jnp.concatenate([row, jnp.zeros((row.shape[0], 128 - row.shape[1]), row.dtype)], 1)


def per_device(
    sizes,
    block_x, block_hx, block_p, block_hp, potential, projectors, coupling,
    atom_count, proj_count, offsets, extents,
):
    cols, cz, cy, cx = block_x.shape
    slots, nproj = projectors.shape[-3], projectors.shape[-2]
    nz, ny, nx = sizes
    own = cz * cy
    turned = [
        jnp.transpose(b, (1, 2, 0, 3)).reshape(own, cols, cx)
        for b in (block_x, block_hx, block_p, block_hp)
    ]
    groups = (("gz", "gy"), ("gx",)) if nz * ny <= 16 else (("gz",), ("gy",), ("gx",))
    size_of = dict(zip(AXES, sizes))
    totals = []
    for group in groups:
        total = 1
        for a in group:
            total *= size_of[a]
        totals.append(total)
    tile = (cols, 128)
    rows = slots * nproj
    scratch = [
        pltpu.VMEM((own,) + tile, F32),
        pltpu.VMEM((own,) + tile, F32),
        pltpu.VMEM((2 * cols, 128), F32),
        pltpu.SMEM(offsets.shape, jnp.int32),
        pltpu.SMEM(extents.shape, jnp.int32),
        pltpu.SMEM(atom_count.shape, jnp.int32),
        pltpu.SMEM(proj_count.shape[2:], jnp.int32),
        pltpu.VMEM((cols, cols, 128), F32),
        pltpu.VMEM((nproj, nproj, slots), F32),
        pltpu.VMEM(potential.shape, F32),
        pltpu.VMEM(projectors.shape[3:], F32),
        pltpu.VMEM((192, own * 128), BF16),
        pltpu.VMEM((3 * cz, cy) + tile, F32),
        pltpu.VMEM((2, cz, cy) + tile, F32),
        pltpu.VMEM((tiles_of(own),) + tile, F32),
        pltpu.VMEM((tiles_of(own),) + tile, F32),
        pltpu.VMEM((2, 2, tiles_of(own)) + tile, F32),
        pltpu.VMEM((2, 2, tiles_of(own)) + tile, F32),
        pltpu.VMEM((2, 8 * (-(-tiles_of(own) // 8)), 128), F32),
        pltpu.VMEM((2, 8 * (-(-tiles_of(own) // 8)), 128), F32),
        pltpu.VMEM((own,) + tile, F32),
        pltpu.VMEM((3 * cz, cy) + tile, F32),
        pltpu.VMEM((cz, cy) + tile, F32),
        pltpu.VMEM((8, rows // 8 * (BZ * BY * BX // 128) + 1, 8, 128), F32),
        pltpu.VMEM((rows // 8 + rows // 16 + 1, 8, 128), F32),
        pltpu.SMEM((7,) + offsets.shape, jnp.int32),
        pltpu.VMEM((slots * BZ * (BY + cy - 1) + BY + 3 * (cy - 1), 8, 128), F32),
        pltpu.VMEM((128, own * 128), BF16),
        pltpu.VMEM((128, cz * (BY - 1) * 128), BF16),
        pltpu.VMEM((128, (BZ - 1) * cy * 128), BF16),
        pltpu.VMEM((128, (BZ - 1) * (BY - 1) * 128), BF16),
        pltpu.VMEM((2 * cols, cz * (BY - 1) * 128), BF16),
        pltpu.VMEM((2, 2, 2, 4, 128), F32),
        pltpu.VMEM((56, 4, 128), F32),
    ]
    scratch += [pltpu.VMEM((size_of[a], cols, 128), F32) for a in ("gx", "gz", "gy")]
    scratch += [pltpu.VMEM((t, cols, 128), F32) for t in totals]
    scratch += [pltpu.VMEM((t, 8, 128), F32) for t in totals]
    scratch += [
        pltpu.SemaphoreType.DMA((3 + 2 * len(groups),)),
        pltpu.SemaphoreType.DMA((3 + 2 * len(groups),)),
        pltpu.SemaphoreType.DMA((8,)),
        pltpu.SemaphoreType.DMA((8,)),
        pltpu.SemaphoreType.DMA((14,)),
        pltpu.SemaphoreType.DMA((14,)),
        pltpu.SemaphoreType.DMA((2,)),
        pltpu.SemaphoreType.DMA((11,)),
        pltpu.SemaphoreType.DMA((3,)),
    ]
    ways = 3 if ny == 2 else 4
    early_z = cz // 3
    scratch += [
        pltpu.VMEM((2, own) + tile, F32),
        pltpu.VMEM((own,) + tile, F32),
        pltpu.VMEM((own,) + tile, F32),
        pltpu.VMEM((ways, 2, early_z * cy) + tile, F32),
        pltpu.VMEM((ways, early_z, cy, 128), F32),
        pltpu.SemaphoreType.DMA((2 * ways,)),
        pltpu.SemaphoreType.DMA((2 * ways,)),
        pltpu.SemaphoreType.DMA((4,)),
        pltpu.SemaphoreType.DMA((4,)),
    ]
    vmem = pl.BlockSpec(memory_space=pltpu.VMEM)
    w, hw, sums = pl.pallas_call(
        functools.partial(kernel, sizes, groups, (cz, cy, cx, slots, nproj, cols)),
        out_shape=(
            pltpu.VMEM((own,) + tile, F32),
            pltpu.VMEM((own,) + tile, F32),
            pltpu.VMEM((2 * cols, 128), F32),
        ),
        in_specs=[pl.BlockSpec(memory_space=pltpu.HBM)] * 11,
        out_specs=(pl.BlockSpec(memory_space=pl.ANY),) * 3,
        scratch_shapes=scratch,
        compiler_params=pltpu.CompilerParams(
            collective_id=0, has_side_effects=True, vmem_limit_bytes=VMEM_LIMIT
        ),
    )(
        offsets, extents, atom_count, proj_count[0, 0],
        jnp.transpose(coupling[0, 0, 0], (1, 2, 0)),
        *turned, potential, projectors[0, 0, 0],
    )
    square = jax.ShapeDtypeStruct((3 * cols, 3 * cols), F32)
    field = jax.ShapeDtypeStruct((own,) + tile, F32)
    w, hw, gram, rayleigh = pl.pallas_call(
        functools.partial(finish_out, 1.0 / (own * cx * nz * ny * nx)),
        out_shape=(field, field, square, square),
        in_specs=[vmem] * 3,
        out_specs=(pl.BlockSpec(memory_space=pl.ANY),) * 4,
        scratch_shapes=[
            pltpu.VMEM(square.shape, F32),
            pltpu.VMEM(square.shape, F32),
            pltpu.SemaphoreType.DMA((4,)),
        ],
        compiler_params=pltpu.CompilerParams(vmem_limit_bytes=4 << 20),
    )(w, hw, sums)
    w, hw = (jnp.transpose(b.reshape(cz, cy, cols, cx), (2, 0, 1, 3)) for b in (w, hw))
    return (w, hw, gram, rayleigh)


def solution(mesh):
    sizes = tuple(mesh.shape[a] for a in AXES)
    in_specs = (
        P(None, "gz", "gy", "gx"),
        P(None, "gz", "gy", "gx"),
        P(None, "gz", "gy", "gx"),
        P(None, "gz", "gy", "gx"),
        P("gz", "gy", "gx"),
        P("gz", "gy", "gx", None, None, None),
        P("gz", "gy", "gx", None, None, None),
        P("gz", "gy", "gx"),
        P("gz", "gy", "gx", None),
        P(None, "gz", "gy", "gx", None),
        P(None, "gz", "gy", "gx", None),
    )
    out_specs = (P(None, "gz", "gy", "gx"), P(None, "gz", "gy", "gx"), P(), P())
    return jax.shard_map(
        functools.partial(per_device, sizes),
        mesh=mesh, in_specs=in_specs, out_specs=out_specs, check_vma=False,
    )
```
